8 devices in a mesh: dp: 2 (over y, z), sp: 4 (over x, core).
Axes of the slice: x: 2, y: 2, z: 1, core: 2. Of those that a mesh axis runs over, the one named last changes fastest.
Arguments:
- x: bfloat16 [16384, 2304], P(('dp', 'sp')), parts along dimension 0
- gain: bfloat16 [2304], replicated
- wq: bfloat16 [2304, 2048], P('sp')
- wk: bfloat16 [2304, 1024], P('sp')
- wv: bfloat16 [2304, 1024], P('sp')
- wo: bfloat16 [2048, 2304], P('sp')
Outputs:
- output: bfloat16 [16384, 2304], P(('dp', 'sp')), parts along dimension 0
There are 2 independent parts. The reference program is written for one: setup_inputs(seed, part) draws one part's arguments, and reference() takes and returns one part's arrays. A program takes and returns all parts, laid end to end along the dimension named above; an argument that names none is the same for every part.
All inputs are finite; a program needn't handle non-finite values.
Results may differ from the reference program's by a relative error of at most 0.012.
Values are sent between devices in bfloat16 or wider.
A program may use at most 2 GiB of HBM per device.

```python
import jax
import jax.numpy as jnp
from jax import lax

ROWS = 8192
D = 2304
HEADS = 8
KV_HEADS = 4
HEAD = 256
THETA = 10000


def setup_inputs(seed: int = 0, part: int = 0) -> dict:
    kx, kn, kq, kk, kv, ko = jax.random.split(jax.random.key(seed), 6)

    def weights(key, rows, columns):
        return jax.random.normal(key, (rows, columns), jnp.float32) * rows**-0.5

    drawn = {
        "x": jax.random.normal(jax.random.fold_in(kx, part), (ROWS, D), jnp.float32),
        "gain": 1 + 0.1 * jax.random.normal(kn, (D,), jnp.float32),
        "wq": 2 * weights(kq, D, HEADS * HEAD),
        "wk": 2 * weights(kk, D, KV_HEADS * HEAD),
        "wv": 4 * weights(kv, D, KV_HEADS * HEAD),
        "wo": weights(ko, HEADS * HEAD, D),
    }
    return {k: v.astype(jnp.bfloat16) for k, v in drawn.items()}


def normed(x, gain):
    wide = x.astype(jnp.float32)
    scale = lax.rsqrt(jnp.mean(wide * wide, -1, keepdims=True) + 1e-6)
    return (wide * scale * gain.astype(jnp.float32)).astype(jnp.bfloat16)


def turned(t, place, theta):
    half = t.shape[-1] // 2
    angle = place.astype(jnp.float32)[:, None] * theta ** (-jnp.arange(half, dtype=jnp.float32) / half)
    cos, sin = jnp.cos(angle)[:, None], jnp.sin(angle)[:, None]
    a, b = t[..., :half].astype(jnp.float32), t[..., half:].astype(jnp.float32)
    return jnp.concatenate([a * cos - b * sin, b * cos + a * sin], -1).astype(jnp.bfloat16)


def matmul(a, w):
    return jnp.dot(a, w, preferred_element_type=jnp.float32).astype(jnp.bfloat16)


def einsum(form, a, b):
    return jnp.einsum(form, a.astype(jnp.float32), b.astype(jnp.float32))


def attention(q, k, v):
    scores = einsum("tgsd,ugd->gstu", q, k) * q.shape[-1] ** -0.5
    token = jnp.arange(q.shape[0])
    scores = jnp.where(token[:, None] >= token, scores, -jnp.inf)
    weights = jax.nn.softmax(scores, -1).astype(jnp.bfloat16)
    return einsum("gstu,ugd->tgsd", weights, v).astype(jnp.bfloat16)


def reference(x, gain, wq, wk, wv, wo):
    a, place = normed(x, gain), jnp.arange(ROWS)
    q = turned(matmul(a, wq).reshape(ROWS, HEADS, HEAD), place, THETA).reshape(ROWS, KV_HEADS, -1, HEAD)
    k = turned(matmul(a, wk).reshape(ROWS, KV_HEADS, HEAD), place, THETA)
    v = matmul(a, wv).reshape(ROWS, KV_HEADS, HEAD)
    seen = attention(q, k, v).reshape(ROWS, HEADS * HEAD)
    return (x.astype(jnp.float32) + jnp.dot(seen, wo, preferred_element_type=jnp.float32)).astype(jnp.bfloat16)
```

```python
import functools

import jax
import jax.numpy as jnp
from jax import lax
from jax.experimental import pallas as pl
from jax.experimental.pallas import tpu as pltpu
from jax.sharding import PartitionSpec as P

NEG = -1e30
HIDDEN = 2 * NEG
LOG2E = 1.4426950408889634
VMEM = 56 * 2**20
HEAD = 256
THETA = 10000
SCALE = HEAD**-0.5
E = SCALE * LOG2E
STRIP = 512
BK = 512
CHUNKS = 4


SIBLING = [(0, 1), (1, 0), (2, 3), (3, 2)]
ACROSS = [(0, 2), (2, 0), (1, 3), (3, 1)]
BACK = [(0, 2), (1, 3)]
GROUPS = [(0, 1), (1, 0)]
ORDER = ((3, 2, 0, 1), (0, 1, 2, 3))


def _dot(a, b, ca, cb):
    return lax.dot_general(a, b, (((ca,), (cb,)), ((), ())), preferred_element_type=jnp.float32)


def _project(at_ref, a0_ref, a1_ref, own_ref, sib_ref, wx_ref, wy_ref, cos_ref, sin_ref, *rest, first):
    out_ref, sent_ref, w_s = rest if first else (rest[1], None, rest[2])
    slot, chip, core, group = at_ref[0], at_ref[1], at_ref[2], at_ref[3]
    i = pl.program_id(0)
    rows = own_ref.shape[1]

    @pl.when(i == 0)
    def _():
        here, there = 2 * rows * chip, 2 * rows * (1 - chip)
        for at, ref in ((here + rows * core, own_ref), (here + rows * (1 - core), sib_ref)):
            w_s[pl.ds(pl.multiple_of(at, 64), rows), :] = ref[0]
        for at, ref in ((there + rows * group, wx_ref), (there + rows * (1 - group), wy_ref)):
            w_s[pl.ds(pl.multiple_of(at, 64), rows), :] = ref[...]

    def part(a_ref):
        t = _dot(a_ref[...], w_s[...], 1, 0).astype(jnp.bfloat16).astype(jnp.float32)
        cos, sin = cos_ref[...], sin_ref[...]
        half = HEAD // 2
        for n in range(2):
            p, q = t[:, n * HEAD : n * HEAD + half], t[:, n * HEAD + half : (n + 1) * HEAD]
            u, v = p * cos - q * sin, q * cos + p * sin
            if n == 1:
                u, v = jnp.where(slot < 2, u, p), jnp.where(slot < 2, v, q)
            got = jnp.concatenate([u, v], axis=1).astype(jnp.bfloat16)
            out_ref[0, n] = got
            if sent_ref is not None:
                sent_ref[n] = got

    @pl.when(i < pl.num_programs(0) // 2)
    def _():
        part(a0_ref)

    @pl.when(i >= pl.num_programs(0) // 2)
    def _():
        part(a1_ref)


def project(at, a_own, a_sib, w_own, w_sib, wx, wy, cos, sin, done):
    tokens, depth = a_own.shape
    rows, width = wx.shape
    bm = 512
    n = tokens // bm
    first = done is None

    def place(i, at_ref):
        return jnp.where(i < n, at_ref[2] * n + i, (1 - at_ref[2]) * n + i - n)

    weights = pl.BlockSpec((1, rows, width), lambda i, at_ref: (at_ref[0], 0, 0))
    fetched = pl.BlockSpec((rows, width), lambda i, at_ref: (0, 0))
    table = pl.BlockSpec((bm, HEAD // 2), lambda i, at_ref: (place(i, at_ref), 0))
    specs = [
        pl.BlockSpec((bm, depth), lambda i, at_ref: (jnp.minimum(i, n - 1), 0)),
        pl.BlockSpec((bm, depth), lambda i, at_ref: (jnp.maximum(i - n, 0), 0)),
        weights, weights, fetched, fetched, table, table,
    ]
    given = [a_own, a_sib, w_own, w_sib, wx, wy, cos, sin]
    out_shape = [jax.ShapeDtypeStruct((4, 2, 2 * tokens, HEAD), jnp.bfloat16)]
    out_specs = [pl.BlockSpec((1, 2, bm, HEAD), lambda i, at_ref: (at_ref[0], 0, place(i, at_ref), 0))]
    alias = {}
    if first:
        out_shape.append(jax.ShapeDtypeStruct((2, 2 * tokens, HEAD), jnp.bfloat16))
        out_specs.append(pl.BlockSpec((2, bm, HEAD), lambda i, at_ref: (0, place(i, at_ref), 0)))
    else:
        given.append(done)
        specs.append(pl.BlockSpec(memory_space=pl.ANY))
        alias = {len(given): 0}
    return pl.pallas_call(
        functools.partial(_project, first=first),
        grid_spec=pltpu.PrefetchScalarGridSpec(
            num_scalar_prefetch=1, grid=(2 * n,), in_specs=specs, out_specs=out_specs,
            scratch_shapes=[pltpu.VMEM((4 * rows, width), jnp.bfloat16)],
        ),
        out_shape=out_shape,
        input_output_aliases=alias,
        compiler_params=pltpu.CompilerParams(dimension_semantics=("arbitrary",), vmem_limit_bytes=VMEM),
        cost_estimate=pl.CostEstimate(flops=4 * tokens * depth * width, transcendentals=0, bytes_accessed=4 * tokens * depth),
        name="project",
    )(at, *given)


def _step(strips, k, v, top_s, mix_s):
    scores = [_dot(k, q, 1, 1) for _, q, _ in strips]
    weights, keeps = [], []
    for (at, _, ok), s in zip(strips, scores):
        if ok is not None:
            s = jnp.where(ok, s, HIDDEN)
        cols = slice(at, at + STRIP)
        old = top_s[:, cols]
        top = jnp.maximum(old, s.max(axis=0, keepdims=True))
        top_s[:, cols] = top
        weights.append(jnp.exp2((s - top) * E).astype(jnp.bfloat16))
        keeps.append(jnp.exp2((old - top) * E))
    values = jnp.concatenate([v.T, jnp.ones((8, BK), jnp.bfloat16)], axis=0)
    for (at, _, _), p, keep in zip(strips, weights, keeps):
        cols = slice(at, at + STRIP)
        mix_s[:, cols] = mix_s[:, cols] * keep + _dot(values, p, 1, 0)


def _finish(at, top_s, mix_s):
    cols = slice(at, at + STRIP)
    total = mix_s[HEAD : HEAD + 1, cols]
    return (mix_s[:HEAD, cols] * (1 / total)).T, top_s[:, cols] * SCALE + jnp.log(total)


def _own(q_ref, k_ref, v_ref, o_ref, lse_ref, top_s, mix_s):
    bq = q_ref.shape[2]
    iq = pl.program_id(1)
    per = bq // STRIP
    top_s[...] = jnp.full(top_s.shape, NEG, jnp.float32)
    mix_s[...] = jnp.zeros(mix_s.shape, jnp.float32)

    def block(j, least):
        here = pl.ds(pl.multiple_of(j * BK, BK), BK)
        ok = None
        if least is not None:
            ok = lax.broadcasted_iota(jnp.int32, (BK, STRIP), 1) >= lax.broadcasted_iota(jnp.int32, (BK, STRIP), 0)
        strips = []
        for n in range(2):
            for s in range(least or 0, per):
                q = q_ref[0, n, s * STRIP : (s + 1) * STRIP, :]
                strips.append((n * bq + s * STRIP, q, ok if s == least else None))
        _step(strips, k_ref[0, 0, here, :], v_ref[0, 0, here, :], top_s, mix_s)

    lax.fori_loop(0, iq * per, lambda j, _: block(j, None), None)
    for s in range(per):
        block(iq * per + s, s)
    for n in range(2):
        for s in range(per):
            out, lse = _finish(n * bq + s * STRIP, top_s, mix_s)
            o_ref[0, n, s * STRIP : (s + 1) * STRIP, :] = out
            lse_ref[0, n : n + 1, s * STRIP : (s + 1) * STRIP] = lse


def attend_own(made):
    tokens = made.shape[2]
    bq = 2048
    return pl.pallas_call(
        _own,
        grid=(2, tokens // bq),
        in_specs=[
            pl.BlockSpec((1, 2, bq, HEAD), lambda h, i: (h, 0, i, 0)),
            pl.BlockSpec((1, 1, tokens, HEAD), lambda h, i: (2 + h, 0, 0, 0)),
            pl.BlockSpec((1, 1, tokens, HEAD), lambda h, i: (2 + h, 1, 0, 0)),
        ],
        out_specs=[
            pl.BlockSpec((1, 2, bq, HEAD), lambda h, i: (h, 0, i, 0)),
            pl.BlockSpec((1, 2, bq), lambda h, i: (h, 0, i)),
        ],
        out_shape=[jax.ShapeDtypeStruct((2, 2, tokens, HEAD), jnp.float32), jax.ShapeDtypeStruct((2, 2, tokens), jnp.float32)],
        scratch_shapes=[pltpu.VMEM((1, 2 * bq), jnp.float32), pltpu.VMEM((HEAD + 8, 2 * bq), jnp.float32)],
        compiler_params=pltpu.CompilerParams(dimension_semantics=("arbitrary", "arbitrary"), vmem_limit_bytes=VMEM),
        cost_estimate=pl.CostEstimate(flops=8 * tokens * tokens * HEAD, transcendentals=2 * tokens * tokens, bytes_accessed=2 * made.size),
        name="attend_own",
    )(made, made, made)


def _cross(at_ref, q_ref, k_ref, v_ref, o_in, lse_in, o_ref, lse_ref, top_s, mix_s):
    carried = at_ref[1] == 1
    pieces = [(n, m) for n in range(2) for m in range(2)]
    for s, (n, m) in enumerate(pieces):
        cols = slice(s * STRIP, (s + 1) * STRIP)
        top_s[:, cols] = jnp.where(carried, jnp.maximum(lse_in[0, n, m : m + 1, :] * (1 / SCALE), NEG), NEG)
        mix_s[:HEAD, cols] = jnp.where(carried, o_in[0, n, m].T, 0.0)
        mix_s[HEAD:, cols] = jnp.full((8, STRIP), jnp.where(carried, 1.0, 0.0), jnp.float32)

    def block(j, _):
        here = pl.ds(pl.multiple_of(j * BK, BK), BK)
        strips = [(s * STRIP, q_ref[n, m], None) for s, (n, m) in enumerate(pieces)]
        _step(strips, k_ref[0, here, :], v_ref[0, here, :], top_s, mix_s)

    lax.fori_loop(0, k_ref.shape[1] // BK, block, None)
    for s, (n, m) in enumerate(pieces):
        out, lse = _finish(s * STRIP, top_s, mix_s)
        o_ref[n, m] = out.astype(o_ref.dtype)
        lse_ref[n, m : m + 1, :] = lse


def attend_cross(at, q, kv, own_o, own_lse, i):
    tokens = kv.shape[1]
    half = tokens // 2
    bq = half // CHUNKS
    whole = lambda n: pl.BlockSpec((1, tokens, HEAD), lambda g, at_ref: (n, 0, 0))
    return pl.pallas_call(
        _cross,
        grid_spec=pltpu.PrefetchScalarGridSpec(
            num_scalar_prefetch=1, grid=(1,),
            in_specs=[
                pl.BlockSpec((2, 2, bq, HEAD), lambda g, at_ref: (0, 0, i, 0)), whole(0), whole(1),
                pl.BlockSpec((1, 2, 2, bq, HEAD), lambda g, at_ref: (1, 0, 0, i, 0)),
                pl.BlockSpec((1, 2, 2, bq), lambda g, at_ref: (1, 0, 0, i)),
            ],
            out_specs=[
                pl.BlockSpec((2, 2, bq, HEAD), lambda g, at_ref: (0, 0, 0, 0)),
                pl.BlockSpec((2, 2, bq), lambda g, at_ref: (0, 0, 0)),
            ],
            scratch_shapes=[pltpu.VMEM((1, 4 * bq), jnp.float32), pltpu.VMEM((HEAD + 8, 4 * bq), jnp.float32)],
        ),
        out_shape=[jax.ShapeDtypeStruct((2, 2, bq, HEAD), jnp.bfloat16), jax.ShapeDtypeStruct((2, 2, bq), jnp.float32)],
        compiler_params=pltpu.CompilerParams(dimension_semantics=("arbitrary",), vmem_limit_bytes=VMEM),
        cost_estimate=pl.CostEstimate(flops=16 * bq * tokens * HEAD, transcendentals=4 * bq * tokens, bytes_accessed=2 * kv.size),
        name="attend_cross",
    )(at, q.reshape(2, 2, half, HEAD), kv, kv, own_o.reshape(2, 2, 2, half, HEAD), own_lse.reshape(2, 2, 2, half))


def _output(at_ref, own_ref, sib_ref, x_ref, w_own, w_sib, wx, wy, vx, vy, *rest):
    y_ref = rest[-1]
    chip, group = at_ref[1], at_ref[3]
    y = x_ref[...].astype(jnp.float32)
    for o_ref, w, from_x, from_y in ((own_ref, w_own, wx, wy), (sib_ref, w_sib, vx, vy)):
        for n in range(2):
            y += _dot(o_ref[chip, n], w[n * HEAD : (n + 1) * HEAD, :], 1, 0)
        y += _dot(o_ref[1 - chip, group], from_x[...], 1, 0)
        y += _dot(o_ref[1 - chip, 1 - group], from_y[...], 1, 0)
    y_ref[...] = y.astype(y_ref.dtype)


def output(at, own, sib, x, w_own, w_sib, wx, wy, vx, vy, i, done):
    rows, width = own.shape[2], x.shape[1]
    bn = 768
    part = pl.BlockSpec(own.shape, lambda j, at_ref: (0, 0, 0, 0))
    here = pl.BlockSpec((rows, bn), lambda j, at_ref: (i, j))
    specs = [part, part, here] + [pl.BlockSpec((w.shape[0], bn), lambda j, at_ref: (0, j)) for w in (w_own, w_sib, wx, wy, vx, vy)]
    given = [own, sib, x, w_own, w_sib, wx, wy, vx, vy]
    alias = {}
    if done is not None:
        given.append(done)
        specs.append(pl.BlockSpec(memory_space=pl.ANY))
        alias = {len(given): 0}
    return pl.pallas_call(
        _output,
        grid_spec=pltpu.PrefetchScalarGridSpec(num_scalar_prefetch=1, grid=(width // bn,), in_specs=specs, out_specs=here),
        out_shape=jax.ShapeDtypeStruct(x.shape, jnp.bfloat16),
        input_output_aliases=alias,
        compiler_params=pltpu.CompilerParams(dimension_semantics=("arbitrary",), vmem_limit_bytes=VMEM),
        cost_estimate=pl.CostEstimate(flops=2 * rows * 8 * HEAD * width, transcendentals=0, bytes_accessed=16 * HEAD * width),
        name="output",
    )(at, *given)


def normed(x, gain):
    wide = x.astype(jnp.float32)
    scale = lax.rsqrt(jnp.mean(wide * wide, -1, keepdims=True) + 1e-6)
    return (wide * scale * gain.astype(jnp.float32)).astype(jnp.bfloat16)


def tables(place):
    half = HEAD // 2
    angle = place.astype(jnp.float32)[:, None] * THETA ** (-jnp.arange(half, dtype=jnp.float32) / half)
    return jnp.cos(angle), jnp.sin(angle)


def solution(mesh):
    def step(x, gain, wq, wk, wv, wo):
        own = x.shape[0]
        rank, group = lax.axis_index("sp"), lax.axis_index("dp")
        chip, core = rank // 2, rank % 2

        def columns(n):
            cut = lambda w, at, width: lax.dynamic_slice_in_dim(w, at, width, axis=1)
            blocks = [cut(wq, 2 * HEAD * (2 * p + n), 2 * HEAD) for p in range(2)]
            blocks += [jnp.concatenate([cut(w, HEAD * (2 * p + n), HEAD) for w in (wk, wv)], axis=1) for p in range(2)]
            return jnp.stack(blocks)

        w_own = columns(core)
        w_sib = lax.ppermute(columns(1 - core), "sp", SIBLING)
        w_half = jnp.where(group == core, w_own, w_sib)
        pick = lambda n, which: jnp.where(which == 0, ORDER[0][n], ORDER[1][n])
        wx, wy = [], []
        for n in range(4):
            wx.append(lax.ppermute(lax.dynamic_index_in_dim(w_half, pick(n, 1 - chip), keepdims=False), "sp", ACROSS))
            wy.append(lax.ppermute(wx[n], "dp", GROUPS))

        a_own = normed(x, gain)
        a_sib = lax.ppermute(a_own, "sp", SIBLING)
        cos, sin = tables(chip * 2 * own + jnp.arange(2 * own))

        made, sent = None, None
        for n in range(4):
            at = jnp.stack([pick(n, chip), chip, core, group]).astype(jnp.int32)
            got = project(at, a_own, a_sib, w_own, w_sib, wx[n], wy[n], cos, sin, made)
            made = got[0]
            if n == 0:
                sent = got[1]
        came = lax.ppermute(sent, "sp", ACROSS)

        wo_here, _ = lax.optimization_barrier((wo, sent))
        wo_half = lax.dynamic_slice_in_dim(wo_here, group * HEAD, HEAD, axis=0)
        ox = lax.ppermute(wo_half, "sp", ACROSS)
        oy = lax.ppermute(ox, "dp", GROUPS)
        wo_sib, ox_sib, oy_sib = (lax.ppermute(w, "sp", SIBLING) for w in (wo, ox, oy))

        own_o, own_lse = attend_own(made)
        q_cross = jnp.where(chip == 0, came, made[1])
        kv_cross = jnp.where(chip == 0, made[2], came)

        half = own // CHUNKS
        y = None
        for i in range(CHUNKS):
            o, lse = attend_cross(at, q_cross, kv_cross, own_o, own_lse, i)
            far, far_lse = lax.ppermute(o, "sp", BACK), lax.ppermute(lse, "sp", BACK)
            cut = lambda t: lax.slice_in_dim(t.reshape(2, 2, 2, own, *t.shape[3:]), i * half, (i + 1) * half, axis=3)
            mine, mine_lse = cut(own_o), cut(own_lse)
            far_lse = jnp.where(chip == 0, NEG, far_lse)
            top = jnp.maximum(mine_lse[0], far_lse)
            wa, wb = jnp.exp(mine_lse[0] - top), jnp.exp(far_lse - top)
            low = (mine[0] * wa[..., None] + far.astype(jnp.float32) * wb[..., None]) / (wa + wb)[..., None]
            high = jnp.where(chip == 0, mine[1], o.astype(jnp.float32))
            both = jnp.stack([low, high]).astype(jnp.bfloat16)
            keep = lax.dynamic_index_in_dim(both, core, axis=2, keepdims=False)
            give = lax.dynamic_index_in_dim(both, 1 - core, axis=2, keepdims=False)
            take = lax.ppermute(give, "sp", SIBLING)
            y = output(at, keep, take, x, wo, wo_sib, ox, oy, ox_sib, oy_sib, i, y)
        return y

    tokens, whole = P(("dp", "sp"), None), P("sp", None)
    return jax.shard_map(
        step,
        mesh=mesh,
        in_specs=(tokens, P(None), whole, whole, whole, whole),
        out_specs=tokens,
        check_vma=False,
    )
```

```python
import functools

import jax
import jax.numpy as jnp
from jax import lax
from jax.experimental import pallas as pl
from jax.experimental.pallas import tpu as pltpu
from jax.sharding import PartitionSpec as P


NEG = -1e30
HIDDEN = 2 * NEG
LOG2E = 1.4426950408889634
VMEM = 56 * 2**20
HEAD = 256
THETA = 10000
SCALE = HEAD**-0.5
E = SCALE * LOG2E
STRIP = 512
BK = 512
CHUNKS = 4


SIBLING = [(0, 1), (1, 0), (2, 3), (3, 2)]
ACROSS = [(0, 2), (2, 0), (1, 3), (3, 1)]
BACK = [(0, 2), (1, 3)]
GROUPS = [(0, 1), (1, 0)]
ORDER = ((3, 2, 0, 1), (0, 1, 2, 3))


def _dot(a, b, ca, cb):
    return lax.dot_general(a, b, (((ca,), (cb,)), ((), ())), preferred_element_type=jnp.float32)


def _project(at_ref, a0_ref, a1_ref, own_ref, sib_ref, wx_ref, wy_ref, cos_ref, sin_ref, *rest, first):
    out_ref, sent_ref, w_s = rest if first else (rest[1], None, rest[2])
    slot, chip, core, group = at_ref[0], at_ref[1], at_ref[2], at_ref[3]
    i = pl.program_id(0)
    rows = own_ref.shape[1]

    @pl.when(i == 0)
    def _():
        here, there = 2 * rows * chip, 2 * rows * (1 - chip)
        for at, ref in ((here + rows * core, own_ref), (here + rows * (1 - core), sib_ref)):
            w_s[pl.ds(pl.multiple_of(at, 64), rows), :] = ref[0]
        for at, ref in ((there + rows * group, wx_ref), (there + rows * (1 - group), wy_ref)):
            w_s[pl.ds(pl.multiple_of(at, 64), rows), :] = ref[...]

    def part(a_ref):
        t = _dot(a_ref[...], w_s[...], 1, 0).astype(jnp.bfloat16).astype(jnp.float32)
        cos, sin = cos_ref[...], sin_ref[...]
        half = HEAD // 2
        for n in range(2):
            p, q = t[:, n * HEAD : n * HEAD + half], t[:, n * HEAD + half : (n + 1) * HEAD]
            u, v = p * cos - q * sin, q * cos + p * sin
            if n == 1:
                u, v = jnp.where(slot < 2, u, p), jnp.where(slot < 2, v, q)
            got = jnp.concatenate([u, v], axis=1).astype(jnp.bfloat16)
            out_ref[0, n] = got
            if sent_ref is not None:
                sent_ref[n] = got

    @pl.when(i < pl.num_programs(0) // 2)
    def _():
        part(a0_ref)

    @pl.when(i >= pl.num_programs(0) // 2)
    def _():
        part(a1_ref)


def project(at, a_own, a_sib, w_own, w_sib, wx, wy, cos, sin, done):
    tokens, depth = a_own.shape
    rows, width = wx.shape
    bm = 512
    n = tokens // bm
    first = done is None

    def place(i, at_ref):
        return jnp.where(i < n, at_ref[2] * n + i, (1 - at_ref[2]) * n + i - n)

    weights = pl.BlockSpec((1, rows, width), lambda i, at_ref: (at_ref[0], 0, 0))
    fetched = pl.BlockSpec((rows, width), lambda i, at_ref: (0, 0))
    table = pl.BlockSpec((bm, HEAD // 2), lambda i, at_ref: (place(i, at_ref), 0))
    specs = [
        pl.BlockSpec((bm, depth), lambda i, at_ref: (jnp.minimum(i, n - 1), 0)),
        pl.BlockSpec((bm, depth), lambda i, at_ref: (jnp.maximum(i - n, 0), 0)),
        weights, weights, fetched, fetched, table, table,
    ]
    given = [a_own, a_sib, w_own, w_sib, wx, wy, cos, sin]
    out_shape = [jax.ShapeDtypeStruct((4, 2, 2 * tokens, HEAD), jnp.bfloat16)]
    out_specs = [pl.BlockSpec((1, 2, bm, HEAD), lambda i, at_ref: (at_ref[0], 0, place(i, at_ref), 0))]
    alias = {}
    if first:
        out_shape.append(jax.ShapeDtypeStruct((2, 2 * tokens, HEAD), jnp.bfloat16))
        out_specs.append(pl.BlockSpec((2, bm, HEAD), lambda i, at_ref: (0, place(i, at_ref), 0)))
    else:
        given.append(done)
        specs.append(pl.BlockSpec(memory_space=pl.ANY))
        alias = {len(given): 0}
    return pl.pallas_call(
        functools.partial(_project, first=first),
        grid_spec=pltpu.PrefetchScalarGridSpec(
            num_scalar_prefetch=1, grid=(2 * n,), in_specs=specs, out_specs=out_specs,
            scratch_shapes=[pltpu.VMEM((4 * rows, width), jnp.bfloat16)],
        ),
        out_shape=out_shape,
        input_output_aliases=alias,
        compiler_params=pltpu.CompilerParams(dimension_semantics=("arbitrary",), vmem_limit_bytes=VMEM),
        cost_estimate=pl.CostEstimate(flops=4 * tokens * depth * width, transcendentals=0, bytes_accessed=4 * tokens * depth),
        name="project",
    )(at, *given)


def _step(strips, k, v, top_s, mix_s):
    scores = [_dot(k, q, 1, 1) for _, q, _ in strips]
    weights, keeps = [], []
    for (at, _, ok), s in zip(strips, scores):
        if ok is not None:
            s = jnp.where(ok, s, HIDDEN)
        cols = slice(at, at + STRIP)
        old = top_s[:, cols]
        top = jnp.maximum(old, s.max(axis=0, keepdims=True))
        top_s[:, cols] = top
        weights.append(jnp.exp2((s - top) * E).astype(jnp.bfloat16))
        keeps.append(jnp.exp2((old - top) * E))
    values = jnp.concatenate([v.T, jnp.ones((8, BK), jnp.bfloat16)], axis=0)
    for (at, _, _), p, keep in zip(strips, weights, keeps):
        cols = slice(at, at + STRIP)
        mix_s[:, cols] = mix_s[:, cols] * keep + _dot(values, p, 1, 0)


def _finish(at, top_s, mix_s):
    cols = slice(at, at + STRIP)
    total = mix_s[HEAD : HEAD + 1, cols]
    return (mix_s[:HEAD, cols] * (1 / total)).T, top_s[:, cols] * SCALE + jnp.log(total)


def _own(q_ref, k_ref, v_ref, o_ref, lse_ref, top_s, mix_s):
    bq = q_ref.shape[2]
    iq = pl.program_id(1)
    per = bq // STRIP
    top_s[...] = jnp.full(top_s.shape, NEG, jnp.float32)
    mix_s[...] = jnp.zeros(mix_s.shape, jnp.float32)

    def block(j, least):
        here = pl.ds(pl.multiple_of(j * BK, BK), BK)
        ok = None
        if least is not None:
            ok = lax.broadcasted_iota(jnp.int32, (BK, STRIP), 1) >= lax.broadcasted_iota(jnp.int32, (BK, STRIP), 0)
        strips = []
        for n in range(2):
            for s in range(least or 0, per):
                q = q_ref[0, n, s * STRIP : (s + 1) * STRIP, :]
                strips.append((n * bq + s * STRIP, q, ok if s == least else None))
        _step(strips, k_ref[0, 0, here, :], v_ref[0, 0, here, :], top_s, mix_s)

    lax.fori_loop(0, iq * per, lambda j, _: block(j, None), None)
    for s in range(per):
        block(iq * per + s, s)
    for n in range(2):
        for s in range(per):
            out, lse = _finish(n * bq + s * STRIP, top_s, mix_s)
            o_ref[0, n, s * STRIP : (s + 1) * STRIP, :] = out
            lse_ref[0, n : n + 1, s * STRIP : (s + 1) * STRIP] = lse


def attend_own(made):
    tokens = made.shape[2]
    bq = 2048
    return pl.pallas_call(
        _own,
        grid=(2, tokens // bq),
        in_specs=[
            pl.BlockSpec((1, 2, bq, HEAD), lambda h, i: (h, 0, i, 0)),
            pl.BlockSpec((1, 1, tokens, HEAD), lambda h, i: (2 + h, 0, 0, 0)),
            pl.BlockSpec((1, 1, tokens, HEAD), lambda h, i: (2 + h, 1, 0, 0)),
        ],
        out_specs=[
            pl.BlockSpec((1, 2, bq, HEAD), lambda h, i: (h, 0, i, 0)),
            pl.BlockSpec((1, 2, bq), lambda h, i: (h, 0, i)),
        ],
        out_shape=[jax.ShapeDtypeStruct((2, 2, tokens, HEAD), jnp.float32), jax.ShapeDtypeStruct((2, 2, tokens), jnp.float32)],
        scratch_shapes=[pltpu.VMEM((1, 2 * bq), jnp.float32), pltpu.VMEM((HEAD + 8, 2 * bq), jnp.float32)],
        compiler_params=pltpu.CompilerParams(dimension_semantics=("arbitrary", "arbitrary"), vmem_limit_bytes=VMEM),
        cost_estimate=pl.CostEstimate(flops=8 * tokens * tokens * HEAD, transcendentals=2 * tokens * tokens, bytes_accessed=2 * made.size),
        name="attend_own",
    )(made, made, made)


def _cross(at_ref, q_ref, k_ref, v_ref, o_in, lse_in, o_ref, lse_ref, top_s, mix_s):
    carried = at_ref[1] == 1
    pieces = [(n, m) for n in range(2) for m in range(2)]
    for s, (n, m) in enumerate(pieces):
        cols = slice(s * STRIP, (s + 1) * STRIP)
        top_s[:, cols] = jnp.where(carried, jnp.maximum(lse_in[0, n, m : m + 1, :] * (1 / SCALE), NEG), NEG)
        mix_s[:HEAD, cols] = jnp.where(carried, o_in[0, n, m].T, 0.0)
        mix_s[HEAD:, cols] = jnp.full((8, STRIP), jnp.where(carried, 1.0, 0.0), jnp.float32)

    def block(j, _):
        here = pl.ds(pl.multiple_of(j * BK, BK), BK)
        strips = [(s * STRIP, q_ref[n, m], None) for s, (n, m) in enumerate(pieces)]
        _step(strips, k_ref[0, here, :], v_ref[0, here, :], top_s, mix_s)

    lax.fori_loop(0, k_ref.shape[1] // BK, block, None)
    for s, (n, m) in enumerate(pieces):
        out, lse = _finish(s * STRIP, top_s, mix_s)
        o_ref[n, m] = out.astype(o_ref.dtype)
        lse_ref[n, m : m + 1, :] = lse


def attend_cross(at, q, kv, own_o, own_lse, i):
    tokens = kv.shape[1]
    half = tokens // 2
    bq = half // CHUNKS
    whole = lambda n: pl.BlockSpec((1, tokens, HEAD), lambda g, at_ref: (n, 0, 0))
    return pl.pallas_call(
        _cross,
        grid_spec=pltpu.PrefetchScalarGridSpec(
            num_scalar_prefetch=1, grid=(1,),
            in_specs=[
                pl.BlockSpec((2, 2, bq, HEAD), lambda g, at_ref: (0, 0, i, 0)), whole(0), whole(1),
                pl.BlockSpec((1, 2, 2, bq, HEAD), lambda g, at_ref: (1, 0, 0, i, 0)),
                pl.BlockSpec((1, 2, 2, bq), lambda g, at_ref: (1, 0, 0, i)),
            ],
            out_specs=[
                pl.BlockSpec((2, 2, bq, HEAD), lambda g, at_ref: (0, 0, 0, 0)),
                pl.BlockSpec((2, 2, bq), lambda g, at_ref: (0, 0, 0)),
            ],
            scratch_shapes=[pltpu.VMEM((1, 4 * bq), jnp.float32), pltpu.VMEM((HEAD + 8, 4 * bq), jnp.float32)],
        ),
        out_shape=[jax.ShapeDtypeStruct((2, 2, bq, HEAD), jnp.bfloat16), jax.ShapeDtypeStruct((2, 2, bq), jnp.float32)],
        compiler_params=pltpu.CompilerParams(dimension_semantics=("arbitrary",), vmem_limit_bytes=VMEM),
        cost_estimate=pl.CostEstimate(flops=16 * bq * tokens * HEAD, transcendentals=4 * bq * tokens, bytes_accessed=2 * kv.size),
        name="attend_cross",
    )(at, q.reshape(2, 2, half, HEAD), kv, kv, own_o.reshape(2, 2, 2, half, HEAD), own_lse.reshape(2, 2, 2, half))


def _merge(at_ref, own_ref, lse_ref, far_ref, far_lse_ref, o_ref, keep_ref, give_ref):
    chip, core = at_ref[1], at_ref[2]
    for to_ref, m in ((keep_ref, core), (give_ref, 1 - core)):
        lse = lse_ref[0, 0, pl.ds(m, 1), :]
        far_lse = jnp.where(chip == 0, NEG, far_lse_ref[0, pl.ds(m, 1), :])
        top = jnp.maximum(lse, far_lse)
        wa, wb = jnp.exp(lse - top), jnp.exp(far_lse - top)
        total = 1 / (wa + wb)
        tall = lambda row: jnp.broadcast_to(row, (128, row.shape[1])).T
        wa, wb = tall(wa * total), tall(wb * total)
        for at in (0, 128):
            cols = slice(at, at + 128)
            to_ref[0, 0, :, cols] = (own_ref[0, 0, m, :, cols] * wa + far_ref[0, m, :, cols].astype(jnp.float32) * wb).astype(jnp.bfloat16)
        to_ref[1, 0] = jnp.where(chip == 0, own_ref[1, 0, m].astype(jnp.bfloat16), o_ref[0, m])


def merge(at, own_o, own_lse, far, far_lse, o, i):
    half, bq = own_o.shape[2] // 2, o.shape[2]
    part = pl.BlockSpec((1, 2, bq, HEAD), lambda n, at_ref: (n, 0, 0, 0))
    result = pl.BlockSpec((2, 1, bq, HEAD), lambda n, at_ref: (0, n, 0, 0))
    return pl.pallas_call(
        _merge,
        grid_spec=pltpu.PrefetchScalarGridSpec(
            num_scalar_prefetch=1, grid=(2,),
            in_specs=[
                pl.BlockSpec((2, 1, 2, bq, HEAD), lambda n, at_ref: (0, n, 0, i, 0)),
                pl.BlockSpec((2, 1, 2, bq), lambda n, at_ref: (0, n, 0, i)),
                part, pl.BlockSpec((1, 2, bq), lambda n, at_ref: (n, 0, 0)), part,
            ],
            out_specs=[result, result],
        ),
        out_shape=[jax.ShapeDtypeStruct((2, 2, bq, HEAD), jnp.bfloat16)] * 2,
        compiler_params=pltpu.CompilerParams(dimension_semantics=("arbitrary",), vmem_limit_bytes=VMEM),
        cost_estimate=pl.CostEstimate(flops=64 * bq * HEAD, transcendentals=0, bytes_accessed=64 * bq * HEAD),
        name="merge",
    )(at, own_o.reshape(2, 2, 2, half, HEAD), own_lse.reshape(2, 2, 2, half), far, far_lse, o)


def _output(at_ref, own_ref, sib_ref, x_ref, w_own, w_sib, wx, wy, vx, vy, *rest):
    y_ref = rest[-1]
    chip, group = at_ref[1], at_ref[3]
    y = x_ref[...].astype(jnp.float32)
    for o_ref, w, from_x, from_y in ((own_ref, w_own, wx, wy), (sib_ref, w_sib, vx, vy)):
        for n in range(2):
            y += _dot(o_ref[chip, n], w[n * HEAD : (n + 1) * HEAD, :], 1, 0)
        y += _dot(o_ref[1 - chip, group], from_x[...], 1, 0)
        y += _dot(o_ref[1 - chip, 1 - group], from_y[...], 1, 0)
    y_ref[...] = y.astype(y_ref.dtype)


def output(at, own, sib, x, w_own, w_sib, wx, wy, vx, vy, i, done):
    rows, width = own.shape[2], x.shape[1]
    bn = 768
    part = pl.BlockSpec(own.shape, lambda j, at_ref: (0, 0, 0, 0))
    here = pl.BlockSpec((rows, bn), lambda j, at_ref: (i, j))
    specs = [part, part, here] + [pl.BlockSpec((w.shape[0], bn), lambda j, at_ref: (0, j)) for w in (w_own, w_sib, wx, wy, vx, vy)]
    given = [own, sib, x, w_own, w_sib, wx, wy, vx, vy]
    alias = {}
    if done is not None:
        given.append(done)
        specs.append(pl.BlockSpec(memory_space=pl.ANY))
        alias = {len(given): 0}
    return pl.pallas_call(
        _output,
        grid_spec=pltpu.PrefetchScalarGridSpec(num_scalar_prefetch=1, grid=(width // bn,), in_specs=specs, out_specs=here),
        out_shape=jax.ShapeDtypeStruct(x.shape, jnp.bfloat16),
        input_output_aliases=alias,
        compiler_params=pltpu.CompilerParams(dimension_semantics=("arbitrary",), vmem_limit_bytes=VMEM),
        cost_estimate=pl.CostEstimate(flops=2 * rows * 8 * HEAD * width, transcendentals=0, bytes_accessed=16 * HEAD * width),
        name="output",
    )(at, *given)


def normed(x, gain):
    wide = x.astype(jnp.float32)
    scale = lax.rsqrt(jnp.mean(wide * wide, -1, keepdims=True) + 1e-6)
    return (wide * scale * gain.astype(jnp.float32)).astype(jnp.bfloat16)


def tables(place):
    half = HEAD // 2
    angle = place.astype(jnp.float32)[:, None] * THETA ** (-jnp.arange(half, dtype=jnp.float32) / half)
    return jnp.cos(angle), jnp.sin(angle)


def solution(mesh):
    def step(x, gain, wq, wk, wv, wo):
        own = x.shape[0]
        rank, group = lax.axis_index("sp"), lax.axis_index("dp")
        chip, core = rank // 2, rank % 2

        def columns(n):
            cut = lambda w, at, width: lax.dynamic_slice_in_dim(w, at, width, axis=1)
            blocks = [cut(wq, 2 * HEAD * (2 * p + n), 2 * HEAD) for p in range(2)]
            blocks += [jnp.concatenate([cut(w, HEAD * (2 * p + n), HEAD) for w in (wk, wv)], axis=1) for p in range(2)]
            return jnp.stack(blocks)

        w_own, w_give = columns(core), columns(1 - core)
        w_sib = lax.ppermute(w_give, "sp", SIBLING)
        x_late, _ = lax.optimization_barrier((x, w_give))
        w_half = jnp.where(group == core, w_own, w_sib)
        pick = lambda n, which: jnp.where(which == 0, ORDER[0][n], ORDER[1][n])
        wx, wy = [], []
        for n in range(4):
            wx.append(lax.ppermute(lax.dynamic_index_in_dim(w_half, pick(n, 1 - chip), keepdims=False), "sp", ACROSS))
            wy.append(lax.ppermute(wx[n], "dp", GROUPS))

        a_own = normed(x_late, gain)
        a_sib = lax.ppermute(a_own, "sp", SIBLING)
        cos, sin = tables(chip * 2 * own + jnp.arange(2 * own))

        made, sent = None, None
        for n in range(4):
            at = jnp.stack([pick(n, chip), chip, core, group]).astype(jnp.int32)
            got = project(at, a_own, a_sib, w_own, w_sib, wx[n], wy[n], cos, sin, made)
            made = got[0]
            if n == 0:
                sent = got[1]
        came = lax.ppermute(sent, "sp", ACROSS)

        wo_here, _ = lax.optimization_barrier((wo, sent))
        wo_half = lax.dynamic_slice_in_dim(wo_here, group * HEAD, HEAD, axis=0)
        ox = lax.ppermute(wo_half, "sp", ACROSS)
        oy = lax.ppermute(ox, "dp", GROUPS)
        wo_sib, ox_sib, oy_sib = (lax.ppermute(w, "sp", SIBLING) for w in (wo_here, ox, oy))

        own_o, own_lse = attend_own(made)
        q_cross = jnp.where(chip == 0, came, made[1])
        kv_cross = jnp.where(chip == 0, made[2], came)

        y = None
        for i in range(CHUNKS):
            o, lse = attend_cross(at, q_cross, kv_cross, own_o, own_lse, i)
            far, far_lse = lax.ppermute(o, "sp", BACK), lax.ppermute(lse, "sp", BACK)
            keep, give = merge(at, own_o, own_lse, far, far_lse, o, i)
            take = lax.ppermute(give, "sp", SIBLING)
            y = output(at, keep, take, x, wo, wo_sib, ox, oy, ox_sib, oy_sib, i, y)
        return y

    tokens, whole = P(("dp", "sp"), None), P("sp", None)
    return jax.shard_map(
        step,
        mesh=mesh,
        in_specs=(tokens, P(None), whole, whole, whole, whole),
        out_specs=tokens,
        check_vma=False,
    )
```

```python
import functools

import jax
import jax.numpy as jnp
from jax import lax
from jax.experimental import pallas as pl
from jax.experimental.pallas import tpu as pltpu
from jax.sharding import PartitionSpec as P


NEG = -1e30
HIDDEN = 2 * NEG
LOG2E = 1.4426950408889634
VMEM = 56 * 2**20
HEAD = 256
THETA = 10000
SCALE = HEAD**-0.5
E = SCALE * LOG2E
STRIP = 512
KEYS = 2048
CHUNKS = 4


SIBLING = [(0, 1), (1, 0), (2, 3), (3, 2)]
ACROSS = [(0, 2), (2, 0), (1, 3), (3, 1)]
BACK = [(0, 2), (1, 3)]
GROUPS = [(0, 1), (1, 0)]
ORDER = ((3, 1, 0, 2), (0, 2, 1, 3))
OTHERS, CHIP, CORE, GROUP = 4, 8, 9, 10


def _dot(a, b, ca, cb):
    return lax.dot_general(a, b, (((ca,), (cb,)), ((), ())), preferred_element_type=jnp.float32)


def _share(at_ref, *refs):
    for q_ref, k_ref, v_ref, to_ref in (refs[:3] + refs[6:7], refs[3:6] + refs[7:8]):
        to_ref[0] = q_ref[...]
        to_ref[1, :, :HEAD] = k_ref[...]
        to_ref[1, :, HEAD:] = v_ref[...]


def share(at, wq, wk, wv):
    rows = wq.shape[0]
    specs = []
    for mine in (True, False):
        at_block = lambda p, at_ref, mine=mine: (0, 2 * p + (at_ref[CORE] if mine else 1 - at_ref[CORE]))
        specs += [pl.BlockSpec((rows, 2 * HEAD), at_block), pl.BlockSpec((rows, HEAD), at_block), pl.BlockSpec((rows, HEAD), at_block)]
    out = pl.BlockSpec((2, rows, 2 * HEAD), lambda p, at_ref: (p, 0, 0))
    return pl.pallas_call(
        _share,
        grid_spec=pltpu.PrefetchScalarGridSpec(num_scalar_prefetch=1, grid=(2,), in_specs=specs, out_specs=[out, out]),
        out_shape=[jax.ShapeDtypeStruct((4, rows, 2 * HEAD), jnp.bfloat16)] * 2,
        compiler_params=pltpu.CompilerParams(dimension_semantics=("arbitrary",), vmem_limit_bytes=VMEM),
        cost_estimate=pl.CostEstimate(flops=1000, transcendentals=0, bytes_accessed=4 * wq.size * 2),
        name="share",
    )(at, wq, wk, wv, wq, wk, wv)


def _leave(at_ref, own_ref, sib_ref, *to_refs):
    for n, to_ref in enumerate(to_refs):
        slot = at_ref[OTHERS + n]

        @pl.when(at_ref[GROUP] == at_ref[CORE])
        def _():
            to_ref[...] = own_ref[slot]

        @pl.when(at_ref[GROUP] != at_ref[CORE])
        def _():
            to_ref[...] = sib_ref[slot]


def leave(at, w_own, w_sib):
    whole = pl.BlockSpec(w_own.shape, lambda i, at_ref: (0, 0, 0))
    out = pl.BlockSpec(w_own.shape[1:], lambda i, at_ref: (0, 0))
    return pl.pallas_call(
        _leave,
        grid_spec=pltpu.PrefetchScalarGridSpec(num_scalar_prefetch=1, grid=(1,), in_specs=[whole, whole], out_specs=[out] * 4),
        out_shape=[jax.ShapeDtypeStruct(w_own.shape[1:], jnp.bfloat16)] * 4,
        compiler_params=pltpu.CompilerParams(dimension_semantics=("arbitrary",), vmem_limit_bytes=VMEM),
        cost_estimate=pl.CostEstimate(flops=1000, transcendentals=0, bytes_accessed=6 * w_own.size),
        name="leave",
    )(at, w_own, w_sib)


def _normed(x_ref, gain_ref, a_ref):
    wide = x_ref[...].astype(jnp.float32)
    scale = lax.rsqrt(jnp.mean(wide * wide, -1, keepdims=True) + 1e-6)
    a_ref[...] = (wide * scale * gain_ref[...].astype(jnp.float32)).astype(jnp.bfloat16)


def normed(x, gain):
    rows, depth = x.shape
    block = pl.BlockSpec((256, depth), lambda i: (i, 0))
    return pl.pallas_call(
        _normed,
        grid=(rows // 256,),
        in_specs=[block, pl.BlockSpec((1, depth), lambda i: (0, 0))],
        out_specs=block,
        out_shape=jax.ShapeDtypeStruct(x.shape, jnp.bfloat16),
        compiler_params=pltpu.CompilerParams(dimension_semantics=("arbitrary",), vmem_limit_bytes=VMEM),
        cost_estimate=pl.CostEstimate(flops=8 * x.size, transcendentals=0, bytes_accessed=4 * x.size),
        name="normed",
    )(x, gain[None])


def _project(at_ref, a0_ref, a1_ref, own_ref, sib_ref, wx_ref, wy_ref, cos_ref, sin_ref, *rest, which):
    out_ref, sent_ref, w_s = rest if which == 0 else (rest[1], None, rest[2])
    slot, chip, core, group = at_ref[which], at_ref[CHIP], at_ref[CORE], at_ref[GROUP]
    i = pl.program_id(0)
    rows = own_ref.shape[1]

    @pl.when(i == 0)
    def _():
        here, there = 2 * rows * chip, 2 * rows * (1 - chip)
        for at, ref in ((here + rows * core, own_ref), (here + rows * (1 - core), sib_ref)):
            w_s[pl.ds(pl.multiple_of(at, 64), rows), :] = ref[0]
        for at, ref in ((there + rows * group, wx_ref), (there + rows * (1 - group), wy_ref)):
            w_s[pl.ds(pl.multiple_of(at, 64), rows), :] = ref[...]

    def part(a_ref):
        t = _dot(a_ref[...], w_s[...], 1, 0).astype(jnp.bfloat16).astype(jnp.float32)
        cos, sin = cos_ref[...], sin_ref[...]
        half = HEAD // 2
        for n in range(2):
            p, q = t[:, n * HEAD : n * HEAD + half], t[:, n * HEAD + half : (n + 1) * HEAD]
            u, v = p * cos - q * sin, q * cos + p * sin
            if n == 1:
                u, v = jnp.where(slot % 2 == 0, u, p), jnp.where(slot % 2 == 0, v, q)
            got = jnp.concatenate([u, v], axis=1).astype(jnp.bfloat16)
            out_ref[0, n] = got
            if sent_ref is not None:
                sent_ref[n] = got

    @pl.when(i < pl.num_programs(0) // 2)
    def _():
        part(a0_ref)

    @pl.when(i >= pl.num_programs(0) // 2)
    def _():
        part(a1_ref)


def project(at, a_own, a_sib, w_own, w_sib, wx, wy, cos, sin, which, done):
    tokens, depth = a_own.shape
    rows, width = wx.shape
    bm = 512
    n = tokens // bm
    first = which == 0

    def place(i, at_ref):
        return jnp.where(i < n, at_ref[CORE] * n + i, (1 - at_ref[CORE]) * n + i - n)

    weights = pl.BlockSpec((1, rows, width), lambda i, at_ref: (at_ref[which], 0, 0))
    fetched = pl.BlockSpec((rows, width), lambda i, at_ref: (0, 0))
    table = pl.BlockSpec((bm, HEAD // 2), lambda i, at_ref: (place(i, at_ref), 0))
    specs = [
        pl.BlockSpec((bm, depth), lambda i, at_ref: (jnp.minimum(i, n - 1), 0)),
        pl.BlockSpec((bm, depth), lambda i, at_ref: (jnp.maximum(i - n, 0), 0)),
        weights, weights, fetched, fetched, table, table,
    ]
    given = [a_own, a_sib, w_own, w_sib, wx, wy, cos, sin]
    out_shape = [jax.ShapeDtypeStruct((4, 2, 2 * tokens, HEAD), jnp.bfloat16)]
    out_specs = [pl.BlockSpec((1, 2, bm, HEAD), lambda i, at_ref: (at_ref[which], 0, place(i, at_ref), 0))]
    alias = {}
    if first:
        out_shape.append(jax.ShapeDtypeStruct((2, 2 * tokens, HEAD), jnp.bfloat16))
        out_specs.append(pl.BlockSpec((2, bm, HEAD), lambda i, at_ref: (0, place(i, at_ref), 0)))
    else:
        given.append(done)
        specs.append(pl.BlockSpec(memory_space=pl.ANY))
        alias = {len(given): 0}
    return pl.pallas_call(
        functools.partial(_project, which=which),
        grid_spec=pltpu.PrefetchScalarGridSpec(
            num_scalar_prefetch=1, grid=(2 * n,), in_specs=specs, out_specs=out_specs,
            scratch_shapes=[pltpu.VMEM((4 * rows, width), jnp.bfloat16)],
        ),
        out_shape=out_shape,
        input_output_aliases=alias,
        compiler_params=pltpu.CompilerParams(dimension_semantics=("arbitrary",), vmem_limit_bytes=VMEM),
        cost_estimate=pl.CostEstimate(flops=4 * tokens * depth * width, transcendentals=0, bytes_accessed=4 * tokens * depth),
        name="project",
    )(at, *given)


def _block(strips, k, v, top_s, mix_s):
    values = jnp.concatenate([v.T, jnp.ones((8, v.shape[0]), jnp.bfloat16)], axis=0)
    score = lambda strip: _dot(k[: strip[2]], strip[1], 1, 1)
    coming = score(strips[0])
    for n, (at, _, keys, ok) in enumerate(strips):
        s = coming
        if n + 1 < len(strips):
            coming = score(strips[n + 1])
        if ok is not None:
            last = jnp.where(ok, s[keys - STRIP :], HIDDEN)
            s = last if keys == STRIP else jnp.concatenate([s[: keys - STRIP], last], axis=0)
        cols = slice(at, at + STRIP)
        old = top_s[:, cols]
        top = jnp.maximum(old, s.max(axis=0, keepdims=True))
        top_s[:, cols] = top
        p = jnp.exp2((s - top) * E).astype(jnp.bfloat16)
        mix_s[:, cols] = mix_s[:, cols] * jnp.exp2((old - top) * E) + _dot(values[:, :keys], p, 1, 0)


def _own(q_ref, k_ref, v_ref, o_ref, lse_ref, top_s, mix_s):
    bq = q_ref.shape[2]
    iq = pl.program_id(1)
    top_s[...] = jnp.full(top_s.shape, NEG, jnp.float32)
    mix_s[...] = jnp.zeros(mix_s.shape, jnp.float32)
    places = [(n, s) for n in range(2) for s in range(0, bq, STRIP)]

    def block(j, diagonal):
        here = pl.ds(pl.multiple_of(j * bq, bq), bq)
        ok = None
        if diagonal:
            ok = lax.broadcasted_iota(jnp.int32, (STRIP, STRIP), 1) >= lax.broadcasted_iota(jnp.int32, (STRIP, STRIP), 0)
        strips = [(n * bq + s, q_ref[0, n, s : s + STRIP, :], s + STRIP if diagonal else bq, ok) for n, s in places]
        _block(strips, k_ref[0, 0, here, :], v_ref[0, 0, here, :], top_s, mix_s)

    lax.fori_loop(0, iq, lambda j, _: block(j, False), None)
    block(iq, True)
    for n, s in places:
        cols = slice(n * bq + s, n * bq + s + STRIP)
        total = mix_s[HEAD : HEAD + 1, cols]
        o_ref[0, n, s : s + STRIP, :] = (mix_s[:HEAD, cols] * (1 / total)).T
        lse_ref[0, n : n + 1, s : s + STRIP] = top_s[:, cols] * SCALE + jnp.log(total)


def attend_own(made):
    tokens = made.shape[2]
    bq = KEYS
    return pl.pallas_call(
        _own,
        grid=(2, tokens // bq),
        in_specs=[
            pl.BlockSpec((1, 2, bq, HEAD), lambda h, i: (2 * h, 0, i, 0)),
            pl.BlockSpec((1, 1, tokens, HEAD), lambda h, i: (2 * h + 1, 0, 0, 0)),
            pl.BlockSpec((1, 1, tokens, HEAD), lambda h, i: (2 * h + 1, 1, 0, 0)),
        ],
        out_specs=[
            pl.BlockSpec((1, 2, bq, HEAD), lambda h, i: (h, 0, i, 0)),
            pl.BlockSpec((1, 2, bq), lambda h, i: (h, 0, i)),
        ],
        out_shape=[jax.ShapeDtypeStruct((2, 2, tokens, HEAD), jnp.float32), jax.ShapeDtypeStruct((2, 2, tokens), jnp.float32)],
        scratch_shapes=[pltpu.VMEM((1, 2 * bq), jnp.float32), pltpu.VMEM((HEAD + 8, 2 * bq), jnp.float32)],
        compiler_params=pltpu.CompilerParams(dimension_semantics=("arbitrary", "arbitrary"), vmem_limit_bytes=VMEM),
        cost_estimate=pl.CostEstimate(flops=8 * tokens * tokens * HEAD, transcendentals=2 * tokens * tokens, bytes_accessed=2 * made.size),
        name="attend_own",
    )(made, made, made)


def _cross(at_ref, came_ref, made_ref, own_ref, lse_in, o_ref, lse_ref, q_s, k_s, v_s, in_s, top_s, mix_s, sem, *, chunk):
    bq = o_ref.shape[2]
    tokens = k_s.shape[0]
    rows = pl.ds(chunk * bq, bq)
    pieces = [(n, m) for n in range(2) for m in range(2)]
    count = tokens // KEYS
    first = at_ref[CHIP] == 0

    def queries(q_from):
        half = tokens // 2
        return [pltpu.make_async_copy(q_from.at[n, pl.ds(m * half + chunk * bq, bq), :], q_s.at[n, m], sem.at[2 * n + m]) for n, m in pieces]

    def keys(kv_from, b):
        here = pl.ds(pl.multiple_of(b * KEYS, KEYS), KEYS)
        return [pltpu.make_async_copy(kv_from.at[n, here, :], to.at[here, :], sem.at[4 + 2 * b + n]) for n, to in enumerate((k_s, v_s))]

    def start(q_from, kv_from):
        for copy in queries(q_from) + [copy for b in range(count) for copy in keys(kv_from, b)]:
            copy.start()

    @pl.when(first)
    def _():
        start(came_ref, made_ref.at[1])

    @pl.when(jnp.logical_not(first))
    def _():
        start(made_ref.at[2], came_ref)

    carry = pltpu.make_async_copy(own_ref.at[1, :, :, rows, :], in_s, sem.at[4 + 2 * count])
    carry.start()
    top_s[...] = jnp.full(top_s.shape, NEG, jnp.float32)
    mix_s[...] = jnp.zeros(mix_s.shape, jnp.float32)
    for copy in queries(came_ref):
        copy.wait()

    def block(b, _):
        for copy in keys(came_ref, b):
            copy.wait()
        here = pl.ds(pl.multiple_of(b * KEYS, KEYS), KEYS)
        strips = [(s * STRIP, q_s[n, m], KEYS, None) for s, (n, m) in enumerate(pieces)]
        _block(strips, k_s[here, :], v_s[here, :], top_s, mix_s)

    lax.fori_loop(0, count, block, None)
    carry.wait()
    for s, (n, m) in enumerate(pieces):
        cols = slice(s * STRIP, (s + 1) * STRIP)
        top, total = top_s[:, cols] * SCALE, mix_s[HEAD : HEAD + 1, cols]
        before = jnp.where(first, NEG, lse_in[0, n, m : m + 1, :])
        most = jnp.maximum(top, before)
        wa, wb = jnp.exp(top - most), jnp.exp(before - most)
        whole = total * wa + wb
        scale = 1 / whole
        tall = lambda row: jnp.broadcast_to(row, (128, STRIP)).T
        out, kept = (mix_s[:HEAD, cols] * (wa * scale)).T, tall(wb * scale)
        for at in (0, 128):
            o_ref[n, m, :, at : at + 128] = (out[:, at : at + 128] + in_s[n, m, :, at : at + 128] * kept).astype(o_ref.dtype)
        lse_ref[n, m : m + 1, :] = most + jnp.log(whole)


def attend_cross(at, came, made, own_o, own_lse, i):
    tokens = made.shape[2]
    half = tokens // 2
    bq = half // CHUNKS
    anywhere = pl.BlockSpec(memory_space=pl.ANY)
    return pl.pallas_call(
        functools.partial(_cross, chunk=i),
        grid_spec=pltpu.PrefetchScalarGridSpec(
            num_scalar_prefetch=1, grid=(1,),
            in_specs=[anywhere, anywhere, anywhere, pl.BlockSpec((1, 2, 2, bq), lambda g, at_ref: (1, 0, 0, i))],
            out_specs=[
                pl.BlockSpec((2, 2, bq, HEAD), lambda g, at_ref: (0, 0, 0, 0)),
                pl.BlockSpec((2, 2, bq), lambda g, at_ref: (0, 0, 0)),
            ],
            scratch_shapes=[
                pltpu.VMEM((2, 2, bq, HEAD), jnp.bfloat16), pltpu.VMEM((tokens, HEAD), jnp.bfloat16), pltpu.VMEM((tokens, HEAD), jnp.bfloat16),
                pltpu.VMEM((2, 2, bq, HEAD), jnp.float32), pltpu.VMEM((1, 4 * bq), jnp.float32), pltpu.VMEM((HEAD + 8, 4 * bq), jnp.float32),
                pltpu.SemaphoreType.DMA((5 + 2 * (tokens // KEYS),)),
            ],
        ),
        out_shape=[jax.ShapeDtypeStruct((2, 2, bq, HEAD), jnp.bfloat16), jax.ShapeDtypeStruct((2, 2, bq), jnp.float32)],
        compiler_params=pltpu.CompilerParams(dimension_semantics=("arbitrary",), vmem_limit_bytes=VMEM),
        cost_estimate=pl.CostEstimate(flops=16 * bq * tokens * HEAD, transcendentals=4 * bq * tokens, bytes_accessed=8 * tokens * HEAD),
        name="attend_cross",
    )(at, came, made, own_o.reshape(2, 2, 2, half, HEAD), own_lse.reshape(2, 2, 2, half))


def _merge(at_ref, own_ref, lse_ref, far_ref, far_lse_ref, o_ref, keep_ref, give_ref):
    chip, core = at_ref[CHIP], at_ref[CORE]
    for to_ref, m in ((keep_ref, core), (give_ref, 1 - core)):
        lse = lse_ref[0, 0, pl.ds(m, 1), :]
        far_lse = jnp.where(chip == 0, NEG, far_lse_ref[0, pl.ds(m, 1), :])
        top = jnp.maximum(lse, far_lse)
        wa, wb = jnp.exp(lse - top), jnp.exp(far_lse - top)
        total = 1 / (wa + wb)
        tall = lambda row: jnp.broadcast_to(row, (128, row.shape[1])).T
        wa, wb = tall(wa * total), tall(wb * total)
        for at in (0, 128):
            cols = slice(at, at + 128)
            to_ref[0, 0, :, cols] = (own_ref[0, 0, m, :, cols] * wa + far_ref[0, m, :, cols].astype(jnp.float32) * wb).astype(jnp.bfloat16)
        to_ref[1, 0] = jnp.where(chip == 0, own_ref[1, 0, m].astype(jnp.bfloat16), o_ref[0, m])


def merge(at, own_o, own_lse, far, far_lse, o, i):
    half, bq = own_o.shape[2] // 2, o.shape[2]
    part = pl.BlockSpec((1, 2, bq, HEAD), lambda n, at_ref: (n, 0, 0, 0))
    result = pl.BlockSpec((2, 1, bq, HEAD), lambda n, at_ref: (0, n, 0, 0))
    return pl.pallas_call(
        _merge,
        grid_spec=pltpu.PrefetchScalarGridSpec(
            num_scalar_prefetch=1, grid=(2,),
            in_specs=[
                pl.BlockSpec((2, 1, 2, bq, HEAD), lambda n, at_ref: (0, n, 0, i, 0)),
                pl.BlockSpec((2, 1, 2, bq), lambda n, at_ref: (0, n, 0, i)),
                part, pl.BlockSpec((1, 2, bq), lambda n, at_ref: (n, 0, 0)), part,
            ],
            out_specs=[result, result],
        ),
        out_shape=[jax.ShapeDtypeStruct((2, 2, bq, HEAD), jnp.bfloat16)] * 2,
        compiler_params=pltpu.CompilerParams(dimension_semantics=("arbitrary",), vmem_limit_bytes=VMEM),
        cost_estimate=pl.CostEstimate(flops=64 * bq * HEAD, transcendentals=0, bytes_accessed=64 * bq * HEAD),
        name="merge",
    )(at, own_o.reshape(2, 2, 2, half, HEAD), own_lse.reshape(2, 2, 2, half), far, far_lse, o)


def _output(at_ref, x_ref, w_own, w_sib, wx, wy, vx, vy, *rest, count):
    y_ref = rest[-1]
    chip, group = at_ref[CHIP], at_ref[GROUP]
    rows = y_ref.shape[0] // count
    for i in range(count):
        here = slice(i * rows, (i + 1) * rows)
        parts, weights = [], []
        for o_ref, w, from_x, from_y in ((rest[2 * i], w_own, wx, wy), (rest[2 * i + 1], w_sib, vx, vy)):
            parts += [o_ref[chip, 0], o_ref[chip, 1], o_ref[1 - chip, group], o_ref[1 - chip, 1 - group]]
            weights += [w[:HEAD, :], w[HEAD:, :], from_x[...], from_y[...]]
        y = _dot(jnp.concatenate(parts, axis=1), jnp.concatenate(weights, axis=0), 1, 0)
        y_ref[here, :] = (x_ref[here, :].astype(jnp.float32) + y).astype(y_ref.dtype)


def output(at, x, weights, results, first, done):
    count = len(results)
    rows, width = results[0][0].shape[2], x.shape[1]
    bn = 768
    part = pl.BlockSpec(results[0][0].shape, lambda j, at_ref: (0, 0, 0, 0))
    here = pl.BlockSpec((count * rows, bn), lambda j, at_ref: (first // count, j))
    given = [x, *weights] + [r for pair in results for r in pair]
    specs = [here] + [pl.BlockSpec((w.shape[0], bn), lambda j, at_ref: (0, j)) for w in weights] + [part] * (2 * count)
    alias = {}
    if done is not None:
        given.append(done)
        specs.append(pl.BlockSpec(memory_space=pl.ANY))
        alias = {len(given): 0}
    return pl.pallas_call(
        functools.partial(_output, count=count),
        grid_spec=pltpu.PrefetchScalarGridSpec(num_scalar_prefetch=1, grid=(width // bn,), in_specs=specs, out_specs=here),
        out_shape=jax.ShapeDtypeStruct(x.shape, jnp.bfloat16),
        input_output_aliases=alias,
        compiler_params=pltpu.CompilerParams(dimension_semantics=("arbitrary",), vmem_limit_bytes=VMEM),
        cost_estimate=pl.CostEstimate(flops=2 * count * rows * 8 * HEAD * width, transcendentals=0, bytes_accessed=16 * HEAD * width),
        name="output",
    )(at, *given)


def tables(place):
    half = HEAD // 2
    angle = place.astype(jnp.float32)[:, None] * THETA ** (-jnp.arange(half, dtype=jnp.float32) / half)
    return jnp.cos(angle), jnp.sin(angle)


def solution(mesh):
    def step(x, gain, wq, wk, wv, wo):
        own = x.shape[0]
        rank, group = lax.axis_index("sp"), lax.axis_index("dp")
        chip, core = rank // 2, rank % 2

        pick = lambda n, which: jnp.where(which == 0, ORDER[0][n], ORDER[1][n])
        at = jnp.stack([pick(n, chip) for n in range(4)] + [pick(n, 1 - chip) for n in range(4)] + [chip, core, group]).astype(jnp.int32)

        w_own, w_give = share(at, wq, wk, wv)
        w_sib = lax.ppermute(w_give, "sp", SIBLING)
        x_sib = lax.ppermute(x, "sp", SIBLING)
        leaving = leave(at, w_own, w_sib)
        wx, wy = [], []
        for n in range(4):
            wx.append(lax.ppermute(leaving[n], "sp", ACROSS))
            wy.append(lax.ppermute(wx[n], "dp", GROUPS))

        a_own = normed(x, gain)
        a_sib = normed(x_sib, gain)
        cos, sin = tables(chip * 2 * own + jnp.arange(2 * own))

        made, sent = None, None
        for n in range(4):
            got = project(at, a_own, a_sib, w_own, w_sib, wx[n], wy[n], cos, sin, n, made)
            made = got[0]
            if n == 0:
                sent = got[1]
        came = lax.ppermute(sent, "sp", ACROSS)

        wo_here, _ = lax.optimization_barrier((wo, sent))
        wo_half = lax.dynamic_slice_in_dim(wo_here, group * HEAD, HEAD, axis=0)
        ox = lax.ppermute(wo_half, "sp", ACROSS)
        oy = lax.ppermute(ox, "dp", GROUPS)
        wo_sib, ox_sib, oy_sib = (lax.ppermute(w, "sp", SIBLING) for w in (wo_here, ox, oy))
        weights = (wo, wo_sib, ox, oy, ox_sib, oy_sib)

        own_o, own_lse = attend_own(made)

        results = []
        for i in range(CHUNKS):
            o, lse = attend_cross(at, came, made, own_o, own_lse, i)
            far, far_lse = lax.ppermute(o, "sp", BACK), lax.ppermute(lse, "sp", BACK)
            keep, give = merge(at, own_o, own_lse, far, far_lse, o, i)
            results.append((keep, lax.ppermute(give, "sp", SIBLING)))
        y = output(at, x, weights, results[:-1], 0, None)
        y = output(at, x, weights, results[-1:], CHUNKS - 1, y)
        return y

    tokens, whole = P(("dp", "sp"), None), P("sp", None)
    return jax.shard_map(
        step,
        mesh=mesh,
        in_specs=(tokens, P(None), whole, whole, whole, whole),
        out_specs=tokens,
        check_vma=False,
    )
```

```python
import functools

import jax
import jax.numpy as jnp
from jax import lax
from jax.experimental import pallas as pl
from jax.experimental.pallas import tpu as pltpu
from jax.sharding import PartitionSpec as P


NEG = -1e30
HIDDEN = 2 * NEG
LOG2E = 1.4426950408889634
VMEM = 56 * 2**20
HEAD = 256
THETA = 10000
SCALE = HEAD**-0.5
E = SCALE * LOG2E
STRIP = 512
KEYS = 1024
CHUNKS = 4


SIBLING = [(0, 1), (1, 0), (2, 3), (3, 2)]
ACROSS = [(0, 2), (2, 0), (1, 3), (3, 1)]
BACK = [(0, 2), (1, 3)]
GROUPS = [(0, 1), (1, 0)]
ORDER = ((3, 1, 0, 2), (0, 2, 1, 3))
OTHERS, CHIP, CORE, GROUP = 4, 8, 9, 10


def _dot(a, b, ca, cb):
    return lax.dot_general(a, b, (((ca,), (cb,)), ((), ())), preferred_element_type=jnp.float32)


def _share(at_ref, *refs):
    for q_ref, k_ref, v_ref, to_ref in (refs[:3] + refs[6:7], refs[3:6] + refs[7:8]):
        to_ref[0] = q_ref[...]
        to_ref[1, :, :HEAD] = k_ref[...]
        to_ref[1, :, HEAD:] = v_ref[...]


def share(at, wq, wk, wv):
    rows = wq.shape[0]
    specs = []
    for mine in (True, False):
        at_block = lambda p, at_ref, mine=mine: (0, 2 * p + (at_ref[CORE] if mine else 1 - at_ref[CORE]))
        specs += [pl.BlockSpec((rows, 2 * HEAD), at_block), pl.BlockSpec((rows, HEAD), at_block), pl.BlockSpec((rows, HEAD), at_block)]
    out = pl.BlockSpec((2, rows, 2 * HEAD), lambda p, at_ref: (p, 0, 0))
    return pl.pallas_call(
        _share,
        grid_spec=pltpu.PrefetchScalarGridSpec(num_scalar_prefetch=1, grid=(2,), in_specs=specs, out_specs=[out, out]),
        out_shape=[jax.ShapeDtypeStruct((4, rows, 2 * HEAD), jnp.bfloat16)] * 2,
        compiler_params=pltpu.CompilerParams(dimension_semantics=("arbitrary",), vmem_limit_bytes=VMEM),
        cost_estimate=pl.CostEstimate(flops=1000, transcendentals=0, bytes_accessed=4 * wq.size * 2),
        name="share",
    )(at, wq, wk, wv, wq, wk, wv)


def _leave(at_ref, own_ref, sib_ref, *to_refs):
    for n, to_ref in enumerate(to_refs):
        slot = at_ref[OTHERS + n]

        @pl.when(at_ref[GROUP] == at_ref[CORE])
        def _():
            to_ref[...] = own_ref[slot]

        @pl.when(at_ref[GROUP] != at_ref[CORE])
        def _():
            to_ref[...] = sib_ref[slot]


def leave(at, w_own, w_sib):
    whole = pl.BlockSpec(w_own.shape, lambda i, at_ref: (0, 0, 0))
    out = pl.BlockSpec(w_own.shape[1:], lambda i, at_ref: (0, 0))
    return pl.pallas_call(
        _leave,
        grid_spec=pltpu.PrefetchScalarGridSpec(num_scalar_prefetch=1, grid=(1,), in_specs=[whole, whole], out_specs=[out] * 4),
        out_shape=[jax.ShapeDtypeStruct(w_own.shape[1:], jnp.bfloat16)] * 4,
        compiler_params=pltpu.CompilerParams(dimension_semantics=("arbitrary",), vmem_limit_bytes=VMEM),
        cost_estimate=pl.CostEstimate(flops=1000, transcendentals=0, bytes_accessed=6 * w_own.size),
        name="leave",
    )(at, w_own, w_sib)


def _normed(x_ref, gain_ref, a_ref):
    wide = x_ref[...].astype(jnp.float32)
    scale = lax.rsqrt(jnp.mean(wide * wide, -1, keepdims=True) + 1e-6)
    a_ref[...] = (wide * scale * gain_ref[...].astype(jnp.float32)).astype(jnp.bfloat16)


def normed(x, gain):
    rows, depth = x.shape
    block = pl.BlockSpec((256, depth), lambda i: (i, 0))
    return pl.pallas_call(
        _normed,
        grid=(rows // 256,),
        in_specs=[block, pl.BlockSpec((1, depth), lambda i: (0, 0))],
        out_specs=block,
        out_shape=jax.ShapeDtypeStruct(x.shape, jnp.bfloat16),
        compiler_params=pltpu.CompilerParams(dimension_semantics=("arbitrary",), vmem_limit_bytes=VMEM),
        cost_estimate=pl.CostEstimate(flops=8 * x.size, transcendentals=0, bytes_accessed=4 * x.size),
        name="normed",
    )(x, gain[None])


def _project(at_ref, a0_ref, a1_ref, own_ref, sib_ref, wx_ref, wy_ref, cos_ref, sin_ref, *rest, which):
    out_ref, sent_ref, w_s = rest if which == 0 else (rest[1], None, rest[2])
    slot, chip, core, group = at_ref[which], at_ref[CHIP], at_ref[CORE], at_ref[GROUP]
    i = pl.program_id(0)
    rows = own_ref.shape[1]

    @pl.when(i == 0)
    def _():
        here, there = 2 * rows * chip, 2 * rows * (1 - chip)
        for at, ref in ((here + rows * core, own_ref), (here + rows * (1 - core), sib_ref)):
            w_s[pl.ds(pl.multiple_of(at, 64), rows), :] = ref[0]
        for at, ref in ((there + rows * group, wx_ref), (there + rows * (1 - group), wy_ref)):
            w_s[pl.ds(pl.multiple_of(at, 64), rows), :] = ref[...]

    def part(a_ref):
        t = _dot(a_ref[...], w_s[...], 1, 0).astype(jnp.bfloat16).astype(jnp.float32)
        cos, sin = cos_ref[...], sin_ref[...]
        half = HEAD // 2
        for n in range(2):
            p, q = t[:, n * HEAD : n * HEAD + half], t[:, n * HEAD + half : (n + 1) * HEAD]
            u, v = p * cos - q * sin, q * cos + p * sin
            if n == 1:
                u, v = jnp.where(slot % 2 == 0, u, p), jnp.where(slot % 2 == 0, v, q)
            got = jnp.concatenate([u, v], axis=1).astype(jnp.bfloat16)
            out_ref[0, n] = got
            if sent_ref is not None:
                sent_ref[n] = got

    @pl.when(i < pl.num_programs(0) // 2)
    def _():
        part(a0_ref)

    @pl.when(i >= pl.num_programs(0) // 2)
    def _():
        part(a1_ref)


def project(at, a_own, a_sib, w_own, w_sib, wx, wy, cos, sin, which, done):
    tokens, depth = a_own.shape
    rows, width = wx.shape
    bm = 512
    n = tokens // bm
    first = which == 0

    def place(i, at_ref):
        return jnp.where(i < n, at_ref[CORE] * n + i, (1 - at_ref[CORE]) * n + i - n)

    weights = pl.BlockSpec((1, rows, width), lambda i, at_ref: (at_ref[which], 0, 0))
    fetched = pl.BlockSpec((rows, width), lambda i, at_ref: (0, 0))
    table = pl.BlockSpec((bm, HEAD // 2), lambda i, at_ref: (place(i, at_ref), 0))
    specs = [
        pl.BlockSpec((bm, depth), lambda i, at_ref: (jnp.minimum(i, n - 1), 0)),
        pl.BlockSpec((bm, depth), lambda i, at_ref: (jnp.maximum(i - n, 0), 0)),
        weights, weights, fetched, fetched, table, table,
    ]
    given = [a_own, a_sib, w_own, w_sib, wx, wy, cos, sin]
    out_shape = [jax.ShapeDtypeStruct((4, 2, 2 * tokens, HEAD), jnp.bfloat16)]
    out_specs = [pl.BlockSpec((1, 2, bm, HEAD), lambda i, at_ref: (at_ref[which], 0, place(i, at_ref), 0))]
    alias = {}
    if first:
        out_shape.append(jax.ShapeDtypeStruct((2, 2 * tokens, HEAD), jnp.bfloat16))
        out_specs.append(pl.BlockSpec((2, bm, HEAD), lambda i, at_ref: (0, place(i, at_ref), 0)))
    else:
        given.append(done)
        specs.append(pl.BlockSpec(memory_space=pl.ANY))
        alias = {len(given): 0}
    return pl.pallas_call(
        functools.partial(_project, which=which),
        grid_spec=pltpu.PrefetchScalarGridSpec(
            num_scalar_prefetch=1, grid=(2 * n,), in_specs=specs, out_specs=out_specs,
            scratch_shapes=[pltpu.VMEM((4 * rows, width), jnp.bfloat16)],
        ),
        out_shape=out_shape,
        input_output_aliases=alias,
        compiler_params=pltpu.CompilerParams(dimension_semantics=("arbitrary",), vmem_limit_bytes=VMEM),
        cost_estimate=pl.CostEstimate(flops=4 * tokens * depth * width, transcendentals=0, bytes_accessed=4 * tokens * depth),
        name="project",
    )(at, *given)


def _weigh(scores, i, values, top_s, mix_s, ok=None):
    if ok is not None:
        least = scores.shape[0] - STRIP
        last = jnp.where(ok, scores[least:], HIDDEN)
        scores = jnp.concatenate([scores[:least], last], axis=0) if least else last
    old = top_s[i]
    top = jnp.maximum(old, scores.max(axis=0, keepdims=True))
    top_s[i] = top
    p = jnp.exp2((scores - top) * E).astype(jnp.bfloat16)
    mix_s[i] = mix_s[i] * jnp.exp2((old - top) * E) + _dot(values, p, 1, 0)


def _turn(v, at, to_s):
    to_s[:HEAD, pl.ds(at, v.shape[0])] = v.T
    to_s[HEAD:, pl.ds(at, v.shape[0])] = jnp.ones((8, v.shape[0]), jnp.bfloat16)


def _own(q_ref, k_ref, v_ref, o_ref, lse_ref, score_s, value_s, top_s, mix_s):
    bq = q_ref.shape[2]
    iq = pl.program_id(1)
    top_s[...] = jnp.full(top_s.shape, NEG, jnp.float32)
    mix_s[...] = jnp.zeros(mix_s.shape, jnp.float32)
    ok = lax.broadcasted_iota(jnp.int32, (STRIP, STRIP), 1) >= lax.broadcasted_iota(jnp.int32, (STRIP, STRIP), 0)
    head = lambda i: lax.rem(lax.div(i, 2), 2)
    strip = lambda i: lax.rem(i, 2) + 2 * (1 - lax.div(i, 4))
    rows = lambda s, size=STRIP: pl.ds(pl.multiple_of(s * STRIP, STRIP), size)
    queries = lambda i: q_ref[0, head(i), rows(strip(i)), :]
    keys = lambda j: pl.ds(pl.multiple_of(j * KEYS, KEYS), KEYS)

    @pl.when(iq == 0)
    def _():
        lax.fori_loop(0, k_ref.shape[2] // KEYS, lambda j, _: _turn(v_ref[0, 0, keys(j), :], pl.multiple_of(j * KEYS, KEYS), value_s), None)

    score = lambda j, i: _dot(k_ref[0, 0, keys(j), :], queries(i), 1, 1)
    groups = 2 * (bq // KEYS) * iq + 1
    score_s[0] = score(0, 0)

    def group(g, _):
        j, base = lax.div(g, 2), 4 * lax.rem(g, 2)
        for u in range(4):
            near = (j, base + u + 1) if u < 3 else (lax.div(jnp.minimum(g + 1, groups - 1), 2), lax.rem(base + 4, 8))
            score_s[(u + 1) % 2] = score(*near)
            _weigh(score_s[u % 2], base + u, value_s[:, keys(j)], top_s, mix_s)

    lax.fori_loop(0, groups, group, None)

    def pair(d, _):
        n, half = lax.div(d, 2), lax.rem(d, 2)
        i = 4 * (1 - half) + 2 * n
        at = pl.multiple_of((iq * (bq // KEYS) + half) * KEYS, KEYS)
        some, all_ = pl.ds(at, STRIP), pl.ds(at, KEYS)
        score_s[0, :STRIP] = _dot(k_ref[0, 0, some, :], queries(i), 1, 1)
        score_s[1] = _dot(k_ref[0, 0, all_, :], queries(i + 1), 1, 1)
        _weigh(score_s[0, :STRIP], i, value_s[:, some], top_s, mix_s, ok)
        _weigh(score_s[1], i + 1, value_s[:, all_], top_s, mix_s, ok)

    lax.fori_loop(0, 4, pair, None)

    for i in range(8):
        n, s = i // 2 % 2, i % 2 + 2 * (1 - i // 4)
        total = mix_s[i, HEAD : HEAD + 1, :]
        here = slice(s * STRIP, (s + 1) * STRIP)
        o_ref[0, n, here, :] = (mix_s[i, :HEAD, :] * (1 / total)).T
        lse_ref[0, n : n + 1, here] = top_s[i] * SCALE + jnp.log(total)


def attend_own(made):
    tokens = made.shape[2]
    bq = 2 * KEYS
    return pl.pallas_call(
        _own,
        grid=(2, tokens // bq),
        in_specs=[
            pl.BlockSpec((1, 2, bq, HEAD), lambda h, i: (2 * h, 0, i, 0)),
            pl.BlockSpec((1, 1, tokens, HEAD), lambda h, i: (2 * h + 1, 0, 0, 0)),
            pl.BlockSpec((1, 1, tokens, HEAD), lambda h, i: (2 * h + 1, 1, 0, 0)),
        ],
        out_specs=[
            pl.BlockSpec((1, 2, bq, HEAD), lambda h, i: (h, 0, i, 0)),
            pl.BlockSpec((1, 2, bq), lambda h, i: (h, 0, i)),
        ],
        out_shape=[jax.ShapeDtypeStruct((2, 2, tokens, HEAD), jnp.float32), jax.ShapeDtypeStruct((2, 2, tokens), jnp.float32)],
        scratch_shapes=[
            pltpu.VMEM((2, KEYS, STRIP), jnp.float32), pltpu.VMEM((HEAD + 8, tokens), jnp.bfloat16),
            pltpu.VMEM((8, 1, STRIP), jnp.float32), pltpu.VMEM((8, HEAD + 8, STRIP), jnp.float32),
        ],
        compiler_params=pltpu.CompilerParams(dimension_semantics=("arbitrary", "arbitrary"), vmem_limit_bytes=VMEM),
        cost_estimate=pl.CostEstimate(flops=8 * tokens * tokens * HEAD, transcendentals=2 * tokens * tokens, bytes_accessed=2 * made.size),
        name="attend_own",
    )(made, made, made)


def _cross(at_ref, came_ref, made_ref, own_ref, lse_in, o_ref, lse_ref, q_s, k_s, v_s, in_s, score_s, value_s, top_s, mix_s, sem, *, chunk):
    bq = o_ref.shape[2]
    tokens = k_s.shape[0]
    rows = pl.ds(chunk * bq, bq)
    pieces = [(n, m) for n in range(2) for m in range(2)]
    count = tokens // KEYS
    first = at_ref[CHIP] == 0

    def queries(q_from):
        half = tokens // 2
        return [pltpu.make_async_copy(q_from.at[n, pl.ds(m * half + chunk * bq, bq), :], q_s.at[n, m], sem.at[2 * n + m]) for n, m in pieces]

    def keys(kv_from, b, n):
        rows = pl.ds(pl.multiple_of(b * KEYS, KEYS), KEYS)
        return pltpu.make_async_copy(kv_from.at[n, rows, :], (k_s, v_s)[n].at[rows, :], sem.at[4 + 2 * b + n])

    def start(q_from, kv_from):
        for copy in queries(q_from) + [keys(kv_from, b, n) for b in range(count) for n in range(2)]:
            copy.start()

    @pl.when(first)
    def _():
        start(came_ref, made_ref.at[1])

    @pl.when(jnp.logical_not(first))
    def _():
        start(made_ref.at[2], came_ref)

    carry = pltpu.make_async_copy(own_ref.at[1, :, :, rows, :], in_s, sem.at[4 + 2 * count])
    carry.start()
    top_s[...] = jnp.full(top_s.shape, NEG, jnp.float32)
    mix_s[...] = jnp.zeros(mix_s.shape, jnp.float32)
    for copy in queries(came_ref) + [keys(came_ref, 0, 0)]:
        copy.wait()
    here = lambda b: pl.ds(pl.multiple_of(b * KEYS, KEYS), KEYS)
    score = lambda b, i: _dot(k_s[here(b), :], q_s[pieces[i]], 1, 1)
    score_s[0] = score(0, 0)

    def block(b, _):
        @pl.when(b + 1 < count)
        def _():
            keys(came_ref, b + 1, 0).wait()

        keys(came_ref, b, 1).wait()
        _turn(v_s[here(b), :], 0, value_s)
        for i in range(4):
            score_s[(i + 1) % 2] = score(b, i + 1) if i < 3 else score(jnp.minimum(b + 1, count - 1), 0)
            _weigh(score_s[i % 2], i, value_s[...], top_s, mix_s)

    lax.fori_loop(0, count, block, None)
    carry.wait()
    for s, (n, m) in enumerate(pieces):
        top, total = top_s[s] * SCALE, mix_s[s, HEAD : HEAD + 1, :]
        before = jnp.where(first, NEG, lse_in[0, n, m : m + 1, :])
        most = jnp.maximum(top, before)
        wa, wb = jnp.exp(top - most), jnp.exp(before - most)
        whole = total * wa + wb
        scale = 1 / whole
        tall = lambda row: jnp.broadcast_to(row, (128, STRIP)).T
        out, kept = (mix_s[s, :HEAD, :] * (wa * scale)).T, tall(wb * scale)
        for at in (0, 128):
            o_ref[n, m, :, at : at + 128] = (out[:, at : at + 128] + in_s[n, m, :, at : at + 128] * kept).astype(o_ref.dtype)
        lse_ref[n, m : m + 1, :] = most + jnp.log(whole)


def attend_cross(at, came, made, own_o, own_lse, i):
    tokens = made.shape[2]
    half = tokens // 2
    bq = half // CHUNKS
    anywhere = pl.BlockSpec(memory_space=pl.ANY)
    return pl.pallas_call(
        functools.partial(_cross, chunk=i),
        grid_spec=pltpu.PrefetchScalarGridSpec(
            num_scalar_prefetch=1, grid=(1,),
            in_specs=[anywhere, anywhere, anywhere, pl.BlockSpec((1, 2, 2, bq), lambda g, at_ref: (1, 0, 0, i))],
            out_specs=[
                pl.BlockSpec((2, 2, bq, HEAD), lambda g, at_ref: (0, 0, 0, 0)),
                pl.BlockSpec((2, 2, bq), lambda g, at_ref: (0, 0, 0)),
            ],
            scratch_shapes=[
                pltpu.VMEM((2, 2, bq, HEAD), jnp.bfloat16), pltpu.VMEM((tokens, HEAD), jnp.bfloat16), pltpu.VMEM((tokens, HEAD), jnp.bfloat16),
                pltpu.VMEM((2, 2, bq, HEAD), jnp.float32), pltpu.VMEM((2, KEYS, STRIP), jnp.float32), pltpu.VMEM((HEAD + 8, KEYS), jnp.bfloat16),
                pltpu.VMEM((4, 1, STRIP), jnp.float32), pltpu.VMEM((4, HEAD + 8, STRIP), jnp.float32),
                pltpu.SemaphoreType.DMA((5 + 2 * (tokens // KEYS),)),
            ],
        ),
        out_shape=[jax.ShapeDtypeStruct((2, 2, bq, HEAD), jnp.bfloat16), jax.ShapeDtypeStruct((2, 2, bq), jnp.float32)],
        compiler_params=pltpu.CompilerParams(dimension_semantics=("arbitrary",), vmem_limit_bytes=VMEM),
        cost_estimate=pl.CostEstimate(flops=16 * bq * tokens * HEAD, transcendentals=4 * bq * tokens, bytes_accessed=8 * tokens * HEAD),
        name="attend_cross",
    )(at, came, made, own_o.reshape(2, 2, 2, half, HEAD), own_lse.reshape(2, 2, 2, half))


def _merge(at_ref, own_ref, lse_ref, far_ref, far_lse_ref, o_ref, keep_ref, give_ref):
    chip, core = at_ref[CHIP], at_ref[CORE]
    for to_ref, m in ((keep_ref, core), (give_ref, 1 - core)):
        lse = lse_ref[0, 0, pl.ds(m, 1), :]
        far_lse = jnp.where(chip == 0, NEG, far_lse_ref[0, pl.ds(m, 1), :])
        top = jnp.maximum(lse, far_lse)
        wa, wb = jnp.exp(lse - top), jnp.exp(far_lse - top)
        total = 1 / (wa + wb)
        tall = lambda row: jnp.broadcast_to(row, (128, row.shape[1])).T
        wa, wb = tall(wa * total), tall(wb * total)
        for at in (0, 128):
            cols = slice(at, at + 128)
            to_ref[0, 0, :, cols] = (own_ref[0, 0, m, :, cols] * wa + far_ref[0, m, :, cols].astype(jnp.float32) * wb).astype(jnp.bfloat16)
        to_ref[1, 0] = jnp.where(chip == 0, own_ref[1, 0, m].astype(jnp.bfloat16), o_ref[0, m])


def merge(at, own_o, own_lse, far, far_lse, o, i):
    half, bq = own_o.shape[2] // 2, o.shape[2]
    part = pl.BlockSpec((1, 2, bq, HEAD), lambda n, at_ref: (n, 0, 0, 0))
    result = pl.BlockSpec((2, 1, bq, HEAD), lambda n, at_ref: (0, n, 0, 0))
    return pl.pallas_call(
        _merge,
        grid_spec=pltpu.PrefetchScalarGridSpec(
            num_scalar_prefetch=1, grid=(2,),
            in_specs=[
                pl.BlockSpec((2, 1, 2, bq, HEAD), lambda n, at_ref: (0, n, 0, i, 0)),
                pl.BlockSpec((2, 1, 2, bq), lambda n, at_ref: (0, n, 0, i)),
                part, pl.BlockSpec((1, 2, bq), lambda n, at_ref: (n, 0, 0)), part,
            ],
            out_specs=[result, result],
        ),
        out_shape=[jax.ShapeDtypeStruct((2, 2, bq, HEAD), jnp.bfloat16)] * 2,
        compiler_params=pltpu.CompilerParams(dimension_semantics=("arbitrary",), vmem_limit_bytes=VMEM),
        cost_estimate=pl.CostEstimate(flops=64 * bq * HEAD, transcendentals=0, bytes_accessed=64 * bq * HEAD),
        name="merge",
    )(at, own_o.reshape(2, 2, 2, half, HEAD), own_lse.reshape(2, 2, 2, half), far, far_lse, o)


def _output(at_ref, x_ref, w_own, w_sib, wx, wy, vx, vy, *rest, count):
    y_ref = rest[-1]
    chip, group = at_ref[CHIP], at_ref[GROUP]
    rows = y_ref.shape[0] // count
    for i in range(count):
        here = slice(i * rows, (i + 1) * rows)
        parts, weights = [], []
        for o_ref, w, from_x, from_y in ((rest[2 * i], w_own, wx, wy), (rest[2 * i + 1], w_sib, vx, vy)):
            parts += [o_ref[chip, 0], o_ref[chip, 1], o_ref[1 - chip, group], o_ref[1 - chip, 1 - group]]
            weights += [w[:HEAD, :], w[HEAD:, :], from_x[...], from_y[...]]
        y = _dot(jnp.concatenate(parts, axis=1), jnp.concatenate(weights, axis=0), 1, 0)
        y_ref[here, :] = (x_ref[here, :].astype(jnp.float32) + y).astype(y_ref.dtype)


def output(at, x, weights, results, first, done):
    count = len(results)
    rows, width = results[0][0].shape[2], x.shape[1]
    bn = 768
    part = pl.BlockSpec(results[0][0].shape, lambda j, at_ref: (0, 0, 0, 0))
    here = pl.BlockSpec((count * rows, bn), lambda j, at_ref: (first // count, j))
    given = [x, *weights] + [r for pair in results for r in pair]
    specs = [here] + [pl.BlockSpec((w.shape[0], bn), lambda j, at_ref: (0, j)) for w in weights] + [part] * (2 * count)
    alias = {}
    if done is not None:
        given.append(done)
        specs.append(pl.BlockSpec(memory_space=pl.ANY))
        alias = {len(given): 0}
    return pl.pallas_call(
        functools.partial(_output, count=count),
        grid_spec=pltpu.PrefetchScalarGridSpec(num_scalar_prefetch=1, grid=(width // bn,), in_specs=specs, out_specs=here),
        out_shape=jax.ShapeDtypeStruct(x.shape, jnp.bfloat16),
        input_output_aliases=alias,
        compiler_params=pltpu.CompilerParams(dimension_semantics=("arbitrary",), vmem_limit_bytes=VMEM),
        cost_estimate=pl.CostEstimate(flops=2 * count * rows * 8 * HEAD * width, transcendentals=0, bytes_accessed=16 * HEAD * width),
        name="output",
    )(at, *given)


def tables(place):
    half = HEAD // 2
    angle = place.astype(jnp.float32)[:, None] * THETA ** (-jnp.arange(half, dtype=jnp.float32) / half)
    return jnp.cos(angle), jnp.sin(angle)


def solution(mesh):
    def step(x, gain, wq, wk, wv, wo):
        own = x.shape[0]
        rank, group = lax.axis_index("sp"), lax.axis_index("dp")
        chip, core = rank // 2, rank % 2

        pick = lambda n, which: jnp.where(which == 0, ORDER[0][n], ORDER[1][n])
        at = jnp.stack([pick(n, chip) for n in range(4)] + [pick(n, 1 - chip) for n in range(4)] + [chip, core, group]).astype(jnp.int32)

        w_own, w_give = share(at, wq, wk, wv)
        w_sib = lax.ppermute(w_give, "sp", SIBLING)
        leaving = leave(at, w_own, w_sib)
        wx, wy = [], []
        for n in range(4):
            wx.append(lax.ppermute(leaving[n], "sp", ACROSS))
            wy.append(lax.ppermute(wx[n], "dp", GROUPS))

        a_own = normed(x, gain)
        a_sib = lax.ppermute(a_own, "sp", SIBLING)
        cos, sin = tables(chip * 2 * own + jnp.arange(2 * own))

        made, sent = None, None
        for n in range(4):
            got = project(at, a_own, a_sib, w_own, w_sib, wx[n], wy[n], cos, sin, n, made)
            made = got[0]
            if n == 0:
                sent = got[1]
        came = lax.ppermute(sent, "sp", ACROSS)

        wo_here, _ = lax.optimization_barrier((wo, sent))
        wo_half = lax.dynamic_slice_in_dim(wo_here, group * HEAD, HEAD, axis=0)
        ox = lax.ppermute(wo_half, "sp", ACROSS)
        oy = lax.ppermute(ox, "dp", GROUPS)
        wo_sib, ox_sib, oy_sib = (lax.ppermute(w, "sp", SIBLING) for w in (wo_here, ox, oy))
        weights = (wo, wo_sib, ox, oy, ox_sib, oy_sib)

        own_o, own_lse = attend_own(made)

        results = []
        for i in range(CHUNKS):
            o, lse = attend_cross(at, came, made, own_o, own_lse, i)
            far, far_lse = lax.ppermute(o, "sp", BACK), lax.ppermute(lse, "sp", BACK)
            keep, give = merge(at, own_o, own_lse, far, far_lse, o, i)
            results.append((keep, lax.ppermute(give, "sp", SIBLING)))
        y = output(at, x, weights, results[:-1], 0, None)
        y = output(at, x, weights, results[-1:], CHUNKS - 1, y)
        return y

    tokens, whole = P(("dp", "sp"), None), P("sp", None)
    return jax.shard_map(
        step,
        mesh=mesh,
        in_specs=(tokens, P(None), whole, whole, whole, whole),
        out_specs=tokens,
        check_vma=False,
    )
```

```python
import functools

import jax
import jax.numpy as jnp
from jax import lax
from jax.experimental import pallas as pl
from jax.experimental.pallas import tpu as pltpu
from jax.sharding import PartitionSpec as P


NEG = -1e30
HIDDEN = 2 * NEG
LOG2E = 1.4426950408889634
VMEM = 56 * 2**20
HEAD = 256
THETA = 10000
SCALE = HEAD**-0.5
E = SCALE * LOG2E
STRIP = 512
KEYS = 1024
CHUNKS = 4


SIBLING = [(0, 1), (1, 0), (2, 3), (3, 2)]
ACROSS = [(0, 2), (2, 0), (1, 3), (3, 1)]
BACK = [(0, 2), (1, 3)]
GROUPS = [(0, 1), (1, 0)]
ORDER = ((3, 1, 0, 2), (0, 2, 1, 3))
OTHERS, CHIP, CORE, GROUP = 4, 8, 9, 10


def _dot(a, b, ca, cb):
    return lax.dot_general(a, b, (((ca,), (cb,)), ((), ())), preferred_element_type=jnp.float32)


def _share(at_ref, *refs):
    for q_ref, k_ref, v_ref, to_ref in (refs[:3] + refs[6:7], refs[3:6] + refs[7:8]):
        to_ref[0] = q_ref[...]
        to_ref[1, :, :HEAD] = k_ref[...]
        to_ref[1, :, HEAD:] = v_ref[...]


def share(at, wq, wk, wv):
    rows = wq.shape[0]
    specs = []
    for mine in (True, False):
        at_block = lambda p, at_ref, mine=mine: (0, 2 * p + (at_ref[CORE] if mine else 1 - at_ref[CORE]))
        specs += [pl.BlockSpec((rows, 2 * HEAD), at_block), pl.BlockSpec((rows, HEAD), at_block), pl.BlockSpec((rows, HEAD), at_block)]
    out = pl.BlockSpec((2, rows, 2 * HEAD), lambda p, at_ref: (p, 0, 0))
    return pl.pallas_call(
        _share,
        grid_spec=pltpu.PrefetchScalarGridSpec(num_scalar_prefetch=1, grid=(2,), in_specs=specs, out_specs=[out, out]),
        out_shape=[jax.ShapeDtypeStruct((4, rows, 2 * HEAD), jnp.bfloat16)] * 2,
        compiler_params=pltpu.CompilerParams(dimension_semantics=("arbitrary",), vmem_limit_bytes=VMEM),
        cost_estimate=pl.CostEstimate(flops=1000, transcendentals=0, bytes_accessed=4 * wq.size * 2),
        name="share",
    )(at, wq, wk, wv, wq, wk, wv)


def _leave(at_ref, own_ref, sib_ref, *to_refs):
    for n, to_ref in enumerate(to_refs):
        slot = at_ref[OTHERS + n]

        @pl.when(at_ref[GROUP] == at_ref[CORE])
        def _():
            to_ref[...] = own_ref[slot]

        @pl.when(at_ref[GROUP] != at_ref[CORE])
        def _():
            to_ref[...] = sib_ref[slot]


def leave(at, w_own, w_sib):
    whole = pl.BlockSpec(w_own.shape, lambda i, at_ref: (0, 0, 0))
    out = pl.BlockSpec(w_own.shape[1:], lambda i, at_ref: (0, 0))
    return pl.pallas_call(
        _leave,
        grid_spec=pltpu.PrefetchScalarGridSpec(num_scalar_prefetch=1, grid=(1,), in_specs=[whole, whole], out_specs=[out] * 4),
        out_shape=[jax.ShapeDtypeStruct(w_own.shape[1:], jnp.bfloat16)] * 4,
        compiler_params=pltpu.CompilerParams(dimension_semantics=("arbitrary",), vmem_limit_bytes=VMEM),
        cost_estimate=pl.CostEstimate(flops=1000, transcendentals=0, bytes_accessed=6 * w_own.size),
        name="leave",
    )(at, w_own, w_sib)


def _normed(x_ref, gain_ref, a_ref):
    wide = x_ref[...].astype(jnp.float32)
    scale = lax.rsqrt(jnp.mean(wide * wide, -1, keepdims=True) + 1e-6)
    a_ref[...] = (wide * scale * gain_ref[...].astype(jnp.float32)).astype(jnp.bfloat16)


def normed(x, gain):
    rows, depth = x.shape
    block = pl.BlockSpec((256, depth), lambda i: (i, 0))
    return pl.pallas_call(
        _normed,
        grid=(rows // 256,),
        in_specs=[block, pl.BlockSpec((1, depth), lambda i: (0, 0))],
        out_specs=block,
        out_shape=jax.ShapeDtypeStruct(x.shape, jnp.bfloat16),
        compiler_params=pltpu.CompilerParams(dimension_semantics=("arbitrary",), vmem_limit_bytes=VMEM),
        cost_estimate=pl.CostEstimate(flops=8 * x.size, transcendentals=0, bytes_accessed=4 * x.size),
        name="normed",
    )(x, gain[None])


def _project(at_ref, a0_ref, a1_ref, own_ref, sib_ref, wx_ref, wy_ref, cos_ref, sin_ref, *rest, which):
    out_ref, sent_ref, w_s = rest if which == 0 else (rest[1], None, rest[2])
    slot, chip, core, group = at_ref[which], at_ref[CHIP], at_ref[CORE], at_ref[GROUP]
    i = pl.program_id(0)
    rows = own_ref.shape[1]

    @pl.when(i == 0)
    def _():
        here, there = 2 * rows * chip, 2 * rows * (1 - chip)
        for at, ref in ((here + rows * core, own_ref), (here + rows * (1 - core), sib_ref)):
            w_s[pl.ds(pl.multiple_of(at, 64), rows), :] = ref[0]
        for at, ref in ((there + rows * group, wx_ref), (there + rows * (1 - group), wy_ref)):
            w_s[pl.ds(pl.multiple_of(at, 64), rows), :] = ref[...]

    def part(a_ref):
        half = HEAD // 2
        for at in range(0, a_ref.shape[0], 256):
            here = slice(at, at + 256)
            t = _dot(a_ref[here, :], w_s[...], 1, 0).astype(jnp.bfloat16).astype(jnp.float32)
            cos, sin = cos_ref[here, :], sin_ref[here, :]
            for n in range(2):
                p, q = t[:, n * HEAD : n * HEAD + half], t[:, n * HEAD + half : (n + 1) * HEAD]
                u, v = p * cos - q * sin, q * cos + p * sin
                if n == 1:
                    u, v = jnp.where(slot % 2 == 0, u, p), jnp.where(slot % 2 == 0, v, q)
                got = jnp.concatenate([u, v], axis=1).astype(jnp.bfloat16)
                out_ref[0, n, here, :] = got
                if sent_ref is not None:
                    sent_ref[n, here, :] = got

    @pl.when(i < pl.num_programs(0) // 2)
    def _():
        part(a0_ref)

    @pl.when(i >= pl.num_programs(0) // 2)
    def _():
        part(a1_ref)


def project(at, a_own, a_sib, w_own, w_sib, wx, wy, cos, sin, which, done):
    tokens, depth = a_own.shape
    rows, width = wx.shape
    bm = 1024
    n = tokens // bm
    first = which == 0

    def place(i, at_ref):
        return jnp.where(i < n, at_ref[CORE] * n + i, (1 - at_ref[CORE]) * n + i - n)

    weights = pl.BlockSpec((1, rows, width), lambda i, at_ref: (at_ref[which], 0, 0))
    fetched = pl.BlockSpec((rows, width), lambda i, at_ref: (0, 0))
    table = pl.BlockSpec((bm, HEAD // 2), lambda i, at_ref: (place(i, at_ref), 0))
    specs = [
        pl.BlockSpec((bm, depth), lambda i, at_ref: (jnp.minimum(i, n - 1), 0)),
        pl.BlockSpec((bm, depth), lambda i, at_ref: (jnp.maximum(i - n, 0), 0)),
        weights, weights, fetched, fetched, table, table,
    ]
    given = [a_own, a_sib, w_own, w_sib, wx, wy, cos, sin]
    out_shape = [jax.ShapeDtypeStruct((4, 2, 2 * tokens, HEAD), jnp.bfloat16)]
    out_specs = [pl.BlockSpec((1, 2, bm, HEAD), lambda i, at_ref: (at_ref[which], 0, place(i, at_ref), 0))]
    alias = {}
    if first:
        out_shape.append(jax.ShapeDtypeStruct((2, 2 * tokens, HEAD), jnp.bfloat16))
        out_specs.append(pl.BlockSpec((2, bm, HEAD), lambda i, at_ref: (0, place(i, at_ref), 0)))
    else:
        given.append(done)
        specs.append(pl.BlockSpec(memory_space=pl.ANY))
        alias = {len(given): 0}
    return pl.pallas_call(
        functools.partial(_project, which=which),
        grid_spec=pltpu.PrefetchScalarGridSpec(
            num_scalar_prefetch=1, grid=(2 * n,), in_specs=specs, out_specs=out_specs,
            scratch_shapes=[pltpu.VMEM((4 * rows, width), jnp.bfloat16)],
        ),
        out_shape=out_shape,
        input_output_aliases=alias,
        compiler_params=pltpu.CompilerParams(dimension_semantics=("arbitrary",), vmem_limit_bytes=VMEM),
        cost_estimate=pl.CostEstimate(flops=4 * tokens * depth * width, transcendentals=0, bytes_accessed=4 * tokens * depth),
        name="project",
    )(at, *given)


def _weigh(scores, i, values, top_s, mix_s, ok=None):
    if ok is not None:
        least = scores.shape[0] - STRIP
        last = jnp.where(ok, scores[least:], HIDDEN)
        scores = jnp.concatenate([scores[:least], last], axis=0) if least else last
    old = top_s[i]
    top = jnp.maximum(old, scores.max(axis=0, keepdims=True))
    top_s[i] = top
    p = jnp.exp2((scores - top) * E).astype(jnp.bfloat16)
    mix_s[i] = mix_s[i] * jnp.exp2((old - top) * E) + _dot(values, p, 1, 0)


def _turn(v, at, to_s):
    to_s[:HEAD, pl.ds(at, v.shape[0])] = v.T
    to_s[HEAD:, pl.ds(at, v.shape[0])] = jnp.ones((8, v.shape[0]), jnp.bfloat16)


def _own(q_ref, k_ref, v_ref, o_ref, lse_ref, score_s, value_s, top_s, mix_s):
    bq = q_ref.shape[2]
    iq = pl.program_id(1)
    top_s[...] = jnp.full(top_s.shape, NEG, jnp.float32)
    mix_s[...] = jnp.zeros(mix_s.shape, jnp.float32)
    ok = lax.broadcasted_iota(jnp.int32, (STRIP, STRIP), 1) >= lax.broadcasted_iota(jnp.int32, (STRIP, STRIP), 0)
    head = lambda i: lax.rem(lax.div(i, 2), 2)
    strip = lambda i: lax.rem(i, 2) + 2 * (1 - lax.div(i, 4))
    rows = lambda s, size=STRIP: pl.ds(pl.multiple_of(s * STRIP, STRIP), size)
    queries = lambda i: q_ref[0, head(i), rows(strip(i)), :]
    keys = lambda j: pl.ds(pl.multiple_of(j * KEYS, KEYS), KEYS)

    @pl.when(iq == 0)
    def _():
        lax.fori_loop(0, k_ref.shape[2] // KEYS, lambda j, _: _turn(v_ref[0, 0, keys(j), :], pl.multiple_of(j * KEYS, KEYS), value_s), None)

    score = lambda j, i: _dot(k_ref[0, 0, keys(j), :], queries(i), 1, 1)
    groups = 2 * (bq // KEYS) * iq + 1
    score_s[0] = score(0, 0)

    def group(g, _):
        j, base = lax.div(g, 2), 4 * lax.rem(g, 2)
        for u in range(4):
            near = (j, base + u + 1) if u < 3 else (lax.div(jnp.minimum(g + 1, groups - 1), 2), lax.rem(base + 4, 8))
            score_s[(u + 1) % 2] = score(*near)
            _weigh(score_s[u % 2], base + u, value_s[:, keys(j)], top_s, mix_s)

    lax.fori_loop(0, groups, group, None)

    def pair(d, _):
        n, half = lax.div(d, 2), lax.rem(d, 2)
        i = 4 * (1 - half) + 2 * n
        at = pl.multiple_of((iq * (bq // KEYS) + half) * KEYS, KEYS)
        some, all_ = pl.ds(at, STRIP), pl.ds(at, KEYS)
        score_s[0, :STRIP] = _dot(k_ref[0, 0, some, :], queries(i), 1, 1)
        score_s[1] = _dot(k_ref[0, 0, all_, :], queries(i + 1), 1, 1)
        _weigh(score_s[0, :STRIP], i, value_s[:, some], top_s, mix_s, ok)
        _weigh(score_s[1], i + 1, value_s[:, all_], top_s, mix_s, ok)

    lax.fori_loop(0, 4, pair, None)

    for i in range(8):
        n, s = i // 2 % 2, i % 2 + 2 * (1 - i // 4)
        total = mix_s[i, HEAD : HEAD + 1, :]
        here = slice(s * STRIP, (s + 1) * STRIP)
        o_ref[0, n, :, here] = mix_s[i, :HEAD, :] * (1 / total)
        lse_ref[0, 0, n : n + 1, here] = top_s[i] * SCALE + jnp.log(total)


def attend_own(made):
    tokens = made.shape[2]
    bq = 2 * KEYS
    return pl.pallas_call(
        _own,
        grid=(2, tokens // bq),
        in_specs=[
            pl.BlockSpec((1, 2, bq, HEAD), lambda h, i: (2 * h, 0, i, 0)),
            pl.BlockSpec((1, 1, tokens, HEAD), lambda h, i: (2 * h + 1, 0, 0, 0)),
            pl.BlockSpec((1, 1, tokens, HEAD), lambda h, i: (2 * h + 1, 1, 0, 0)),
        ],
        out_specs=[
            pl.BlockSpec((1, 2, HEAD, bq), lambda h, i: (h, 0, 0, i)),
            pl.BlockSpec((1, 1, 2, bq), lambda h, i: (h, i, 0, 0)),
        ],
        out_shape=[jax.ShapeDtypeStruct((2, 2, HEAD, tokens), jnp.float32), jax.ShapeDtypeStruct((2, tokens // bq, 2, bq), jnp.float32)],
        scratch_shapes=[
            pltpu.VMEM((2, KEYS, STRIP), jnp.float32), pltpu.VMEM((HEAD + 8, tokens), jnp.bfloat16),
            pltpu.VMEM((8, 1, STRIP), jnp.float32), pltpu.VMEM((8, HEAD + 8, STRIP), jnp.float32),
        ],
        compiler_params=pltpu.CompilerParams(dimension_semantics=("arbitrary", "arbitrary"), vmem_limit_bytes=VMEM),
        cost_estimate=pl.CostEstimate(flops=8 * tokens * tokens * HEAD, transcendentals=2 * tokens * tokens, bytes_accessed=2 * made.size),
        name="attend_own",
    )(made, made, made)


def _cross(at_ref, came_ref, made_ref, own_ref, lse_in, o_ref, q_s, k_s, v_s, in_s, score_s, value_s, top_s, mix_s, sem, *, chunk):
    bq = o_ref.shape[3]
    tokens = k_s.shape[0]
    pieces = [(n, m) for n in range(2) for m in range(2)]
    count = tokens // KEYS
    first = at_ref[CHIP] == 0

    def queries(q_from):
        half = tokens // 2
        return [pltpu.make_async_copy(q_from.at[n, pl.ds(m * half + chunk * bq, bq), :], q_s.at[n, m], sem.at[2 * n + m]) for n, m in pieces]

    def keys(kv_from, b, n):
        rows = pl.ds(pl.multiple_of(b * KEYS, KEYS), KEYS)
        return pltpu.make_async_copy(kv_from.at[n, rows, :], (k_s, v_s)[n].at[rows, :], sem.at[4 + 2 * b + n])

    def start(q_from, kv_from):
        for copy in queries(q_from) + [keys(kv_from, b, n) for b in range(count) for n in range(2)]:
            copy.start()

    @pl.when(first)
    def _():
        start(came_ref, made_ref.at[1])

    @pl.when(jnp.logical_not(first))
    def _():
        start(made_ref.at[2], came_ref)

    carries = [
        pltpu.make_async_copy(own_ref.at[1, n, :, pl.ds(m * (tokens // 2) + chunk * bq, bq)], in_s.at[n, m], sem.at[4 + 2 * count + 2 * n + m])
        for n, m in pieces
    ]
    for copy in carries:
        copy.start()
    top_s[...] = jnp.full(top_s.shape, NEG, jnp.float32)
    mix_s[...] = jnp.zeros(mix_s.shape, jnp.float32)
    for copy in queries(came_ref) + [keys(came_ref, 0, 0)]:
        copy.wait()
    here = lambda b: pl.ds(pl.multiple_of(b * KEYS, KEYS), KEYS)
    score = lambda b, i: _dot(k_s[here(b), :], q_s[pieces[i]], 1, 1)
    score_s[0] = score(0, 0)

    def block(b, _):
        @pl.when(b + 1 < count)
        def _():
            keys(came_ref, b + 1, 0).wait()

        keys(came_ref, b, 1).wait()
        _turn(v_s[here(b), :], 0, value_s)
        for i in range(4):
            score_s[(i + 1) % 2] = score(b, i + 1) if i < 3 else score(jnp.minimum(b + 1, count - 1), 0)
            _weigh(score_s[i % 2], i, value_s[...], top_s, mix_s)

    lax.fori_loop(0, count, block, None)
    for copy in carries:
        copy.wait()
    for s, (n, m) in enumerate(pieces):
        top, total = top_s[s] * SCALE, mix_s[s, HEAD : HEAD + 1, :]
        before = jnp.where(first, NEG, lse_in[0, m, n : n + 1, :])
        most = jnp.maximum(top, before)
        wa, wb = jnp.exp(top - most), jnp.exp(before - most)
        whole = total * wa + wb
        scale = 1 / whole
        o_ref[n, m, :HEAD, :] = (mix_s[s, :HEAD, :] * (wa * scale) + in_s[n, m] * (wb * scale)).astype(o_ref.dtype)
        o_ref[n, m, HEAD:, :] = _apart(most + jnp.log(whole))


def _apart(row):
    rows = []
    for _ in range(3):
        rows.append(row.astype(jnp.bfloat16).astype(jnp.float32))
        row = row - rows[-1]
    return jnp.concatenate(rows + [jnp.zeros((13, row.shape[1]), jnp.float32)], axis=0).astype(jnp.bfloat16)


def _together(rows):
    wide = rows.astype(jnp.float32)
    return wide[0:1] + wide[1:2] + wide[2:3]


def attend_cross(at, came, made, own_o, own_lse, i):
    tokens = made.shape[2]
    half = tokens // 2
    bq = half // CHUNKS
    anywhere = pl.BlockSpec(memory_space=pl.ANY)
    return pl.pallas_call(
        functools.partial(_cross, chunk=i),
        grid_spec=pltpu.PrefetchScalarGridSpec(
            num_scalar_prefetch=1, grid=(1,),
            in_specs=[anywhere, anywhere, anywhere, pl.BlockSpec((1, 2, 2, bq), lambda g, at_ref: (1, 0, 0, i))],
            out_specs=pl.BlockSpec((2, 2, HEAD + 16, bq), lambda g, at_ref: (0, 0, 0, 0)),
            scratch_shapes=[
                pltpu.VMEM((2, 2, bq, HEAD), jnp.bfloat16), pltpu.VMEM((tokens, HEAD), jnp.bfloat16), pltpu.VMEM((tokens, HEAD), jnp.bfloat16),
                pltpu.VMEM((2, 2, HEAD, bq), jnp.float32), pltpu.VMEM((2, KEYS, STRIP), jnp.float32), pltpu.VMEM((HEAD + 8, KEYS), jnp.bfloat16),
                pltpu.VMEM((4, 1, STRIP), jnp.float32), pltpu.VMEM((4, HEAD + 8, STRIP), jnp.float32),
                pltpu.SemaphoreType.DMA((8 + 2 * (tokens // KEYS),)),
            ],
        ),
        out_shape=jax.ShapeDtypeStruct((2, 2, HEAD + 16, bq), jnp.bfloat16),
        compiler_params=pltpu.CompilerParams(dimension_semantics=("arbitrary",), vmem_limit_bytes=VMEM),
        cost_estimate=pl.CostEstimate(flops=16 * bq * tokens * HEAD, transcendentals=4 * bq * tokens, bytes_accessed=8 * tokens * HEAD),
        name="attend_cross",
    )(at, came, made, own_o, own_lse)


def _merge(at_ref, own_ref, lse_ref, far_ref, o_ref, keep_ref, give_ref):
    chip = at_ref[CHIP]
    t, n = pl.program_id(0), pl.program_id(1)

    def fill(to_ref):
        lse = lse_ref[0, 0, pl.ds(n, 1), :]
        far_lse = jnp.where(chip == 0, NEG, _together(far_ref[0, 0, HEAD:, :]))
        top = jnp.maximum(lse, far_lse)
        wa, wb = jnp.exp(lse - top), jnp.exp(far_lse - top)
        scale = 1 / (wa + wb)
        low = own_ref[0, 0] * (wa * scale) + far_ref[0, 0, :HEAD, :].astype(jnp.float32) * (wb * scale)
        high = jnp.where(chip == 0, own_ref[1, 0].astype(jnp.bfloat16), o_ref[0, 0, :HEAD, :])
        to_ref[0, 0] = low.astype(jnp.bfloat16).T
        to_ref[1, 0] = high.T

    @pl.when(t == 0)
    def _():
        fill(keep_ref)

    @pl.when(t == 1)
    def _():
        fill(give_ref)


def merge(at, own_o, own_lse, far, o, i):
    bq = o.shape[3]
    side = lambda t, at_ref: jnp.where(t == 0, at_ref[CORE], 1 - at_ref[CORE])
    part = pl.BlockSpec((1, 1, HEAD + 16, bq), lambda t, n, at_ref: (n, side(t, at_ref), 0, 0))
    return pl.pallas_call(
        _merge,
        grid_spec=pltpu.PrefetchScalarGridSpec(
            num_scalar_prefetch=1, grid=(2, 2),
            in_specs=[
                pl.BlockSpec((2, 1, HEAD, bq), lambda t, n, at_ref: (0, n, 0, side(t, at_ref) * CHUNKS + i)),
                pl.BlockSpec((1, 1, 2, bq), lambda t, n, at_ref: (0, side(t, at_ref), 0, i)),
                part, part,
            ],
            out_specs=[
                pl.BlockSpec((2, 1, bq, HEAD), lambda t, n, at_ref: (0, jnp.where(t == 0, n, 1), 0, 0)),
                pl.BlockSpec((2, 1, bq, HEAD), lambda t, n, at_ref: (0, jnp.where(t == 0, 0, n), 0, 0)),
            ],
        ),
        out_shape=[jax.ShapeDtypeStruct((2, 2, bq, HEAD), jnp.bfloat16)] * 2,
        compiler_params=pltpu.CompilerParams(dimension_semantics=("arbitrary", "arbitrary"), vmem_limit_bytes=VMEM),
        cost_estimate=pl.CostEstimate(flops=64 * bq * HEAD, transcendentals=0, bytes_accessed=64 * bq * HEAD),
        name="merge",
    )(at, own_o, own_lse, far, o)


def _output(at_ref, x_ref, w_own, w_sib, wx, wy, vx, vy, *rest, count):
    y_ref = rest[-1]
    chip, group = at_ref[CHIP], at_ref[GROUP]
    rows = y_ref.shape[0] // count
    for i in range(count):
        here = slice(i * rows, (i + 1) * rows)
        parts, weights = [], []
        for o_ref, w, from_x, from_y in ((rest[2 * i], w_own, wx, wy), (rest[2 * i + 1], w_sib, vx, vy)):
            parts += [o_ref[chip, 0], o_ref[chip, 1], o_ref[1 - chip, group], o_ref[1 - chip, 1 - group]]
            weights += [w[:HEAD, :], w[HEAD:, :], from_x[...], from_y[...]]
        y = _dot(jnp.concatenate(parts, axis=1), jnp.concatenate(weights, axis=0), 1, 0)
        y_ref[here, :] = (x_ref[here, :].astype(jnp.float32) + y).astype(y_ref.dtype)


def output(at, x, weights, results, first, done):
    count = len(results)
    rows, width = results[0][0].shape[2], x.shape[1]
    bn = 768
    part = pl.BlockSpec(results[0][0].shape, lambda j, at_ref: (0, 0, 0, 0))
    here = pl.BlockSpec((count * rows, bn), lambda j, at_ref: (first // count, j))
    given = [x, *weights] + [r for pair in results for r in pair]
    specs = [here] + [pl.BlockSpec((w.shape[0], bn), lambda j, at_ref: (0, j)) for w in weights] + [part] * (2 * count)
    alias = {}
    if done is not None:
        given.append(done)
        specs.append(pl.BlockSpec(memory_space=pl.ANY))
        alias = {len(given): 0}
    return pl.pallas_call(
        functools.partial(_output, count=count),
        grid_spec=pltpu.PrefetchScalarGridSpec(num_scalar_prefetch=1, grid=(width // bn,), in_specs=specs, out_specs=here),
        out_shape=jax.ShapeDtypeStruct(x.shape, jnp.bfloat16),
        input_output_aliases=alias,
        compiler_params=pltpu.CompilerParams(dimension_semantics=("arbitrary",), vmem_limit_bytes=VMEM),
        cost_estimate=pl.CostEstimate(flops=2 * count * rows * 8 * HEAD * width, transcendentals=0, bytes_accessed=16 * HEAD * width),
        name="output",
    )(at, *given)


def tables(place):
    half = HEAD // 2
    angle = place.astype(jnp.float32)[:, None] * THETA ** (-jnp.arange(half, dtype=jnp.float32) / half)
    return jnp.cos(angle), jnp.sin(angle)


def solution(mesh):
    def step(x, gain, wq, wk, wv, wo):
        own = x.shape[0]
        rank, group = lax.axis_index("sp"), lax.axis_index("dp")
        chip, core = rank // 2, rank % 2

        pick = lambda n, which: jnp.where(which == 0, ORDER[0][n], ORDER[1][n])
        at = jnp.stack([pick(n, chip) for n in range(4)] + [pick(n, 1 - chip) for n in range(4)] + [chip, core, group]).astype(jnp.int32)

        w_own, w_give = share(at, wq, wk, wv)
        w_sib = lax.ppermute(w_give, "sp", SIBLING)
        leaving = leave(at, w_own, w_sib)
        wx, wy = [], []
        for n in range(4):
            wx.append(lax.ppermute(leaving[n], "sp", ACROSS))
            wy.append(lax.ppermute(wx[n], "dp", GROUPS))

        a_own = normed(x, gain)
        a_sib = lax.ppermute(a_own, "sp", SIBLING)
        cos, sin = tables(chip * 2 * own + jnp.arange(2 * own))

        made, sent = None, None
        for n in range(4):
            got = project(at, a_own, a_sib, w_own, w_sib, wx[n], wy[n], cos, sin, n, made)
            made = got[0]
            if n == 0:
                sent = got[1]
        came = lax.ppermute(sent, "sp", ACROSS)

        wo_here, _ = lax.optimization_barrier((wo, sent))
        wo_half = lax.dynamic_slice_in_dim(wo_here, group * HEAD, HEAD, axis=0)
        ox = lax.ppermute(wo_half, "sp", ACROSS)
        oy = lax.ppermute(ox, "dp", GROUPS)
        wo_sib, ox_sib, oy_sib = (lax.ppermute(w, "sp", SIBLING) for w in (wo_here, ox, oy))
        weights = (wo, wo_sib, ox, oy, ox_sib, oy_sib)

        own_o, own_lse = attend_own(made)

        results = []
        for i in range(CHUNKS):
            o = attend_cross(at, came, made, own_o, own_lse, i)
            far = lax.ppermute(o, "sp", BACK)
            keep, give = merge(at, own_o, own_lse, far, o, i)
            results.append((keep, lax.ppermute(give, "sp", SIBLING)))
        y = output(at, x, weights, results[:-1], 0, None)
        y = output(at, x, weights, results[-1:], CHUNKS - 1, y)
        return y

    tokens, whole = P(("dp", "sp"), None), P("sp", None)
    return jax.shard_map(
        step,
        mesh=mesh,
        in_specs=(tokens, P(None), whole, whole, whole, whole),
        out_specs=tokens,
        check_vma=False,
    )
```

```python
import functools

import jax
import jax.numpy as jnp
from jax import lax
from jax.experimental import pallas as pl
from jax.experimental.pallas import tpu as pltpu
from jax.sharding import PartitionSpec as P


NEG = -1e30
HIDDEN = 2 * NEG
LOG2E = 1.4426950408889634
VMEM = 56 * 2**20
HEAD = 256
THETA = 10000
SCALE = HEAD**-0.5
E = SCALE * LOG2E
STRIP = 512
ROWS = 512
KEYS = 1024
CHUNKS = 4


SIBLING = [(0, 1), (1, 0), (2, 3), (3, 2)]
ACROSS = [(0, 2), (2, 0), (1, 3), (3, 1)]
BACK = [(0, 2), (1, 3)]
GROUPS = [(0, 1), (1, 0)]
ORDER = ((3, 1, 0, 2), (0, 2, 1, 3))
OTHERS, CHIP, CORE, GROUP = 4, 8, 9, 10


def _dot(a, b, ca, cb):
    return lax.dot_general(a, b, (((ca,), (cb,)), ((), ())), preferred_element_type=jnp.float32)


def _share(at_ref, *refs):
    for q_ref, k_ref, v_ref, to_ref in (refs[:3] + refs[6:7], refs[3:6] + refs[7:8]):
        to_ref[0] = q_ref[...]
        to_ref[1, :, :HEAD] = k_ref[...]
        to_ref[1, :, HEAD:] = v_ref[...]


def share(at, wq, wk, wv):
    rows = wq.shape[0]
    specs = []
    for mine in (True, False):
        at_block = lambda p, at_ref, mine=mine: (0, 2 * p + (at_ref[CORE] if mine else 1 - at_ref[CORE]))
        specs += [pl.BlockSpec((rows, 2 * HEAD), at_block), pl.BlockSpec((rows, HEAD), at_block), pl.BlockSpec((rows, HEAD), at_block)]
    out = pl.BlockSpec((2, rows, 2 * HEAD), lambda p, at_ref: (p, 0, 0))
    return pl.pallas_call(
        _share,
        grid_spec=pltpu.PrefetchScalarGridSpec(num_scalar_prefetch=1, grid=(2,), in_specs=specs, out_specs=[out, out]),
        out_shape=[jax.ShapeDtypeStruct((4, rows, 2 * HEAD), jnp.bfloat16)] * 2,
        compiler_params=pltpu.CompilerParams(dimension_semantics=("arbitrary",), vmem_limit_bytes=VMEM),
        cost_estimate=pl.CostEstimate(flops=1000, transcendentals=0, bytes_accessed=4 * wq.size * 2),
        name="share",
    )(at, wq, wk, wv, wq, wk, wv)


def _leave(at_ref, own_ref, sib_ref, *to_refs):
    for n, to_ref in enumerate(to_refs):
        slot = at_ref[OTHERS + n]

        @pl.when(at_ref[GROUP] == at_ref[CORE])
        def _():
            to_ref[...] = own_ref[slot]

        @pl.when(at_ref[GROUP] != at_ref[CORE])
        def _():
            to_ref[...] = sib_ref[slot]


def leave(at, w_own, w_sib):
    whole = pl.BlockSpec(w_own.shape, lambda i, at_ref: (0, 0, 0))
    out = pl.BlockSpec(w_own.shape[1:], lambda i, at_ref: (0, 0))
    return pl.pallas_call(
        _leave,
        grid_spec=pltpu.PrefetchScalarGridSpec(num_scalar_prefetch=1, grid=(1,), in_specs=[whole, whole], out_specs=[out] * 4),
        out_shape=[jax.ShapeDtypeStruct(w_own.shape[1:], jnp.bfloat16)] * 4,
        compiler_params=pltpu.CompilerParams(dimension_semantics=("arbitrary",), vmem_limit_bytes=VMEM),
        cost_estimate=pl.CostEstimate(flops=1000, transcendentals=0, bytes_accessed=6 * w_own.size),
        name="leave",
    )(at, w_own, w_sib)


def _normed(x_ref, gain_ref, a_ref):
    wide = x_ref[...].astype(jnp.float32)
    scale = lax.rsqrt(jnp.mean(wide * wide, -1, keepdims=True) + 1e-6)
    a_ref[...] = (wide * scale * gain_ref[...].astype(jnp.float32)).astype(jnp.bfloat16)


def normed(x, gain):
    rows, depth = x.shape
    block = pl.BlockSpec((256, depth), lambda i: (i, 0))
    return pl.pallas_call(
        _normed,
        grid=(rows // 256,),
        in_specs=[block, pl.BlockSpec((1, depth), lambda i: (0, 0))],
        out_specs=block,
        out_shape=jax.ShapeDtypeStruct(x.shape, jnp.bfloat16),
        compiler_params=pltpu.CompilerParams(dimension_semantics=("arbitrary",), vmem_limit_bytes=VMEM),
        cost_estimate=pl.CostEstimate(flops=8 * x.size, transcendentals=0, bytes_accessed=4 * x.size),
        name="normed",
    )(x, gain[None])


def _project(at_ref, a0_ref, a1_ref, own_ref, sib_ref, wx_ref, wy_ref, cos_ref, sin_ref, *rest, which):
    out_ref, sent_ref, w_s = rest if which == 0 else (rest[1], None, rest[2])
    slot, chip, core, group = at_ref[which], at_ref[CHIP], at_ref[CORE], at_ref[GROUP]
    i = pl.program_id(0)
    rows = own_ref.shape[1]

    @pl.when(i == 0)
    def _():
        here, there = 2 * rows * chip, 2 * rows * (1 - chip)
        for at, ref in ((here + rows * core, own_ref), (here + rows * (1 - core), sib_ref)):
            w_s[pl.ds(pl.multiple_of(at, 64), rows), :] = ref[0]
        for at, ref in ((there + rows * group, wx_ref), (there + rows * (1 - group), wy_ref)):
            w_s[pl.ds(pl.multiple_of(at, 64), rows), :] = ref[...]

    def part(a_ref):
        half = HEAD // 2

        def rows_from(r, _):
            here = pl.ds(pl.multiple_of(r * ROWS, ROWS), ROWS)
            t = _dot(a_ref[here, :], w_s[...], 1, 0).astype(jnp.bfloat16).astype(jnp.float32)
            cos, sin = cos_ref[here, :], sin_ref[here, :]
            for n in range(2):
                p, q = t[:, n * HEAD : n * HEAD + half], t[:, n * HEAD + half : (n + 1) * HEAD]
                u, v = p * cos - q * sin, q * cos + p * sin
                if n == 1:
                    u, v = jnp.where(slot % 2 == 0, u, p), jnp.where(slot % 2 == 0, v, q)
                got = jnp.concatenate([u, v], axis=1).astype(jnp.bfloat16)
                out_ref[0, n, here, :] = got
                if sent_ref is not None:
                    sent_ref[n, here, :] = got

        lax.fori_loop(0, a_ref.shape[0] // ROWS, rows_from, None)

    @pl.when(i < pl.num_programs(0) // 2)
    def _():
        part(a0_ref)

    @pl.when(i >= pl.num_programs(0) // 2)
    def _():
        part(a1_ref)


def project(at, a_own, a_sib, w_own, w_sib, wx, wy, cos, sin, which, done):
    tokens, depth = a_own.shape
    rows, width = wx.shape
    bm = 1024
    n = tokens // bm
    first = which == 0

    def place(i, at_ref):
        return jnp.where(i < n, at_ref[CORE] * n + i, (1 - at_ref[CORE]) * n + i - n)

    weights = pl.BlockSpec((1, rows, width), lambda i, at_ref: (at_ref[which], 0, 0))
    fetched = pl.BlockSpec((rows, width), lambda i, at_ref: (0, 0))
    table = pl.BlockSpec((bm, HEAD // 2), lambda i, at_ref: (place(i, at_ref), 0))
    specs = [
        pl.BlockSpec((bm, depth), lambda i, at_ref: (jnp.minimum(i, n - 1), 0)),
        pl.BlockSpec((bm, depth), lambda i, at_ref: (jnp.maximum(i - n, 0), 0)),
        weights, weights, fetched, fetched, table, table,
    ]
    given = [a_own, a_sib, w_own, w_sib, wx, wy, cos, sin]
    out_shape = [jax.ShapeDtypeStruct((4, 2, 2 * tokens, HEAD), jnp.bfloat16)]
    out_specs = [pl.BlockSpec((1, 2, bm, HEAD), lambda i, at_ref: (at_ref[which], 0, place(i, at_ref), 0))]
    alias = {}
    if first:
        out_shape.append(jax.ShapeDtypeStruct((2, 2 * tokens, HEAD), jnp.bfloat16))
        out_specs.append(pl.BlockSpec((2, bm, HEAD), lambda i, at_ref: (0, place(i, at_ref), 0)))
    else:
        given.append(done)
        specs.append(pl.BlockSpec(memory_space=pl.ANY))
        alias = {len(given): 0}
    return pl.pallas_call(
        functools.partial(_project, which=which),
        grid_spec=pltpu.PrefetchScalarGridSpec(
            num_scalar_prefetch=1, grid=(2 * n,), in_specs=specs, out_specs=out_specs,
            scratch_shapes=[pltpu.VMEM((4 * rows, width), jnp.bfloat16)],
        ),
        out_shape=out_shape,
        input_output_aliases=alias,
        compiler_params=pltpu.CompilerParams(dimension_semantics=("arbitrary",), vmem_limit_bytes=VMEM),
        cost_estimate=pl.CostEstimate(flops=4 * tokens * depth * width, transcendentals=0, bytes_accessed=4 * tokens * depth),
        name="project",
    )(at, *given)


def _weigh(scores, i, values, top_s, mix_s, ok=None):
    if ok is not None:
        least = scores.shape[0] - STRIP
        last = jnp.where(ok, scores[least:], HIDDEN)
        scores = jnp.concatenate([scores[:least], last], axis=0) if least else last
    old = top_s[i]
    top = jnp.maximum(old, scores.max(axis=0, keepdims=True))
    top_s[i] = top
    p = jnp.exp2((scores - top) * E).astype(jnp.bfloat16)
    mix_s[i] = mix_s[i] * jnp.exp2((old - top) * E) + _dot(values, p, 1, 0)


def _turn(v, at, to_s):
    to_s[:HEAD, pl.ds(at, v.shape[0])] = v.T
    to_s[HEAD:, pl.ds(at, v.shape[0])] = jnp.ones((8, v.shape[0]), jnp.bfloat16)


def _own(q_ref, k_ref, v_ref, o_ref, lse_ref, score_s, value_s, top_s, mix_s):
    bq = q_ref.shape[2]
    iq = pl.program_id(0)
    top_s[...] = jnp.full(top_s.shape, NEG, jnp.float32)
    mix_s[...] = jnp.zeros(mix_s.shape, jnp.float32)
    ok = lax.broadcasted_iota(jnp.int32, (STRIP, STRIP), 1) >= lax.broadcasted_iota(jnp.int32, (STRIP, STRIP), 0)
    head = lambda i: lax.rem(lax.div(i, 2), 2)
    strip = lambda i: lax.rem(i, 2) + 2 * (1 - lax.div(i, 4))
    rows = lambda s, size=STRIP: pl.ds(pl.multiple_of(s * STRIP, STRIP), size)
    queries = lambda i: q_ref[0, head(i), rows(strip(i)), :]
    keys = lambda j: pl.ds(pl.multiple_of(j * KEYS, KEYS), KEYS)

    @pl.when(iq == 0)
    def _():
        lax.fori_loop(0, k_ref.shape[2] // KEYS, lambda j, _: _turn(v_ref[0, 0, keys(j), :], pl.multiple_of(j * KEYS, KEYS), value_s), None)

    score = lambda j, i: _dot(k_ref[0, 0, keys(j), :], queries(i), 1, 1)
    groups = 2 * (bq // KEYS) * iq + 1
    score_s[0] = score(0, 0)

    def group(g, _):
        j, base = lax.div(g, 2), 4 * lax.rem(g, 2)
        for u in range(4):
            near = (j, base + u + 1) if u < 3 else (lax.div(jnp.minimum(g + 1, groups - 1), 2), lax.rem(base + 4, 8))
            score_s[(u + 1) % 2] = score(*near)
            _weigh(score_s[u % 2], base + u, value_s[:, keys(j)], top_s, mix_s)

    lax.fori_loop(0, groups, group, None)

    def pair(d, _):
        n, half = lax.div(d, 2), lax.rem(d, 2)
        i = 4 * (1 - half) + 2 * n
        at = pl.multiple_of((iq * (bq // KEYS) + half) * KEYS, KEYS)
        some, all_ = pl.ds(at, STRIP), pl.ds(at, KEYS)
        score_s[0, :STRIP] = _dot(k_ref[0, 0, some, :], queries(i), 1, 1)
        score_s[1] = _dot(k_ref[0, 0, all_, :], queries(i + 1), 1, 1)
        _weigh(score_s[0, :STRIP], i, value_s[:, some], top_s, mix_s, ok)
        _weigh(score_s[1], i + 1, value_s[:, all_], top_s, mix_s, ok)

    lax.fori_loop(0, 4, pair, None)

    def finish(i, _):
        total = mix_s[i, HEAD : HEAD + 1, :]
        o_ref[head(i), :, rows(strip(i))] = mix_s[i, :HEAD, :] * (1 / total)
        lse_ref[0, pl.ds(head(i), 1), rows(strip(i))] = top_s[i] * SCALE + jnp.log(total)

    lax.fori_loop(0, 8, finish, None)


def attend_own(made, h):
    tokens = made.shape[2]
    bq = 2 * KEYS
    return pl.pallas_call(
        _own,
        grid=(tokens // bq,),
        in_specs=[
            pl.BlockSpec((1, 2, bq, HEAD), lambda i: (2 * h, 0, i, 0)),
            pl.BlockSpec((1, 1, tokens, HEAD), lambda i: (2 * h + 1, 0, 0, 0)),
            pl.BlockSpec((1, 1, tokens, HEAD), lambda i: (2 * h + 1, 1, 0, 0)),
        ],
        out_specs=[pl.BlockSpec((2, HEAD, bq), lambda i: (0, 0, i)), pl.BlockSpec((1, 2, bq), lambda i: (i, 0, 0))],
        out_shape=[jax.ShapeDtypeStruct((2, HEAD, tokens), jnp.float32), jax.ShapeDtypeStruct((tokens // bq, 2, bq), jnp.float32)],
        scratch_shapes=[
            pltpu.VMEM((2, KEYS, STRIP), jnp.float32), pltpu.VMEM((HEAD + 8, tokens), jnp.bfloat16),
            pltpu.VMEM((8, 1, STRIP), jnp.float32), pltpu.VMEM((8, HEAD + 8, STRIP), jnp.float32),
        ],
        compiler_params=pltpu.CompilerParams(dimension_semantics=("arbitrary",), vmem_limit_bytes=VMEM),
        cost_estimate=pl.CostEstimate(flops=4 * tokens * tokens * HEAD, transcendentals=tokens * tokens, bytes_accessed=made.size),
        name="attend_own",
    )(made, made, made)


def _cross(at_ref, came_ref, made_ref, own_ref, lse_in, o_ref, q_s, k_s, v_s, in_s, score_s, value_s, top_s, mix_s, sem, *, chunk):
    bq = o_ref.shape[3]
    tokens = k_s.shape[0]
    pieces = [(n, m) for n in range(2) for m in range(2)]
    count = tokens // KEYS
    first = at_ref[CHIP] == 0

    def queries(q_from):
        half = tokens // 2
        return [pltpu.make_async_copy(q_from.at[n, pl.ds(m * half + chunk * bq, bq), :], q_s.at[n, m], sem.at[2 * n + m]) for n, m in pieces]

    def keys(kv_from, b, n):
        rows = pl.ds(pl.multiple_of(b * KEYS, KEYS), KEYS)
        return pltpu.make_async_copy(kv_from.at[n, rows, :], (k_s, v_s)[n].at[rows, :], sem.at[4 + 2 * b + n])

    def start(q_from, kv_from):
        for copy in queries(q_from) + [keys(kv_from, b, n) for b in range(count) for n in range(2)]:
            copy.start()

    @pl.when(first)
    def _():
        start(came_ref, made_ref.at[1])

    @pl.when(jnp.logical_not(first))
    def _():
        start(made_ref.at[2], came_ref)

    carries = [
        pltpu.make_async_copy(own_ref.at[n, :, pl.ds(m * (tokens // 2) + chunk * bq, bq)], in_s.at[n, m], sem.at[4 + 2 * count + 2 * n + m])
        for n, m in pieces
    ]
    for copy in carries:
        copy.start()
    top_s[...] = jnp.full(top_s.shape, NEG, jnp.float32)
    mix_s[...] = jnp.zeros(mix_s.shape, jnp.float32)
    for copy in queries(came_ref) + [keys(came_ref, 0, 0)]:
        copy.wait()
    here = lambda b: pl.ds(pl.multiple_of(b * KEYS, KEYS), KEYS)
    score = lambda b, i: _dot(k_s[here(b), :], q_s[pieces[i]], 1, 1)
    score_s[0] = score(0, 0)

    def block(b, _):
        @pl.when(b + 1 < count)
        def _():
            keys(came_ref, b + 1, 0).wait()

        keys(came_ref, b, 1).wait()
        _turn(v_s[here(b), :], 0, value_s)
        for i in range(4):
            score_s[(i + 1) % 2] = score(b, i + 1) if i < 3 else score(jnp.minimum(b + 1, count - 1), 0)
            _weigh(score_s[i % 2], i, value_s[...], top_s, mix_s)

    lax.fori_loop(0, count, block, None)
    for copy in carries:
        copy.wait()

    def finish(s, _):
        n, m = lax.div(s, 2), lax.rem(s, 2)
        top, total = top_s[s] * SCALE, mix_s[s, HEAD : HEAD + 1, :]
        before = jnp.where(first, NEG, lse_in[m, pl.ds(n, 1), :])
        most = jnp.maximum(top, before)
        wa, wb = jnp.exp(top - most), jnp.exp(before - most)
        whole = total * wa + wb
        scale = 1 / whole
        o_ref[n, m, :HEAD, :] = (mix_s[s, :HEAD, :] * (wa * scale) + in_s[n, m] * (wb * scale)).astype(o_ref.dtype)
        o_ref[n, m, HEAD:, :] = _apart(most + jnp.log(whole))

    lax.fori_loop(0, 4, finish, None)


def _apart(row):
    rows = []
    for _ in range(3):
        rows.append(row.astype(jnp.bfloat16).astype(jnp.float32))
        row = row - rows[-1]
    return jnp.concatenate(rows + [jnp.zeros((13, row.shape[1]), jnp.float32)], axis=0).astype(jnp.bfloat16)


def _together(rows):
    wide = rows.astype(jnp.float32)
    return wide[0:1] + wide[1:2] + wide[2:3]


def attend_cross(at, came, made, own_o, own_lse, i):
    tokens = made.shape[2]
    half = tokens // 2
    bq = half // CHUNKS
    anywhere = pl.BlockSpec(memory_space=pl.ANY)
    return pl.pallas_call(
        functools.partial(_cross, chunk=i),
        grid_spec=pltpu.PrefetchScalarGridSpec(
            num_scalar_prefetch=1, grid=(1,),
            in_specs=[anywhere, anywhere, anywhere, pl.BlockSpec((2, 2, bq), lambda g, at_ref: (0, 0, i))],
            out_specs=pl.BlockSpec((2, 2, HEAD + 16, bq), lambda g, at_ref: (0, 0, 0, 0)),
            scratch_shapes=[
                pltpu.VMEM((2, 2, bq, HEAD), jnp.bfloat16), pltpu.VMEM((tokens, HEAD), jnp.bfloat16), pltpu.VMEM((tokens, HEAD), jnp.bfloat16),
                pltpu.VMEM((2, 2, HEAD, bq), jnp.float32), pltpu.VMEM((2, KEYS, STRIP), jnp.float32), pltpu.VMEM((HEAD + 8, KEYS), jnp.bfloat16),
                pltpu.VMEM((4, 1, STRIP), jnp.float32), pltpu.VMEM((4, HEAD + 8, STRIP), jnp.float32),
                pltpu.SemaphoreType.DMA((8 + 2 * (tokens // KEYS),)),
            ],
        ),
        out_shape=jax.ShapeDtypeStruct((2, 2, HEAD + 16, bq), jnp.bfloat16),
        compiler_params=pltpu.CompilerParams(dimension_semantics=("arbitrary",), vmem_limit_bytes=VMEM),
        cost_estimate=pl.CostEstimate(flops=16 * bq * tokens * HEAD, transcendentals=4 * bq * tokens, bytes_accessed=8 * tokens * HEAD),
        name="attend_cross",
    )(at, came, made, own_o, own_lse)


def _merge(at_ref, low_ref, lse_ref, high_ref, far_ref, o_ref, keep_ref, give_ref):
    chip = at_ref[CHIP]
    t, n = pl.program_id(0), pl.program_id(1)

    def fill(to_ref):
        lse = lse_ref[0, pl.ds(n, 1), :]
        far_lse = jnp.where(chip == 0, NEG, _together(far_ref[0, 0, HEAD:, :]))
        top = jnp.maximum(lse, far_lse)
        wa, wb = jnp.exp(lse - top), jnp.exp(far_lse - top)
        scale = 1 / (wa + wb)
        low = low_ref[0] * (wa * scale) + far_ref[0, 0, :HEAD, :].astype(jnp.float32) * (wb * scale)
        high = jnp.where(chip == 0, high_ref[0].astype(jnp.bfloat16), o_ref[0, 0, :HEAD, :])
        to_ref[0, 0] = low.astype(jnp.bfloat16).T
        to_ref[1, 0] = high.T

    @pl.when(t == 0)
    def _():
        fill(keep_ref)

    @pl.when(t == 1)
    def _():
        fill(give_ref)


def merge(at, low, low_lse, high, far, o, i):
    bq = o.shape[3]
    side = lambda t, at_ref: jnp.where(t == 0, at_ref[CORE], 1 - at_ref[CORE])
    mine = pl.BlockSpec((1, HEAD, bq), lambda t, n, at_ref: (n, 0, side(t, at_ref) * CHUNKS + i))
    part = pl.BlockSpec((1, 1, HEAD + 16, bq), lambda t, n, at_ref: (n, side(t, at_ref), 0, 0))
    return pl.pallas_call(
        _merge,
        grid_spec=pltpu.PrefetchScalarGridSpec(
            num_scalar_prefetch=1, grid=(2, 2),
            in_specs=[
                mine, pl.BlockSpec((1, 2, bq), lambda t, n, at_ref: (side(t, at_ref), 0, i)), mine, part, part,
            ],
            out_specs=[
                pl.BlockSpec((2, 1, bq, HEAD), lambda t, n, at_ref: (0, jnp.where(t == 0, n, 1), 0, 0)),
                pl.BlockSpec((2, 1, bq, HEAD), lambda t, n, at_ref: (0, jnp.where(t == 0, 0, n), 0, 0)),
            ],
        ),
        out_shape=[jax.ShapeDtypeStruct((2, 2, bq, HEAD), jnp.bfloat16)] * 2,
        compiler_params=pltpu.CompilerParams(dimension_semantics=("arbitrary", "arbitrary"), vmem_limit_bytes=VMEM),
        cost_estimate=pl.CostEstimate(flops=64 * bq * HEAD, transcendentals=0, bytes_accessed=64 * bq * HEAD),
        name="merge",
    )(at, low, low_lse, high, far, o)


def _output(at_ref, x_ref, w_own, w_sib, wx, wy, vx, vy, *rest, count):
    y_ref = rest[-1]
    chip, group = at_ref[CHIP], at_ref[GROUP]
    rows = y_ref.shape[0] // count
    for i in range(count):
        here = slice(i * rows, (i + 1) * rows)
        parts, weights = [], []
        for o_ref, w, from_x, from_y in ((rest[2 * i], w_own, wx, wy), (rest[2 * i + 1], w_sib, vx, vy)):
            parts += [o_ref[chip, 0], o_ref[chip, 1], o_ref[1 - chip, group], o_ref[1 - chip, 1 - group]]
            weights += [w[:HEAD, :], w[HEAD:, :], from_x[...], from_y[...]]
        y = _dot(jnp.concatenate(parts, axis=1), jnp.concatenate(weights, axis=0), 1, 0)
        y_ref[here, :] = (x_ref[here, :].astype(jnp.float32) + y).astype(y_ref.dtype)


def output(at, x, weights, results, first, done):
    count = len(results)
    rows, width = results[0][0].shape[2], x.shape[1]
    bn = 768
    part = pl.BlockSpec(results[0][0].shape, lambda j, at_ref: (0, 0, 0, 0))
    here = pl.BlockSpec((count * rows, bn), lambda j, at_ref: (first // count, j))
    given = [x, *weights] + [r for pair in results for r in pair]
    specs = [here] + [pl.BlockSpec((w.shape[0], bn), lambda j, at_ref: (0, j)) for w in weights] + [part] * (2 * count)
    alias = {}
    if done is not None:
        given.append(done)
        specs.append(pl.BlockSpec(memory_space=pl.ANY))
        alias = {len(given): 0}
    return pl.pallas_call(
        functools.partial(_output, count=count),
        grid_spec=pltpu.PrefetchScalarGridSpec(num_scalar_prefetch=1, grid=(width // bn,), in_specs=specs, out_specs=here),
        out_shape=jax.ShapeDtypeStruct(x.shape, jnp.bfloat16),
        input_output_aliases=alias,
        compiler_params=pltpu.CompilerParams(dimension_semantics=("arbitrary",), vmem_limit_bytes=VMEM),
        cost_estimate=pl.CostEstimate(flops=2 * count * rows * 8 * HEAD * width, transcendentals=0, bytes_accessed=16 * HEAD * width),
        name="output",
    )(at, *given)


def tables(place):
    half = HEAD // 2
    angle = place.astype(jnp.float32)[:, None] * THETA ** (-jnp.arange(half, dtype=jnp.float32) / half)
    return jnp.cos(angle), jnp.sin(angle)


def solution(mesh):
    def step(x, gain, wq, wk, wv, wo):
        own = x.shape[0]
        rank, group = lax.axis_index("sp"), lax.axis_index("dp")
        chip, core = rank // 2, rank % 2

        pick = lambda n, which: jnp.where(which == 0, ORDER[0][n], ORDER[1][n])
        at = jnp.stack([pick(n, chip) for n in range(4)] + [pick(n, 1 - chip) for n in range(4)] + [chip, core, group]).astype(jnp.int32)

        w_own, w_give = share(at, wq, wk, wv)
        w_sib = lax.ppermute(w_give, "sp", SIBLING)
        leaving = leave(at, w_own, w_sib)
        wx, wy = [], []
        for n in range(4):
            wx.append(lax.ppermute(leaving[n], "sp", ACROSS))
            wy.append(lax.ppermute(wx[n], "dp", GROUPS))

        a_own = normed(x, gain)
        a_sib = lax.ppermute(a_own, "sp", SIBLING)
        cos, sin = tables(chip * 2 * own + jnp.arange(2 * own))

        made, sent = None, None
        for n in range(4):
            got = project(at, a_own, a_sib, w_own, w_sib, wx[n], wy[n], cos, sin, n, made)
            made = got[0]
            if n == 0:
                sent = got[1]
        came = lax.ppermute(sent, "sp", ACROSS)

        wo_here, _ = lax.optimization_barrier((wo, sent))
        wo_half = lax.dynamic_slice_in_dim(wo_here, group * HEAD, HEAD, axis=0)
        ox = lax.ppermute(wo_half, "sp", ACROSS)
        oy = lax.ppermute(ox, "dp", GROUPS)
        wo_sib, ox_sib, oy_sib = (lax.ppermute(w, "sp", SIBLING) for w in (wo_here, ox, oy))
        weights = (wo, wo_sib, ox, oy, ox_sib, oy_sib)

        high, high_lse = attend_own(made, 1)
        parts = []
        for i in range(CHUNKS):
            o = attend_cross(at, came, made, high, high_lse, i)
            parts.append((lax.ppermute(o, "sp", BACK), o))
        low, low_lse = attend_own(made, 0)
        results = []
        for i in range(CHUNKS):
            keep, give = merge(at, low, low_lse, high, *parts[i], i)
            results.append((keep, lax.ppermute(give, "sp", SIBLING)))
        y = output(at, x, weights, results[:-1], 0, None)
        y = output(at, x, weights, results[-1:], CHUNKS - 1, y)
        return y

    tokens, whole = P(("dp", "sp"), None), P("sp", None)
    return jax.shard_map(
        step,
        mesh=mesh,
        in_specs=(tokens, P(None), whole, whole, whole, whole),
        out_specs=tokens,
        check_vma=False,
    )
```

```python
import functools

import jax
import jax.numpy as jnp
from jax import lax
from jax.experimental import pallas as pl
from jax.experimental.pallas import tpu as pltpu
from jax.sharding import PartitionSpec as P


NEG = -1e30
HIDDEN = 2 * NEG
LOG2E = 1.4426950408889634
VMEM = 56 * 2**20
HEAD = 256
THETA = 10000
SCALE = HEAD**-0.5
E = SCALE * LOG2E
STRIP = 512
ROWS = 512
KEYS = 1024
CHUNKS = 4


SIBLING = [(0, 1), (1, 0), (2, 3), (3, 2)]
ACROSS = [(0, 2), (2, 0), (1, 3), (3, 1)]
BACK = [(0, 2), (1, 3)]
GROUPS = [(0, 1), (1, 0)]
ORDER = ((3, 1, 0, 2), (0, 2, 1, 3))
OTHERS, CHIP, CORE, GROUP = 4, 8, 9, 10


def _dot(a, b, ca, cb):
    return lax.dot_general(a, b, (((ca,), (cb,)), ((), ())), preferred_element_type=jnp.float32)


def _share(at_ref, *refs):
    for q_ref, k_ref, v_ref, to_ref in (refs[:3] + refs[6:7], refs[3:6] + refs[7:8]):
        to_ref[0] = q_ref[...]
        to_ref[1, :, :HEAD] = k_ref[...]
        to_ref[1, :, HEAD:] = v_ref[...]


def share(at, wq, wk, wv):
    rows = wq.shape[0]
    specs = []
    for mine in (True, False):
        at_block = lambda p, at_ref, mine=mine: (0, 2 * p + (at_ref[CORE] if mine else 1 - at_ref[CORE]))
        specs += [pl.BlockSpec((rows, 2 * HEAD), at_block), pl.BlockSpec((rows, HEAD), at_block), pl.BlockSpec((rows, HEAD), at_block)]
    out = pl.BlockSpec((2, rows, 2 * HEAD), lambda p, at_ref: (p, 0, 0))
    return pl.pallas_call(
        _share,
        grid_spec=pltpu.PrefetchScalarGridSpec(num_scalar_prefetch=1, grid=(2,), in_specs=specs, out_specs=[out, out]),
        out_shape=[jax.ShapeDtypeStruct((4, rows, 2 * HEAD), jnp.bfloat16)] * 2,
        compiler_params=pltpu.CompilerParams(dimension_semantics=("arbitrary",), vmem_limit_bytes=VMEM),
        cost_estimate=pl.CostEstimate(flops=1000, transcendentals=0, bytes_accessed=4 * wq.size * 2),
        name="share",
    )(at, wq, wk, wv, wq, wk, wv)


def _leave(at_ref, own_ref, sib_ref, *to_refs):
    for n, to_ref in enumerate(to_refs):
        slot = at_ref[OTHERS + n]

        @pl.when(at_ref[GROUP] == at_ref[CORE])
        def _():
            to_ref[...] = own_ref[slot]

        @pl.when(at_ref[GROUP] != at_ref[CORE])
        def _():
            to_ref[...] = sib_ref[slot]


def leave(at, w_own, w_sib):
    whole = pl.BlockSpec(w_own.shape, lambda i, at_ref: (0, 0, 0))
    out = pl.BlockSpec(w_own.shape[1:], lambda i, at_ref: (0, 0))
    return pl.pallas_call(
        _leave,
        grid_spec=pltpu.PrefetchScalarGridSpec(num_scalar_prefetch=1, grid=(1,), in_specs=[whole, whole], out_specs=[out] * 4),
        out_shape=[jax.ShapeDtypeStruct(w_own.shape[1:], jnp.bfloat16)] * 4,
        compiler_params=pltpu.CompilerParams(dimension_semantics=("arbitrary",), vmem_limit_bytes=VMEM),
        cost_estimate=pl.CostEstimate(flops=1000, transcendentals=0, bytes_accessed=6 * w_own.size),
        name="leave",
    )(at, w_own, w_sib)


def _normed(x_ref, gain_ref, a_ref):
    wide = x_ref[...].astype(jnp.float32)
    scale = lax.rsqrt(jnp.mean(wide * wide, -1, keepdims=True) + 1e-6)
    a_ref[...] = (wide * scale * gain_ref[...].astype(jnp.float32)).astype(jnp.bfloat16)


def normed(x, gain):
    rows, depth = x.shape
    block = pl.BlockSpec((512, depth), lambda i: (i, 0))
    return pl.pallas_call(
        _normed,
        grid=(rows // 512,),
        in_specs=[block, pl.BlockSpec((1, depth), lambda i: (0, 0))],
        out_specs=block,
        out_shape=jax.ShapeDtypeStruct(x.shape, jnp.bfloat16),
        compiler_params=pltpu.CompilerParams(dimension_semantics=("arbitrary",), vmem_limit_bytes=VMEM),
        cost_estimate=pl.CostEstimate(flops=8 * x.size, transcendentals=0, bytes_accessed=4 * x.size),
        name="normed",
    )(x, gain[None])


def _project(at_ref, a0_ref, a1_ref, own_ref, sib_ref, wx_ref, wy_ref, cos_ref, sin_ref, *rest, which):
    out_ref, sent_ref, w_s = rest if which == 0 else (rest[1], None, rest[2])
    slot, chip, core, group = at_ref[which], at_ref[CHIP], at_ref[CORE], at_ref[GROUP]
    i = pl.program_id(0)
    rows = own_ref.shape[1]

    @pl.when(i == 0)
    def _():
        here, there = 2 * rows * chip, 2 * rows * (1 - chip)
        for at, ref in ((here + rows * core, own_ref), (here + rows * (1 - core), sib_ref)):
            w_s[pl.ds(pl.multiple_of(at, 64), rows), :] = ref[0]
        for at, ref in ((there + rows * group, wx_ref), (there + rows * (1 - group), wy_ref)):
            w_s[pl.ds(pl.multiple_of(at, 64), rows), :] = ref[...]

    def part(a_ref):
        half = HEAD // 2

        def rows_from(r, _):
            here = pl.ds(pl.multiple_of(r * ROWS, ROWS), ROWS)
            t = _dot(a_ref[here, :], w_s[...], 1, 0).astype(jnp.bfloat16).astype(jnp.float32)
            cos, sin = cos_ref[here, :], sin_ref[here, :]
            for n in range(2):
                p, q = t[:, n * HEAD : n * HEAD + half], t[:, n * HEAD + half : (n + 1) * HEAD]
                u, v = p * cos - q * sin, q * cos + p * sin
                if n == 1:
                    u, v = jnp.where(slot % 2 == 0, u, p), jnp.where(slot % 2 == 0, v, q)
                got = jnp.concatenate([u, v], axis=1).astype(jnp.bfloat16)
                out_ref[0, n, here, :] = got
                if sent_ref is not None:
                    sent_ref[n, here, :] = got

        lax.fori_loop(0, a_ref.shape[0] // ROWS, rows_from, None)

    @pl.when(i < pl.num_programs(0) // 2)
    def _():
        part(a0_ref)

    @pl.when(i >= pl.num_programs(0) // 2)
    def _():
        part(a1_ref)


def project(at, a_own, a_sib, w_own, w_sib, wx, wy, cos, sin, which, done):
    tokens, depth = a_own.shape
    rows, width = wx.shape
    bm = 1024
    n = tokens // bm
    first = which == 0

    def place(i, at_ref):
        return jnp.where(i < n, at_ref[CORE] * n + i, (1 - at_ref[CORE]) * n + i - n)

    weights = pl.BlockSpec((1, rows, width), lambda i, at_ref: (at_ref[which], 0, 0))
    fetched = pl.BlockSpec((rows, width), lambda i, at_ref: (0, 0))
    table = pl.BlockSpec((bm, HEAD // 2), lambda i, at_ref: (place(i, at_ref), 0))
    specs = [
        pl.BlockSpec((bm, depth), lambda i, at_ref: (jnp.minimum(i, n - 1), 0)),
        pl.BlockSpec((bm, depth), lambda i, at_ref: (jnp.maximum(i - n, 0), 0)),
        weights, weights, fetched, fetched, table, table,
    ]
    given = [a_own, a_sib, w_own, w_sib, wx, wy, cos, sin]
    out_shape = [jax.ShapeDtypeStruct((4, 2, 2 * tokens, HEAD), jnp.bfloat16)]
    out_specs = [pl.BlockSpec((1, 2, bm, HEAD), lambda i, at_ref: (at_ref[which], 0, place(i, at_ref), 0))]
    alias = {}
    if first:
        out_shape.append(jax.ShapeDtypeStruct((2, 2 * tokens, HEAD), jnp.bfloat16))
        out_specs.append(pl.BlockSpec((2, bm, HEAD), lambda i, at_ref: (0, place(i, at_ref), 0)))
    else:
        given.append(done)
        specs.append(pl.BlockSpec(memory_space=pl.ANY))
        alias = {len(given): 0}
    return pl.pallas_call(
        functools.partial(_project, which=which),
        grid_spec=pltpu.PrefetchScalarGridSpec(
            num_scalar_prefetch=1, grid=(2 * n,), in_specs=specs, out_specs=out_specs,
            scratch_shapes=[pltpu.VMEM((4 * rows, width), jnp.bfloat16)],
        ),
        out_shape=out_shape,
        input_output_aliases=alias,
        compiler_params=pltpu.CompilerParams(dimension_semantics=("arbitrary",), vmem_limit_bytes=VMEM),
        cost_estimate=pl.CostEstimate(flops=4 * tokens * depth * width, transcendentals=0, bytes_accessed=4 * tokens * depth),
        name="project",
    )(at, *given)


def _weigh(scores, i, values, top_s, mix_s, ok=None):
    if ok is not None:
        least = scores.shape[0] - STRIP
        last = jnp.where(ok, scores[least:], HIDDEN)
        scores = jnp.concatenate([scores[:least], last], axis=0) if least else last
    old = top_s[i]
    top = jnp.maximum(old, scores.max(axis=0, keepdims=True))
    top_s[i] = top
    p = jnp.exp2((scores - top) * E).astype(jnp.bfloat16)
    mix_s[i] = mix_s[i] * jnp.exp2((old - top) * E) + _dot(values, p, 1, 0)


def _turn(v, at, to_s):
    to_s[:HEAD, pl.ds(at, v.shape[0])] = v.T
    to_s[HEAD:, pl.ds(at, v.shape[0])] = jnp.ones((8, v.shape[0]), jnp.bfloat16)


def _own(q_ref, k_ref, v_ref, o_ref, lse_ref, score_s, value_s, top_s, mix_s):
    bq = q_ref.shape[2]
    iq = pl.program_id(0)
    top_s[...] = jnp.full(top_s.shape, NEG, jnp.float32)
    mix_s[...] = jnp.zeros(mix_s.shape, jnp.float32)
    ok = lax.broadcasted_iota(jnp.int32, (STRIP, STRIP), 1) >= lax.broadcasted_iota(jnp.int32, (STRIP, STRIP), 0)
    head = lambda i: lax.rem(lax.div(i, 2), 2)
    strip = lambda i: lax.rem(i, 2) + 2 * (1 - lax.div(i, 4))
    rows = lambda s, size=STRIP: pl.ds(pl.multiple_of(s * STRIP, STRIP), size)
    queries = lambda i: q_ref[0, head(i), rows(strip(i)), :]
    keys = lambda j: pl.ds(pl.multiple_of(j * KEYS, KEYS), KEYS)

    @pl.when(iq == 0)
    def _():
        lax.fori_loop(0, k_ref.shape[2] // KEYS, lambda j, _: _turn(v_ref[0, 0, keys(j), :], pl.multiple_of(j * KEYS, KEYS), value_s), None)

    score = lambda j, i: _dot(k_ref[0, 0, keys(j), :], queries(i), 1, 1)
    groups = 2 * (bq // KEYS) * iq + 1
    score_s[0] = score(0, 0)

    def group(g, _):
        j, base = lax.div(g, 2), 4 * lax.rem(g, 2)
        for u in range(4):
            near = (j, base + u + 1) if u < 3 else (lax.div(jnp.minimum(g + 1, groups - 1), 2), lax.rem(base + 4, 8))
            score_s[(u + 1) % 2] = score(*near)
            _weigh(score_s[u % 2], base + u, value_s[:, keys(j)], top_s, mix_s)

    lax.fori_loop(0, groups, group, None)

    def pair(d, _):
        n, half = lax.div(d, 2), lax.rem(d, 2)
        i = 4 * (1 - half) + 2 * n
        at = pl.multiple_of((iq * (bq // KEYS) + half) * KEYS, KEYS)
        some, all_ = pl.ds(at, STRIP), pl.ds(at, KEYS)
        score_s[0, :STRIP] = _dot(k_ref[0, 0, some, :], queries(i), 1, 1)
        score_s[1] = _dot(k_ref[0, 0, all_, :], queries(i + 1), 1, 1)
        _weigh(score_s[0, :STRIP], i, value_s[:, some], top_s, mix_s, ok)
        _weigh(score_s[1], i + 1, value_s[:, all_], top_s, mix_s, ok)

    lax.fori_loop(0, 4, pair, None)

    def finish(i, _):
        total = mix_s[i, HEAD : HEAD + 1, :]
        o_ref[head(i), :, rows(strip(i))] = mix_s[i, :HEAD, :] * (1 / total)
        lse_ref[0, pl.ds(head(i), 1), rows(strip(i))] = top_s[i] * SCALE + jnp.log(total)

    lax.fori_loop(0, 8, finish, None)


def attend_own(made, h):
    tokens = made.shape[2]
    bq = 2 * KEYS
    return pl.pallas_call(
        _own,
        grid=(tokens // bq,),
        in_specs=[
            pl.BlockSpec((1, 2, bq, HEAD), lambda i: (2 * h, 0, i, 0)),
            pl.BlockSpec((1, 1, tokens, HEAD), lambda i: (2 * h + 1, 0, 0, 0)),
            pl.BlockSpec((1, 1, tokens, HEAD), lambda i: (2 * h + 1, 1, 0, 0)),
        ],
        out_specs=[pl.BlockSpec((2, HEAD, bq), lambda i: (0, 0, i)), pl.BlockSpec((1, 2, bq), lambda i: (i, 0, 0))],
        out_shape=[jax.ShapeDtypeStruct((2, HEAD, tokens), jnp.float32), jax.ShapeDtypeStruct((tokens // bq, 2, bq), jnp.float32)],
        scratch_shapes=[
            pltpu.VMEM((2, KEYS, STRIP), jnp.float32), pltpu.VMEM((HEAD + 8, tokens), jnp.bfloat16),
            pltpu.VMEM((8, 1, STRIP), jnp.float32), pltpu.VMEM((8, HEAD + 8, STRIP), jnp.float32),
        ],
        compiler_params=pltpu.CompilerParams(dimension_semantics=("arbitrary",), vmem_limit_bytes=VMEM),
        cost_estimate=pl.CostEstimate(flops=4 * tokens * tokens * HEAD, transcendentals=tokens * tokens, bytes_accessed=made.size),
        name="attend_own",
    )(made, made, made)


def _cross(at_ref, came_ref, made_ref, own_ref, lse_in, o_ref, q_s, k_s, v_s, in_s, score_s, value_s, top_s, mix_s, sem, *, chunk):
    bq = o_ref.shape[3]
    tokens = k_s.shape[0]
    pieces = [(n, m) for n in range(2) for m in range(2)]
    count = tokens // KEYS
    first = at_ref[CHIP] == 0

    def queries(q_from):
        half = tokens // 2
        return [pltpu.make_async_copy(q_from.at[n, pl.ds(m * half + chunk * bq, bq), :], q_s.at[n, m], sem.at[2 * n + m]) for n, m in pieces]

    def keys(kv_from, b, n):
        rows = pl.ds(pl.multiple_of(b * KEYS, KEYS), KEYS)
        return pltpu.make_async_copy(kv_from.at[n, rows, :], (k_s, v_s)[n].at[rows, :], sem.at[4 + 2 * b + n])

    def start(q_from, kv_from):
        for copy in queries(q_from) + [keys(kv_from, b, n) for b in range(count) for n in range(2)]:
            copy.start()

    @pl.when(first)
    def _():
        start(came_ref, made_ref.at[1])

    @pl.when(jnp.logical_not(first))
    def _():
        start(made_ref.at[2], came_ref)

    carries = [
        pltpu.make_async_copy(own_ref.at[n, :, pl.ds(m * (tokens // 2) + chunk * bq, bq)], in_s.at[n, m], sem.at[4 + 2 * count + 2 * n + m])
        for n, m in pieces
    ]
    for copy in carries:
        copy.start()
    top_s[...] = jnp.full(top_s.shape, NEG, jnp.float32)
    mix_s[...] = jnp.zeros(mix_s.shape, jnp.float32)
    for copy in queries(came_ref) + [keys(came_ref, 0, 0)]:
        copy.wait()
    here = lambda b: pl.ds(pl.multiple_of(b * KEYS, KEYS), KEYS)
    score = lambda b, i: _dot(k_s[here(b), :], q_s[pieces[i]], 1, 1)
    score_s[0] = score(0, 0)

    def block(b, _):
        @pl.when(b + 1 < count)
        def _():
            keys(came_ref, b + 1, 0).wait()

        keys(came_ref, b, 1).wait()
        _turn(v_s[here(b), :], 0, value_s)
        for i in range(4):
            score_s[(i + 1) % 2] = score(b, i + 1) if i < 3 else score(jnp.minimum(b + 1, count - 1), 0)
            _weigh(score_s[i % 2], i, value_s[...], top_s, mix_s)

    lax.fori_loop(0, count, block, None)
    for copy in carries:
        copy.wait()

    def finish(s, _):
        n, m = lax.div(s, 2), lax.rem(s, 2)
        top, total = top_s[s] * SCALE, mix_s[s, HEAD : HEAD + 1, :]
        before = jnp.where(first, NEG, lse_in[m, pl.ds(n, 1), :])
        most = jnp.maximum(top, before)
        wa, wb = jnp.exp(top - most), jnp.exp(before - most)
        whole = total * wa + wb
        scale = 1 / whole
        o_ref[n, m, :HEAD, :] = (mix_s[s, :HEAD, :] * (wa * scale) + in_s[n, m] * (wb * scale)).astype(o_ref.dtype)
        o_ref[n, m, HEAD:, :] = _apart(most + jnp.log(whole))

    lax.fori_loop(0, 4, finish, None)


def _apart(row):
    rows = []
    for _ in range(3):
        rows.append(row.astype(jnp.bfloat16).astype(jnp.float32))
        row = row - rows[-1]
    return jnp.concatenate(rows + [jnp.zeros((13, row.shape[1]), jnp.float32)], axis=0).astype(jnp.bfloat16)


def _together(rows):
    wide = rows.astype(jnp.float32)
    return wide[0:1] + wide[1:2] + wide[2:3]


def attend_cross(at, came, made, own_o, own_lse, i):
    tokens = made.shape[2]
    half = tokens // 2
    bq = half // CHUNKS
    anywhere = pl.BlockSpec(memory_space=pl.ANY)
    return pl.pallas_call(
        functools.partial(_cross, chunk=i),
        grid_spec=pltpu.PrefetchScalarGridSpec(
            num_scalar_prefetch=1, grid=(1,),
            in_specs=[anywhere, anywhere, anywhere, pl.BlockSpec((2, 2, bq), lambda g, at_ref: (0, 0, i))],
            out_specs=pl.BlockSpec((2, 2, HEAD + 16, bq), lambda g, at_ref: (0, 0, 0, 0)),
            scratch_shapes=[
                pltpu.VMEM((2, 2, bq, HEAD), jnp.bfloat16), pltpu.VMEM((tokens, HEAD), jnp.bfloat16), pltpu.VMEM((tokens, HEAD), jnp.bfloat16),
                pltpu.VMEM((2, 2, HEAD, bq), jnp.float32), pltpu.VMEM((2, KEYS, STRIP), jnp.float32), pltpu.VMEM((HEAD + 8, KEYS), jnp.bfloat16),
                pltpu.VMEM((4, 1, STRIP), jnp.float32), pltpu.VMEM((4, HEAD + 8, STRIP), jnp.float32),
                pltpu.SemaphoreType.DMA((8 + 2 * (tokens // KEYS),)),
            ],
        ),
        out_shape=jax.ShapeDtypeStruct((2, 2, HEAD + 16, bq), jnp.bfloat16),
        compiler_params=pltpu.CompilerParams(dimension_semantics=("arbitrary",), vmem_limit_bytes=VMEM),
        cost_estimate=pl.CostEstimate(flops=16 * bq * tokens * HEAD, transcendentals=4 * bq * tokens, bytes_accessed=8 * tokens * HEAD),
        name="attend_cross",
    )(at, came, made, own_o, own_lse)


def _merge(at_ref, low_ref, lse_ref, high_ref, far0_ref, o0_ref, far1_ref, o1_ref, keep_ref, give_ref):
    chip = at_ref[CHIP]
    t, n, c = pl.program_id(0), pl.program_id(1), pl.program_id(2)

    def fill(far_ref, o_ref):
        lse = lse_ref[0, pl.ds(n, 1), :]
        far_lse = jnp.where(chip == 0, NEG, _together(far_ref[0, 0, HEAD:, :]))
        top = jnp.maximum(lse, far_lse)
        wa, wb = jnp.exp(lse - top), jnp.exp(far_lse - top)
        scale = 1 / (wa + wb)
        low = low_ref[0] * (wa * scale) + far_ref[0, 0, :HEAD, :].astype(jnp.float32) * (wb * scale)
        high = jnp.where(chip == 0, high_ref[0].astype(jnp.bfloat16), o_ref[0, 0, :HEAD, :])
        for p, part in ((0, low.astype(jnp.bfloat16)), (1, high)):
            turned = part.T

            @pl.when(t == 0)
            def _():
                keep_ref[p, 0] = turned

            @pl.when(t == 1)
            def _():
                give_ref[p, 0] = turned

    @pl.when(c == 0)
    def _():
        fill(far0_ref, o0_ref)

    @pl.when(c == 1)
    def _():
        fill(far1_ref, o1_ref)


def merge(at, low, low_lse, high, first, second, i):
    bq = first[0].shape[3]
    side = lambda t, at_ref: jnp.where(t == 0, at_ref[CORE], 1 - at_ref[CORE])
    mine = pl.BlockSpec((1, HEAD, bq), lambda t, n, c, at_ref: (n, 0, side(t, at_ref) * CHUNKS + 2 * i + c))
    part = pl.BlockSpec((1, 1, HEAD + 16, bq), lambda t, n, c, at_ref: (n, side(t, at_ref), 0, 0))
    return pl.pallas_call(
        _merge,
        grid_spec=pltpu.PrefetchScalarGridSpec(
            num_scalar_prefetch=1, grid=(2, 2, 2),
            in_specs=[mine, pl.BlockSpec((1, 2, bq), lambda t, n, c, at_ref: (side(t, at_ref), 0, 2 * i + c)), mine, part, part, part, part],
            out_specs=[
                pl.BlockSpec((2, 1, bq, HEAD), lambda t, n, c, at_ref: (0, jnp.where(t == 0, n, 1), jnp.where(t == 0, c, 1), 0)),
                pl.BlockSpec((2, 1, bq, HEAD), lambda t, n, c, at_ref: (0, jnp.where(t == 0, 0, n), jnp.where(t == 0, 0, c), 0)),
            ],
        ),
        out_shape=[jax.ShapeDtypeStruct((2, 2, 2 * bq, HEAD), jnp.bfloat16)] * 2,
        compiler_params=pltpu.CompilerParams(dimension_semantics=("arbitrary",) * 3, vmem_limit_bytes=VMEM),
        cost_estimate=pl.CostEstimate(flops=128 * bq * HEAD, transcendentals=0, bytes_accessed=128 * bq * HEAD),
        name="merge",
    )(at, low, low_lse, high, *first, *second)


def _output(at_ref, own_ref, sib_ref, x_ref, w_own, w_sib, wx, wy, vx, vy, *rest):
    y_ref = rest[-1]
    chip, group = at_ref[CHIP], at_ref[GROUP]
    weights = jnp.concatenate([w_own[...], wx[...], wy[...], w_sib[...], vx[...], vy[...]], axis=0)
    for at in range(0, y_ref.shape[0], 512):
        here = slice(at, at + 512)
        parts = []
        for o_ref in (own_ref, sib_ref):
            parts += [o_ref[chip, 0, here], o_ref[chip, 1, here], o_ref[1 - chip, group, here], o_ref[1 - chip, 1 - group, here]]
        y = _dot(jnp.concatenate(parts, axis=1), weights, 1, 0)
        y_ref[here, :] = (x_ref[here, :].astype(jnp.float32) + y).astype(y_ref.dtype)


def output(at, x, weights, own, sib, i, done):
    rows, width = own.shape[2], x.shape[1]
    bn = 768
    part = pl.BlockSpec(own.shape, lambda j, at_ref: (0, 0, 0, 0))
    here = pl.BlockSpec((rows, bn), lambda j, at_ref: (i, j))
    given = [own, sib, x, *weights]
    specs = [part, part, here] + [pl.BlockSpec((w.shape[0], bn), lambda j, at_ref: (0, j)) for w in weights]
    alias = {}
    if done is not None:
        given.append(done)
        specs.append(pl.BlockSpec(memory_space=pl.ANY))
        alias = {len(given): 0}
    return pl.pallas_call(
        _output,
        grid_spec=pltpu.PrefetchScalarGridSpec(num_scalar_prefetch=1, grid=(width // bn,), in_specs=specs, out_specs=here),
        out_shape=jax.ShapeDtypeStruct(x.shape, jnp.bfloat16),
        input_output_aliases=alias,
        compiler_params=pltpu.CompilerParams(dimension_semantics=("arbitrary",), vmem_limit_bytes=VMEM),
        cost_estimate=pl.CostEstimate(flops=2 * rows * 8 * HEAD * width, transcendentals=0, bytes_accessed=16 * HEAD * width),
        name="output",
    )(at, *given)


def tables(place):
    half = HEAD // 2
    angle = place.astype(jnp.float32)[:, None] * THETA ** (-jnp.arange(half, dtype=jnp.float32) / half)
    return jnp.cos(angle), jnp.sin(angle)


def solution(mesh):
    def step(x, gain, wq, wk, wv, wo):
        own = x.shape[0]
        rank, group = lax.axis_index("sp"), lax.axis_index("dp")
        chip, core = rank // 2, rank % 2

        pick = lambda n, which: jnp.where(which == 0, ORDER[0][n], ORDER[1][n])
        at = jnp.stack([pick(n, chip) for n in range(4)] + [pick(n, 1 - chip) for n in range(4)] + [chip, core, group]).astype(jnp.int32)

        w_own, w_give = share(at, wq, wk, wv)
        w_sib = lax.ppermute(w_give, "sp", SIBLING)
        leaving = leave(at, w_own, w_sib)
        wx, wy = [], []
        for n in range(4):
            wx.append(lax.ppermute(leaving[n], "sp", ACROSS))
            wy.append(lax.ppermute(wx[n], "dp", GROUPS))

        a_own = normed(x, gain)
        a_sib = lax.ppermute(a_own, "sp", SIBLING)
        cos, sin = tables(chip * 2 * own + jnp.arange(2 * own))

        made, sent = None, None
        for n in range(4):
            got = project(at, a_own, a_sib, w_own, w_sib, wx[n], wy[n], cos, sin, n, made)
            made = got[0]
            if n == 0:
                sent = got[1]
        came = lax.ppermute(sent, "sp", ACROSS)

        wo_here, _ = lax.optimization_barrier((wo, sent))
        wo_half = lax.dynamic_slice_in_dim(wo_here, group * HEAD, HEAD, axis=0)
        ox = lax.ppermute(wo_half, "sp", ACROSS)
        oy = lax.ppermute(ox, "dp", GROUPS)
        wo_sib, ox_sib, oy_sib = (lax.ppermute(w, "sp", SIBLING) for w in (wo_here, ox, oy))
        weights = (wo, wo_sib, ox, oy, ox_sib, oy_sib)

        high, high_lse = attend_own(made, 1)
        parts = []
        for i in range(CHUNKS):
            o = attend_cross(at, came, made, high, high_lse, i)
            parts.append((lax.ppermute(o, "sp", BACK), o))
        low, low_lse = attend_own(made, 0)
        y, results = None, []
        for i in range(CHUNKS // 2):
            keep, give = merge(at, low, low_lse, high, *parts[2 * i : 2 * i + 2], i)
            results.append((keep, lax.ppermute(give, "sp", SIBLING)))
        for i, (keep, take) in enumerate(results):
            y = output(at, x, weights, keep, take, i, y)
        return y

    tokens, whole = P(("dp", "sp"), None), P("sp", None)
    return jax.shard_map(
        step,
        mesh=mesh,
        in_specs=(tokens, P(None), whole, whole, whole, whole),
        out_specs=tokens,
        check_vma=False,
    )
```

```python
import functools

import jax
import jax.numpy as jnp
from jax import lax
from jax.experimental import pallas as pl
from jax.experimental.pallas import tpu as pltpu
from jax.sharding import PartitionSpec as P


NEG = -1e30
HIDDEN = 2 * NEG
LOG2E = 1.4426950408889634
VMEM = 56 * 2**20
HEAD = 256
THETA = 10000
SCALE = HEAD**-0.5
E = SCALE * LOG2E
STRIP = 512
ROWS = 512
KEYS = 1024
CHUNKS = 4


SIBLING = [(0, 1), (1, 0), (2, 3), (3, 2)]
ACROSS = [(0, 2), (2, 0), (1, 3), (3, 1)]
BACK = [(0, 2), (1, 3)]
GROUPS = [(0, 1), (1, 0)]
ORDER = ((3, 1, 0, 2), (0, 2, 1, 3))
OTHERS, CHIP, CORE, GROUP = 4, 8, 9, 10


def _dot(a, b, ca, cb):
    return lax.dot_general(a, b, (((ca,), (cb,)), ((), ())), preferred_element_type=jnp.float32)


def _share(at_ref, *refs):
    for q_ref, k_ref, v_ref, to_ref in (refs[:3] + refs[6:7], refs[3:6] + refs[7:8]):
        to_ref[0] = q_ref[...]
        to_ref[1, :, :HEAD] = k_ref[...]
        to_ref[1, :, HEAD:] = v_ref[...]


def share(at, wq, wk, wv):
    rows = wq.shape[0]
    specs = []
    for mine in (True, False):
        at_block = lambda p, at_ref, mine=mine: (0, 2 * p + (at_ref[CORE] if mine else 1 - at_ref[CORE]))
        specs += [pl.BlockSpec((rows, 2 * HEAD), at_block), pl.BlockSpec((rows, HEAD), at_block), pl.BlockSpec((rows, HEAD), at_block)]
    out = pl.BlockSpec((2, rows, 2 * HEAD), lambda p, at_ref: (p, 0, 0))
    return pl.pallas_call(
        _share,
        grid_spec=pltpu.PrefetchScalarGridSpec(num_scalar_prefetch=1, grid=(2,), in_specs=specs, out_specs=[out, out]),
        out_shape=[jax.ShapeDtypeStruct((4, rows, 2 * HEAD), jnp.bfloat16)] * 2,
        compiler_params=pltpu.CompilerParams(dimension_semantics=("arbitrary",), vmem_limit_bytes=VMEM),
        cost_estimate=pl.CostEstimate(flops=1000, transcendentals=0, bytes_accessed=4 * wq.size * 2),
        name="share",
    )(at, wq, wk, wv, wq, wk, wv)


def _leave(at_ref, own_ref, sib_ref, *to_refs):
    for n, to_ref in enumerate(to_refs):
        slot = at_ref[OTHERS + n]

        @pl.when(at_ref[GROUP] == at_ref[CORE])
        def _():
            to_ref[...] = own_ref[slot]

        @pl.when(at_ref[GROUP] != at_ref[CORE])
        def _():
            to_ref[...] = sib_ref[slot]


def leave(at, w_own, w_sib):
    whole = pl.BlockSpec(w_own.shape, lambda i, at_ref: (0, 0, 0))
    out = pl.BlockSpec(w_own.shape[1:], lambda i, at_ref: (0, 0))
    return pl.pallas_call(
        _leave,
        grid_spec=pltpu.PrefetchScalarGridSpec(num_scalar_prefetch=1, grid=(1,), in_specs=[whole, whole], out_specs=[out] * 4),
        out_shape=[jax.ShapeDtypeStruct(w_own.shape[1:], jnp.bfloat16)] * 4,
        compiler_params=pltpu.CompilerParams(dimension_semantics=("arbitrary",), vmem_limit_bytes=VMEM),
        cost_estimate=pl.CostEstimate(flops=1000, transcendentals=0, bytes_accessed=6 * w_own.size),
        name="leave",
    )(at, w_own, w_sib)


def _normed(x_ref, gain_ref, a_ref):
    wide = x_ref[...].astype(jnp.float32)
    scale = lax.rsqrt(jnp.mean(wide * wide, -1, keepdims=True) + 1e-6)
    a_ref[...] = (wide * scale * gain_ref[...].astype(jnp.float32)).astype(jnp.bfloat16)


def normed(x, gain):
    rows, depth = x.shape
    block = pl.BlockSpec((512, depth), lambda i: (i, 0))
    return pl.pallas_call(
        _normed,
        grid=(rows // 512,),
        in_specs=[block, pl.BlockSpec((1, depth), lambda i: (0, 0))],
        out_specs=block,
        out_shape=jax.ShapeDtypeStruct(x.shape, jnp.bfloat16),
        compiler_params=pltpu.CompilerParams(dimension_semantics=("arbitrary",), vmem_limit_bytes=VMEM),
        cost_estimate=pl.CostEstimate(flops=8 * x.size, transcendentals=0, bytes_accessed=4 * x.size),
        name="normed",
    )(x, gain[None])


def _project(at_ref, a0_ref, a1_ref, own_ref, sib_ref, wx_ref, wy_ref, cos_ref, sin_ref, *rest, which):
    out_ref, sent_ref, w_s = rest if which == 0 else (rest[1], None, rest[2])
    slot, chip, core, group = at_ref[which], at_ref[CHIP], at_ref[CORE], at_ref[GROUP]
    i = pl.program_id(0)
    rows = own_ref.shape[1]

    @pl.when(i == 0)
    def _():
        here, there = 2 * rows * chip, 2 * rows * (1 - chip)
        for at, ref in ((here + rows * core, own_ref), (here + rows * (1 - core), sib_ref)):
            w_s[pl.ds(pl.multiple_of(at, 64), rows), :] = ref[0]
        for at, ref in ((there + rows * group, wx_ref), (there + rows * (1 - group), wy_ref)):
            w_s[pl.ds(pl.multiple_of(at, 64), rows), :] = ref[...]

    def part(a_ref):
        half = HEAD // 2

        def rows_from(r, _):
            here = pl.ds(pl.multiple_of(r * ROWS, ROWS), ROWS)
            t = _dot(a_ref[here, :], w_s[...], 1, 0).astype(jnp.bfloat16).astype(jnp.float32)
            cos, sin = cos_ref[here, :], sin_ref[here, :]
            for n in range(2):
                p, q = t[:, n * HEAD : n * HEAD + half], t[:, n * HEAD + half : (n + 1) * HEAD]
                u, v = p * cos - q * sin, q * cos + p * sin
                if n == 1:
                    u, v = jnp.where(slot % 2 == 0, u, p), jnp.where(slot % 2 == 0, v, q)
                got = jnp.concatenate([u, v], axis=1).astype(jnp.bfloat16)
                out_ref[0, n, here, :] = got
                if sent_ref is not None:
                    sent_ref[n, here, :] = got

        lax.fori_loop(0, a_ref.shape[0] // ROWS, rows_from, None)

    @pl.when(i < pl.num_programs(0) // 2)
    def _():
        part(a0_ref)

    @pl.when(i >= pl.num_programs(0) // 2)
    def _():
        part(a1_ref)


def project(at, a_own, a_sib, w_own, w_sib, wx, wy, cos, sin, which, done):
    tokens, depth = a_own.shape
    rows, width = wx.shape
    bm = 1024
    n = tokens // bm
    first = which == 0

    def place(i, at_ref):
        return jnp.where(i < n, at_ref[CORE] * n + i, (1 - at_ref[CORE]) * n + i - n)

    weights = pl.BlockSpec((1, rows, width), lambda i, at_ref: (at_ref[which], 0, 0))
    fetched = pl.BlockSpec((rows, width), lambda i, at_ref: (0, 0))
    table = pl.BlockSpec((bm, HEAD // 2), lambda i, at_ref: (place(i, at_ref), 0))
    specs = [
        pl.BlockSpec((bm, depth), lambda i, at_ref: (jnp.minimum(i, n - 1), 0)),
        pl.BlockSpec((bm, depth), lambda i, at_ref: (jnp.maximum(i - n, 0), 0)),
        weights, weights, fetched, fetched, table, table,
    ]
    given = [a_own, a_sib, w_own, w_sib, wx, wy, cos, sin]
    out_shape = [jax.ShapeDtypeStruct((4, 2, 2 * tokens, HEAD), jnp.bfloat16)]
    out_specs = [pl.BlockSpec((1, 2, bm, HEAD), lambda i, at_ref: (at_ref[which], 0, place(i, at_ref), 0))]
    alias = {}
    if first:
        out_shape.append(jax.ShapeDtypeStruct((2, 2 * tokens, HEAD), jnp.bfloat16))
        out_specs.append(pl.BlockSpec((2, bm, HEAD), lambda i, at_ref: (0, place(i, at_ref), 0)))
    else:
        given.append(done)
        specs.append(pl.BlockSpec(memory_space=pl.ANY))
        alias = {len(given): 0}
    return pl.pallas_call(
        functools.partial(_project, which=which),
        grid_spec=pltpu.PrefetchScalarGridSpec(
            num_scalar_prefetch=1, grid=(2 * n,), in_specs=specs, out_specs=out_specs,
            scratch_shapes=[pltpu.VMEM((4 * rows, width), jnp.bfloat16)],
        ),
        out_shape=out_shape,
        input_output_aliases=alias,
        compiler_params=pltpu.CompilerParams(dimension_semantics=("arbitrary",), vmem_limit_bytes=VMEM),
        cost_estimate=pl.CostEstimate(flops=4 * tokens * depth * width, transcendentals=0, bytes_accessed=4 * tokens * depth),
        name="project",
    )(at, *given)


def _weigh(scores, i, values, top_s, mix_s, ok=None):
    if ok is not None:
        least = scores.shape[0] - STRIP
        last = jnp.where(ok, scores[least:], HIDDEN)
        scores = jnp.concatenate([scores[:least], last], axis=0) if least else last
    old = top_s[i]
    top = jnp.maximum(old, scores.max(axis=0, keepdims=True))
    top_s[i] = top
    p = jnp.exp2((scores - top) * E).astype(jnp.bfloat16)
    mix_s[i] = mix_s[i] * jnp.exp2((old - top) * E) + _dot(values, p, 1, 0)


def _turn(v, at, to_s):
    to_s[:HEAD, pl.ds(at, v.shape[0])] = v.T
    to_s[HEAD:, pl.ds(at, v.shape[0])] = jnp.ones((8, v.shape[0]), jnp.bfloat16)


def _own(q_ref, k_ref, v_ref, o_ref, lse_ref, score_s, value_s, top_s, mix_s):
    bq = q_ref.shape[2]
    iq = pl.program_id(0)
    top_s[...] = jnp.full(top_s.shape, NEG, jnp.float32)
    mix_s[...] = jnp.zeros(mix_s.shape, jnp.float32)
    ok = lax.broadcasted_iota(jnp.int32, (STRIP, STRIP), 1) >= lax.broadcasted_iota(jnp.int32, (STRIP, STRIP), 0)
    head = lambda i: lax.rem(lax.div(i, 2), 2)
    strip = lambda i: lax.rem(i, 2) + 2 * (1 - lax.div(i, 4))
    rows = lambda s, size=STRIP: pl.ds(pl.multiple_of(s * STRIP, STRIP), size)
    queries = lambda i: q_ref[0, head(i), rows(strip(i)), :]
    keys = lambda j: pl.ds(pl.multiple_of(j * KEYS, KEYS), KEYS)

    @pl.when(iq == 0)
    def _():
        lax.fori_loop(0, k_ref.shape[2] // KEYS, lambda j, _: _turn(v_ref[0, 0, keys(j), :], pl.multiple_of(j * KEYS, KEYS), value_s), None)

    score = lambda j, i: _dot(k_ref[0, 0, keys(j), :], queries(i), 1, 1)
    groups = 2 * (bq // KEYS) * iq + 1
    score_s[0] = score(0, 0)

    def group(g, _):
        j, base = lax.div(g, 2), 4 * lax.rem(g, 2)
        for u in range(4):
            near = (j, base + u + 1) if u < 3 else (lax.div(jnp.minimum(g + 1, groups - 1), 2), lax.rem(base + 4, 8))
            score_s[(u + 1) % 2] = score(*near)
            _weigh(score_s[u % 2], base + u, value_s[:, keys(j)], top_s, mix_s)

    lax.fori_loop(0, groups, group, None)

    def pair(d, _):
        n, half = lax.div(d, 2), lax.rem(d, 2)
        i = 4 * (1 - half) + 2 * n
        at = pl.multiple_of((iq * (bq // KEYS) + half) * KEYS, KEYS)
        some, all_ = pl.ds(at, STRIP), pl.ds(at, KEYS)
        score_s[0, :STRIP] = _dot(k_ref[0, 0, some, :], queries(i), 1, 1)
        score_s[1] = _dot(k_ref[0, 0, all_, :], queries(i + 1), 1, 1)
        _weigh(score_s[0, :STRIP], i, value_s[:, some], top_s, mix_s, ok)
        _weigh(score_s[1], i + 1, value_s[:, all_], top_s, mix_s, ok)

    lax.fori_loop(0, 4, pair, None)

    def finish(i, _):
        total = mix_s[i, HEAD : HEAD + 1, :]
        o_ref[head(i), :, rows(strip(i))] = mix_s[i, :HEAD, :] * (1 / total)
        lse_ref[0, pl.ds(head(i), 1), rows(strip(i))] = top_s[i] * SCALE + jnp.log(total)

    lax.fori_loop(0, 8, finish, None)


def attend_own(made, h):
    tokens = made.shape[2]
    bq = 2 * KEYS
    return pl.pallas_call(
        _own,
        grid=(tokens // bq,),
        in_specs=[
            pl.BlockSpec((1, 2, bq, HEAD), lambda i: (2 * h, 0, i, 0)),
            pl.BlockSpec((1, 1, tokens, HEAD), lambda i: (2 * h + 1, 0, 0, 0)),
            pl.BlockSpec((1, 1, tokens, HEAD), lambda i: (2 * h + 1, 1, 0, 0)),
        ],
        out_specs=[pl.BlockSpec((2, HEAD, bq), lambda i: (0, 0, i)), pl.BlockSpec((1, 2, bq), lambda i: (i, 0, 0))],
        out_shape=[jax.ShapeDtypeStruct((2, HEAD, tokens), jnp.float32), jax.ShapeDtypeStruct((tokens // bq, 2, bq), jnp.float32)],
        scratch_shapes=[
            pltpu.VMEM((2, KEYS, STRIP), jnp.float32), pltpu.VMEM((HEAD + 8, tokens), jnp.bfloat16),
            pltpu.VMEM((8, 1, STRIP), jnp.float32), pltpu.VMEM((8, HEAD + 8, STRIP), jnp.float32),
        ],
        compiler_params=pltpu.CompilerParams(dimension_semantics=("arbitrary",), vmem_limit_bytes=VMEM),
        cost_estimate=pl.CostEstimate(flops=4 * tokens * tokens * HEAD, transcendentals=tokens * tokens, bytes_accessed=made.size),
        name="attend_own",
    )(made, made, made)


def _cross(at_ref, came_ref, made_ref, own_ref, lse_in, o_ref, q_s, k_s, v_s, in_s, score_s, value_s, top_s, mix_s, sem, *, chunk):
    bq = o_ref.shape[3]
    tokens = k_s.shape[0]
    pieces = [(n, m) for n in range(2) for m in range(2)]
    count = tokens // KEYS
    first = at_ref[CHIP] == 0

    def queries(q_from):
        half = tokens // 2
        return [pltpu.make_async_copy(q_from.at[n, pl.ds(m * half + chunk * bq, bq), :], q_s.at[n, m], sem.at[2 * n + m]) for n, m in pieces]

    def keys(kv_from, b, n):
        rows = pl.ds(pl.multiple_of(b * KEYS, KEYS), KEYS)
        return pltpu.make_async_copy(kv_from.at[n, rows, :], (k_s, v_s)[n].at[rows, :], sem.at[4 + 2 * b + n])

    def start(q_from, kv_from):
        for copy in queries(q_from) + [keys(kv_from, b, n) for b in range(count) for n in range(2)]:
            copy.start()

    @pl.when(first)
    def _():
        start(came_ref, made_ref.at[1])

    @pl.when(jnp.logical_not(first))
    def _():
        start(made_ref.at[2], came_ref)

    carries = [
        pltpu.make_async_copy(own_ref.at[n, :, pl.ds(m * (tokens // 2) + chunk * bq, bq)], in_s.at[n, m], sem.at[4 + 2 * count + 2 * n + m])
        for n, m in pieces
    ]
    for copy in carries:
        copy.start()
    top_s[...] = jnp.full(top_s.shape, NEG, jnp.float32)
    mix_s[...] = jnp.zeros(mix_s.shape, jnp.float32)
    for copy in queries(came_ref) + [keys(came_ref, 0, 0)]:
        copy.wait()
    here = lambda b: pl.ds(pl.multiple_of(b * KEYS, KEYS), KEYS)
    score = lambda b, i: _dot(k_s[here(b), :], q_s[pieces[i]], 1, 1)
    score_s[0] = score(0, 0)

    def block(b, _):
        @pl.when(b + 1 < count)
        def _():
            keys(came_ref, b + 1, 0).wait()

        keys(came_ref, b, 1).wait()
        _turn(v_s[here(b), :], 0, value_s)
        for i in range(4):
            score_s[(i + 1) % 2] = score(b, i + 1) if i < 3 else score(jnp.minimum(b + 1, count - 1), 0)
            _weigh(score_s[i % 2], i, value_s[...], top_s, mix_s)

    lax.fori_loop(0, count, block, None)
    for copy in carries:
        copy.wait()

    def finish(s, _):
        n, m = lax.div(s, 2), lax.rem(s, 2)
        top, total = top_s[s] * SCALE, mix_s[s, HEAD : HEAD + 1, :]
        before = jnp.where(first, NEG, lse_in[m, pl.ds(n, 1), :])
        most = jnp.maximum(top, before)
        wa, wb = jnp.exp(top - most), jnp.exp(before - most)
        whole = total * wa + wb
        scale = 1 / whole
        o_ref[n, m, :HEAD, :] = (mix_s[s, :HEAD, :] * (wa * scale) + in_s[n, m] * (wb * scale)).astype(o_ref.dtype)
        o_ref[n, m, HEAD:, :] = _apart(most + jnp.log(whole))

    lax.fori_loop(0, 4, finish, None)


def _apart(row):
    rows = []
    for _ in range(3):
        rows.append(row.astype(jnp.bfloat16).astype(jnp.float32))
        row = row - rows[-1]
    return jnp.concatenate(rows + [jnp.zeros((13, row.shape[1]), jnp.float32)], axis=0).astype(jnp.bfloat16)


def _together(rows):
    wide = rows.astype(jnp.float32)
    return wide[0:1] + wide[1:2] + wide[2:3]


def attend_cross(at, came, made, own_o, own_lse, i):
    tokens = made.shape[2]
    half = tokens // 2
    bq = half // CHUNKS
    anywhere = pl.BlockSpec(memory_space=pl.ANY)
    return pl.pallas_call(
        functools.partial(_cross, chunk=i),
        grid_spec=pltpu.PrefetchScalarGridSpec(
            num_scalar_prefetch=1, grid=(1,),
            in_specs=[anywhere, anywhere, anywhere, pl.BlockSpec((2, 2, bq), lambda g, at_ref: (0, 0, i))],
            out_specs=pl.BlockSpec((2, 2, HEAD + 16, bq), lambda g, at_ref: (0, 0, 0, 0)),
            scratch_shapes=[
                pltpu.VMEM((2, 2, bq, HEAD), jnp.bfloat16), pltpu.VMEM((tokens, HEAD), jnp.bfloat16), pltpu.VMEM((tokens, HEAD), jnp.bfloat16),
                pltpu.VMEM((2, 2, HEAD, bq), jnp.float32), pltpu.VMEM((2, KEYS, STRIP), jnp.float32), pltpu.VMEM((HEAD + 8, KEYS), jnp.bfloat16),
                pltpu.VMEM((4, 1, STRIP), jnp.float32), pltpu.VMEM((4, HEAD + 8, STRIP), jnp.float32),
                pltpu.SemaphoreType.DMA((8 + 2 * (tokens // KEYS),)),
            ],
        ),
        out_shape=jax.ShapeDtypeStruct((2, 2, HEAD + 16, bq), jnp.bfloat16),
        compiler_params=pltpu.CompilerParams(dimension_semantics=("arbitrary",), vmem_limit_bytes=VMEM),
        cost_estimate=pl.CostEstimate(flops=16 * bq * tokens * HEAD, transcendentals=4 * bq * tokens, bytes_accessed=8 * tokens * HEAD),
        name="attend_cross",
    )(at, came, made, own_o, own_lse)


def _merge(at_ref, low0_ref, low1_ref, lse_ref, high0_ref, high1_ref, far0_ref, o0_ref, far1_ref, o1_ref, keep_ref, give_ref):
    chip = at_ref[CHIP]
    n = pl.program_id(0)
    bq = far0_ref.shape[3]

    def fill(to_ref, low_ref, high_ref, side):
        for c, (far_ref, o_ref) in enumerate(((far0_ref, o0_ref), (far1_ref, o1_ref))):
            here = slice(c * bq, (c + 1) * bq)
            lse = lse_ref[side, pl.ds(n, 1), here]
            far_lse = jnp.where(chip == 0, NEG, _together(far_ref[0, side, HEAD:, :]))
            top = jnp.maximum(lse, far_lse)
            wa, wb = jnp.exp(lse - top), jnp.exp(far_lse - top)
            scale = 1 / (wa + wb)
            low = low_ref[0, :, here] * (wa * scale) + far_ref[0, side, :HEAD, :].astype(jnp.float32) * (wb * scale)
            high = jnp.where(chip == 0, high_ref[0, :, here].astype(jnp.bfloat16), o_ref[0, side, :HEAD, :])
            to_ref[0, 0, here, :] = low.astype(jnp.bfloat16).T
            to_ref[1, 0, here, :] = high.T

    @pl.when(at_ref[CORE] == 0)
    def _():
        fill(keep_ref, low0_ref, high0_ref, 0)
        fill(give_ref, low1_ref, high1_ref, 1)

    @pl.when(at_ref[CORE] == 1)
    def _():
        fill(keep_ref, low1_ref, high1_ref, 1)
        fill(give_ref, low0_ref, high0_ref, 0)


def merge(at, low, low_lse, high, first, second, i):
    bq = first[0].shape[3]
    mine = [pl.BlockSpec((1, HEAD, 2 * bq), lambda n, at_ref, side=side: (n, 0, side * CHUNKS // 2 + i)) for side in range(2)]
    part = pl.BlockSpec((1, 2, HEAD + 16, bq), lambda n, at_ref: (n, 0, 0, 0))
    result = pl.BlockSpec((2, 1, 2 * bq, HEAD), lambda n, at_ref: (0, n, 0, 0))
    return pl.pallas_call(
        _merge,
        grid_spec=pltpu.PrefetchScalarGridSpec(
            num_scalar_prefetch=1, grid=(2,),
            in_specs=[*mine, pl.BlockSpec((2, 2, 2 * bq), lambda n, at_ref: (0, 0, i)), *mine, part, part, part, part],
            out_specs=[result, result],
        ),
        out_shape=[jax.ShapeDtypeStruct((2, 2, 2 * bq, HEAD), jnp.bfloat16)] * 2,
        compiler_params=pltpu.CompilerParams(dimension_semantics=("arbitrary",), vmem_limit_bytes=VMEM),
        cost_estimate=pl.CostEstimate(flops=128 * bq * HEAD, transcendentals=0, bytes_accessed=128 * bq * HEAD),
        name="merge",
    )(at, low, low, low_lse, high, high, *first, *second)


def _output(at_ref, own_ref, sib_ref, x_ref, w_own, w_sib, wx, wy, vx, vy, *rest):
    y_ref = rest[-1]
    chip, group = at_ref[CHIP], at_ref[GROUP]
    weights = jnp.concatenate([w_own[...], wx[...], wy[...], w_sib[...], vx[...], vy[...]], axis=0)
    for at in range(0, y_ref.shape[0], 512):
        here = slice(at, at + 512)
        parts = []
        for o_ref in (own_ref, sib_ref):
            parts += [o_ref[chip, 0, here], o_ref[chip, 1, here], o_ref[1 - chip, group, here], o_ref[1 - chip, 1 - group, here]]
        y = _dot(jnp.concatenate(parts, axis=1), weights, 1, 0)
        y_ref[here, :] = (x_ref[here, :].astype(jnp.float32) + y).astype(y_ref.dtype)


def output(at, x, weights, own, sib, i, done):
    rows, width = own.shape[2], x.shape[1]
    bn = 768
    part = pl.BlockSpec(own.shape, lambda j, at_ref: (0, 0, 0, 0))
    here = pl.BlockSpec((rows, bn), lambda j, at_ref: (i, j))
    given = [own, sib, x, *weights]
    specs = [part, part, here] + [pl.BlockSpec((w.shape[0], bn), lambda j, at_ref: (0, j)) for w in weights]
    alias = {}
    if done is not None:
        given.append(done)
        specs.append(pl.BlockSpec(memory_space=pl.ANY))
        alias = {len(given): 0}
    return pl.pallas_call(
        _output,
        grid_spec=pltpu.PrefetchScalarGridSpec(num_scalar_prefetch=1, grid=(width // bn,), in_specs=specs, out_specs=here),
        out_shape=jax.ShapeDtypeStruct(x.shape, jnp.bfloat16),
        input_output_aliases=alias,
        compiler_params=pltpu.CompilerParams(dimension_semantics=("arbitrary",), vmem_limit_bytes=VMEM),
        cost_estimate=pl.CostEstimate(flops=2 * rows * 8 * HEAD * width, transcendentals=0, bytes_accessed=16 * HEAD * width),
        name="output",
    )(at, *given)


def tables(place):
    half = HEAD // 2
    angle = place.astype(jnp.float32)[:, None] * THETA ** (-jnp.arange(half, dtype=jnp.float32) / half)
    return jnp.cos(angle), jnp.sin(angle)


def solution(mesh):
    def step(x, gain, wq, wk, wv, wo):
        own = x.shape[0]
        rank, group = lax.axis_index("sp"), lax.axis_index("dp")
        chip, core = rank // 2, rank % 2

        pick = lambda n, which: jnp.where(which == 0, ORDER[0][n], ORDER[1][n])
        at = jnp.stack([pick(n, chip) for n in range(4)] + [pick(n, 1 - chip) for n in range(4)] + [chip, core, group]).astype(jnp.int32)

        w_own, w_give = share(at, wq, wk, wv)
        w_sib = lax.ppermute(w_give, "sp", SIBLING)
        leaving = leave(at, w_own, w_sib)
        wx, wy = [], []
        for n in range(4):
            wx.append(lax.ppermute(leaving[n], "sp", ACROSS))
            wy.append(lax.ppermute(wx[n], "dp", GROUPS))

        a_own = normed(x, gain)
        a_sib = lax.ppermute(a_own, "sp", SIBLING)
        cos, sin = tables(chip * 2 * own + jnp.arange(2 * own))

        made, sent = None, None
        for n in range(4):
            got = project(at, a_own, a_sib, w_own, w_sib, wx[n], wy[n], cos, sin, n, made)
            made = got[0]
            if n == 0:
                sent = got[1]
        came = lax.ppermute(sent, "sp", ACROSS)

        wo_here, _ = lax.optimization_barrier((wo, sent))
        wo_half = lax.dynamic_slice_in_dim(wo_here, group * HEAD, HEAD, axis=0)
        ox = lax.ppermute(wo_half, "sp", ACROSS)
        oy = lax.ppermute(ox, "dp", GROUPS)
        wo_sib, ox_sib, oy_sib = (lax.ppermute(w, "sp", SIBLING) for w in (wo_here, ox, oy))
        weights = (wo, wo_sib, ox, oy, ox_sib, oy_sib)

        high, high_lse = attend_own(made, 1)
        parts = []
        for i in range(CHUNKS):
            o = attend_cross(at, came, made, high, high_lse, i)
            parts.append((lax.ppermute(o, "sp", BACK), o))
        low, low_lse = attend_own(made, 0)
        y, results = None, []
        for i in range(CHUNKS // 2):
            keep, give = merge(at, low, low_lse, high, *parts[2 * i : 2 * i + 2], i)
            results.append((keep, lax.ppermute(give, "sp", SIBLING)))
        for i, (keep, take) in enumerate(results):
            y = output(at, x, weights, keep, take, i, y)
        return y

    tokens, whole = P(("dp", "sp"), None), P("sp", None)
    return jax.shard_map(
        step,
        mesh=mesh,
        in_specs=(tokens, P(None), whole, whole, whole, whole),
        out_specs=tokens,
        check_vma=False,
    )
```

```python
import functools

import jax
import jax.numpy as jnp
from jax import lax
from jax.experimental import pallas as pl
from jax.experimental.pallas import tpu as pltpu
from jax.sharding import PartitionSpec as P


NEG = -1e30
HIDDEN = 2 * NEG
LOG2E = 1.4426950408889634
VMEM = 56 * 2**20
HEAD = 256
THETA = 10000
SCALE = HEAD**-0.5
E = SCALE * LOG2E
STRIP = 512
ROWS = 512
KEYS = 1024
CHUNKS = 4


SIBLING = [(0, 1), (1, 0), (2, 3), (3, 2)]
ACROSS = [(0, 2), (2, 0), (1, 3), (3, 1)]
BACK = [(0, 2), (1, 3)]
GROUPS = [(0, 1), (1, 0)]
ORDER = ((3, 1, 0, 2), (0, 2, 1, 3))
OTHERS, CHIP, CORE, GROUP = 4, 8, 9, 10


def _dot(a, b, ca, cb):
    return lax.dot_general(a, b, (((ca,), (cb,)), ((), ())), preferred_element_type=jnp.float32)


def _share(at_ref, *refs):
    for q_ref, k_ref, v_ref, to_ref in (refs[:3] + refs[6:7], refs[3:6] + refs[7:8]):
        to_ref[0] = q_ref[...]
        to_ref[1, :, :HEAD] = k_ref[...]
        to_ref[1, :, HEAD:] = v_ref[...]


def share(at, wq, wk, wv):
    rows = wq.shape[0]
    specs = []
    for mine in (True, False):
        at_block = lambda p, at_ref, mine=mine: (0, 2 * p + (at_ref[CORE] if mine else 1 - at_ref[CORE]))
        specs += [pl.BlockSpec((rows, 2 * HEAD), at_block), pl.BlockSpec((rows, HEAD), at_block), pl.BlockSpec((rows, HEAD), at_block)]
    out = pl.BlockSpec((2, rows, 2 * HEAD), lambda p, at_ref: (p, 0, 0))
    return pl.pallas_call(
        _share,
        grid_spec=pltpu.PrefetchScalarGridSpec(num_scalar_prefetch=1, grid=(2,), in_specs=specs, out_specs=[out, out]),
        out_shape=[jax.ShapeDtypeStruct((4, rows, 2 * HEAD), jnp.bfloat16)] * 2,
        compiler_params=pltpu.CompilerParams(dimension_semantics=("arbitrary",), vmem_limit_bytes=VMEM),
        cost_estimate=pl.CostEstimate(flops=1000, transcendentals=0, bytes_accessed=4 * wq.size * 2),
        name="share",
    )(at, wq, wk, wv, wq, wk, wv)


def _leave(at_ref, own_ref, sib_ref, *to_refs):
    for n, to_ref in enumerate(to_refs):
        slot = at_ref[OTHERS + n]

        @pl.when(at_ref[GROUP] == at_ref[CORE])
        def _():
            to_ref[...] = own_ref[slot]

        @pl.when(at_ref[GROUP] != at_ref[CORE])
        def _():
            to_ref[...] = sib_ref[slot]


def leave(at, w_own, w_sib):
    whole = pl.BlockSpec(w_own.shape, lambda i, at_ref: (0, 0, 0))
    out = pl.BlockSpec(w_own.shape[1:], lambda i, at_ref: (0, 0))
    return pl.pallas_call(
        _leave,
        grid_spec=pltpu.PrefetchScalarGridSpec(num_scalar_prefetch=1, grid=(1,), in_specs=[whole, whole], out_specs=[out] * 4),
        out_shape=[jax.ShapeDtypeStruct(w_own.shape[1:], jnp.bfloat16)] * 4,
        compiler_params=pltpu.CompilerParams(dimension_semantics=("arbitrary",), vmem_limit_bytes=VMEM),
        cost_estimate=pl.CostEstimate(flops=1000, transcendentals=0, bytes_accessed=6 * w_own.size),
        name="leave",
    )(at, w_own, w_sib)


def _normed(x_ref, gain_ref, a_ref):
    wide = x_ref[...].astype(jnp.float32)
    scale = lax.rsqrt(jnp.mean(wide * wide, -1, keepdims=True) + 1e-6)
    a_ref[...] = (wide * scale * gain_ref[...].astype(jnp.float32)).astype(jnp.bfloat16)


def normed(x, gain):
    rows, depth = x.shape
    block = pl.BlockSpec((1024, depth), lambda i: (i, 0))
    return pl.pallas_call(
        _normed,
        grid=(rows // 1024,),
        in_specs=[block, pl.BlockSpec((1, depth), lambda i: (0, 0))],
        out_specs=block,
        out_shape=jax.ShapeDtypeStruct(x.shape, jnp.bfloat16),
        compiler_params=pltpu.CompilerParams(dimension_semantics=("arbitrary",), vmem_limit_bytes=VMEM),
        cost_estimate=pl.CostEstimate(flops=8 * x.size, transcendentals=0, bytes_accessed=4 * x.size),
        name="normed",
    )(x, gain[None])


def _project(at_ref, a0_ref, a1_ref, own_ref, sib_ref, wx_ref, wy_ref, cos_ref, sin_ref, *rest, which):
    out_ref, sent_ref, w_s = rest if which == 0 else (rest[1], None, rest[2])
    slot, chip, core, group = at_ref[which], at_ref[CHIP], at_ref[CORE], at_ref[GROUP]
    i = pl.program_id(0)
    rows = own_ref.shape[1]

    @pl.when(i == 0)
    def _():
        here, there = 2 * rows * chip, 2 * rows * (1 - chip)
        for at, ref in ((here + rows * core, own_ref), (here + rows * (1 - core), sib_ref)):
            w_s[pl.ds(pl.multiple_of(at, 64), rows), :] = ref[0]
        for at, ref in ((there + rows * group, wx_ref), (there + rows * (1 - group), wy_ref)):
            w_s[pl.ds(pl.multiple_of(at, 64), rows), :] = ref[...]

    def part(a_ref):
        half = HEAD // 2

        def rows_from(r, _):
            here = pl.ds(pl.multiple_of(r * ROWS, ROWS), ROWS)
            t = _dot(a_ref[here, :], w_s[...], 1, 0).astype(jnp.bfloat16).astype(jnp.float32)
            cos, sin = cos_ref[here, :], sin_ref[here, :]
            for n in range(2):
                p, q = t[:, n * HEAD : n * HEAD + half], t[:, n * HEAD + half : (n + 1) * HEAD]
                u, v = p * cos - q * sin, q * cos + p * sin
                if n == 1:
                    u, v = jnp.where(slot % 2 == 0, u, p), jnp.where(slot % 2 == 0, v, q)
                got = jnp.concatenate([u, v], axis=1).astype(jnp.bfloat16)
                out_ref[0, n, here, :] = got
                if sent_ref is not None:
                    sent_ref[n, here, :] = got

        lax.fori_loop(0, a_ref.shape[0] // ROWS, rows_from, None)

    @pl.when(i < pl.num_programs(0) // 2)
    def _():
        part(a0_ref)

    @pl.when(i >= pl.num_programs(0) // 2)
    def _():
        part(a1_ref)


def project(at, a_own, a_sib, w_own, w_sib, wx, wy, cos, sin, which, done):
    tokens, depth = a_own.shape
    rows, width = wx.shape
    bm = 512
    n = tokens // bm
    first = which == 0

    def place(i, at_ref):
        return jnp.where(i < n, at_ref[CORE] * n + i, (1 - at_ref[CORE]) * n + i - n)

    weights = pl.BlockSpec((1, rows, width), lambda i, at_ref: (at_ref[which], 0, 0))
    fetched = pl.BlockSpec((rows, width), lambda i, at_ref: (0, 0))
    table = pl.BlockSpec((bm, HEAD // 2), lambda i, at_ref: (place(i, at_ref), 0))
    specs = [
        pl.BlockSpec((bm, depth), lambda i, at_ref: (jnp.minimum(i, n - 1), 0)),
        pl.BlockSpec((bm, depth), lambda i, at_ref: (jnp.maximum(i - n, 0), 0)),
        weights, weights, fetched, fetched, table, table,
    ]
    given = [a_own, a_sib, w_own, w_sib, wx, wy, cos, sin]
    out_shape = [jax.ShapeDtypeStruct((4, 2, 2 * tokens, HEAD), jnp.bfloat16)]
    out_specs = [pl.BlockSpec((1, 2, bm, HEAD), lambda i, at_ref: (at_ref[which], 0, place(i, at_ref), 0))]
    alias = {}
    if first:
        out_shape.append(jax.ShapeDtypeStruct((2, 2 * tokens, HEAD), jnp.bfloat16))
        out_specs.append(pl.BlockSpec((2, bm, HEAD), lambda i, at_ref: (0, place(i, at_ref), 0)))
    else:
        given.append(done)
        specs.append(pl.BlockSpec(memory_space=pl.ANY))
        alias = {len(given): 0}
    return pl.pallas_call(
        functools.partial(_project, which=which),
        grid_spec=pltpu.PrefetchScalarGridSpec(
            num_scalar_prefetch=1, grid=(2 * n,), in_specs=specs, out_specs=out_specs,
            scratch_shapes=[pltpu.VMEM((4 * rows, width), jnp.bfloat16)],
        ),
        out_shape=out_shape,
        input_output_aliases=alias,
        compiler_params=pltpu.CompilerParams(dimension_semantics=("arbitrary",), vmem_limit_bytes=VMEM),
        cost_estimate=pl.CostEstimate(flops=4 * tokens * depth * width, transcendentals=0, bytes_accessed=4 * tokens * depth),
        name="project",
    )(at, *given)


def _weigh(scores, i, values, top_s, mix_s, ok=None):
    if ok is not None:
        least = scores.shape[0] - STRIP
        last = jnp.where(ok, scores[least:], HIDDEN)
        scores = jnp.concatenate([scores[:least], last], axis=0) if least else last
    old = top_s[i]
    top = jnp.maximum(old, scores.max(axis=0, keepdims=True))
    top_s[i] = top
    p = jnp.exp2((scores - top) * E).astype(jnp.bfloat16)
    mix_s[i] = mix_s[i] * jnp.exp2((old - top) * E) + _dot(values, p, 1, 0)


def _turn(v, at, to_s):
    to_s[:HEAD, pl.ds(at, v.shape[0])] = v.T
    to_s[HEAD:, pl.ds(at, v.shape[0])] = jnp.ones((8, v.shape[0]), jnp.bfloat16)


def _own(q_ref, k_ref, v_ref, o_ref, lse_ref, score_s, value_s, top_s, mix_s):
    bq = q_ref.shape[2]
    iq = pl.program_id(0)
    top_s[...] = jnp.full(top_s.shape, NEG, jnp.float32)
    mix_s[...] = jnp.zeros(mix_s.shape, jnp.float32)
    ok = lax.broadcasted_iota(jnp.int32, (STRIP, STRIP), 1) >= lax.broadcasted_iota(jnp.int32, (STRIP, STRIP), 0)
    head = lambda i: lax.rem(lax.div(i, 2), 2)
    strip = lambda i: lax.rem(i, 2) + 2 * (1 - lax.div(i, 4))
    rows = lambda s, size=STRIP: pl.ds(pl.multiple_of(s * STRIP, STRIP), size)
    queries = lambda i: q_ref[0, head(i), rows(strip(i)), :]
    keys = lambda j: pl.ds(pl.multiple_of(j * KEYS, KEYS), KEYS)

    @pl.when(iq == 0)
    def _():
        lax.fori_loop(0, k_ref.shape[2] // KEYS, lambda j, _: _turn(v_ref[0, 0, keys(j), :], pl.multiple_of(j * KEYS, KEYS), value_s), None)

    score = lambda j, i: _dot(k_ref[0, 0, keys(j), :], queries(i), 1, 1)
    groups = 2 * (bq // KEYS) * iq + 1
    score_s[0] = score(0, 0)

    def group(g, _):
        j, base = lax.div(g, 2), 4 * lax.rem(g, 2)
        for u in range(4):
            near = (j, base + u + 1) if u < 3 else (lax.div(jnp.minimum(g + 1, groups - 1), 2), lax.rem(base + 4, 8))
            score_s[(u + 1) % 2] = score(*near)
            _weigh(score_s[u % 2], base + u, value_s[:, keys(j)], top_s, mix_s)

    lax.fori_loop(0, groups, group, None)

    def pair(d, _):
        n, half = lax.div(d, 2), lax.rem(d, 2)
        i = 4 * (1 - half) + 2 * n
        at = pl.multiple_of((iq * (bq // KEYS) + half) * KEYS, KEYS)
        some, all_ = pl.ds(at, STRIP), pl.ds(at, KEYS)
        score_s[0, :STRIP] = _dot(k_ref[0, 0, some, :], queries(i), 1, 1)
        score_s[1] = _dot(k_ref[0, 0, all_, :], queries(i + 1), 1, 1)
        _weigh(score_s[0, :STRIP], i, value_s[:, some], top_s, mix_s, ok)
        _weigh(score_s[1], i + 1, value_s[:, all_], top_s, mix_s, ok)

    lax.fori_loop(0, 4, pair, None)

    def finish(i, _):
        total = mix_s[i, HEAD : HEAD + 1, :]
        o_ref[head(i), :, rows(strip(i))] = mix_s[i, :HEAD, :] * (1 / total)
        lse_ref[0, pl.ds(head(i), 1), rows(strip(i))] = top_s[i] * SCALE + jnp.log(total)

    lax.fori_loop(0, 8, finish, None)


def attend_own(made, h):
    tokens = made.shape[2]
    bq = 2 * KEYS
    return pl.pallas_call(
        _own,
        grid=(tokens // bq,),
        in_specs=[
            pl.BlockSpec((1, 2, bq, HEAD), lambda i: (2 * h, 0, i, 0)),
            pl.BlockSpec((1, 1, tokens, HEAD), lambda i: (2 * h + 1, 0, 0, 0)),
            pl.BlockSpec((1, 1, tokens, HEAD), lambda i: (2 * h + 1, 1, 0, 0)),
        ],
        out_specs=[pl.BlockSpec((2, HEAD, bq), lambda i: (0, 0, i)), pl.BlockSpec((1, 2, bq), lambda i: (i, 0, 0))],
        out_shape=[jax.ShapeDtypeStruct((2, HEAD, tokens), jnp.float32), jax.ShapeDtypeStruct((tokens // bq, 2, bq), jnp.float32)],
        scratch_shapes=[
            pltpu.VMEM((2, KEYS, STRIP), jnp.float32), pltpu.VMEM((HEAD + 8, tokens), jnp.bfloat16),
            pltpu.VMEM((8, 1, STRIP), jnp.float32), pltpu.VMEM((8, HEAD + 8, STRIP), jnp.float32),
        ],
        compiler_params=pltpu.CompilerParams(dimension_semantics=("arbitrary",), vmem_limit_bytes=VMEM),
        cost_estimate=pl.CostEstimate(flops=4 * tokens * tokens * HEAD, transcendentals=tokens * tokens, bytes_accessed=made.size),
        name="attend_own",
    )(made, made, made)


def _cross(at_ref, came_ref, made_ref, own_ref, lse_in, o_ref, q_s, k_s, v_s, in_s, score_s, value_s, top_s, mix_s, sem, *, chunk):
    bq = o_ref.shape[3]
    tokens = k_s.shape[0]
    pieces = [(n, m) for n in range(2) for m in range(2)]
    count = tokens // KEYS
    first = at_ref[CHIP] == 0

    def queries(q_from):
        half = tokens // 2
        return [pltpu.make_async_copy(q_from.at[n, pl.ds(m * half + chunk * bq, bq), :], q_s.at[n, m], sem.at[2 * n + m]) for n, m in pieces]

    def keys(kv_from, b, n):
        rows = pl.ds(pl.multiple_of(b * KEYS, KEYS), KEYS)
        return pltpu.make_async_copy(kv_from.at[n, rows, :], (k_s, v_s)[n].at[rows, :], sem.at[4 + 2 * b + n])

    def start(q_from, kv_from):
        for copy in queries(q_from) + [keys(kv_from, b, n) for b in range(count) for n in range(2)]:
            copy.start()

    @pl.when(first)
    def _():
        start(came_ref, made_ref.at[1])

    @pl.when(jnp.logical_not(first))
    def _():
        start(made_ref.at[2], came_ref)

    carries = [
        pltpu.make_async_copy(own_ref.at[n, :, pl.ds(m * (tokens // 2) + chunk * bq, bq)], in_s.at[n, m], sem.at[4 + 2 * count + 2 * n + m])
        for n, m in pieces
    ]
    for copy in carries:
        copy.start()
    top_s[...] = jnp.full(top_s.shape, NEG, jnp.float32)
    mix_s[...] = jnp.zeros(mix_s.shape, jnp.float32)
    for copy in queries(came_ref) + [keys(came_ref, 0, 0)]:
        copy.wait()
    here = lambda b: pl.ds(pl.multiple_of(b * KEYS, KEYS), KEYS)
    score = lambda b, i: _dot(k_s[here(b), :], q_s[pieces[i]], 1, 1)
    score_s[0] = score(0, 0)

    def block(b, _):
        @pl.when(b + 1 < count)
        def _():
            keys(came_ref, b + 1, 0).wait()

        keys(came_ref, b, 1).wait()
        _turn(v_s[here(b), :], 0, value_s)
        for i in range(4):
            score_s[(i + 1) % 2] = score(b, i + 1) if i < 3 else score(jnp.minimum(b + 1, count - 1), 0)
            _weigh(score_s[i % 2], i, value_s[...], top_s, mix_s)

    lax.fori_loop(0, count, block, None)
    for copy in carries:
        copy.wait()

    def finish(s, _):
        n, m = lax.div(s, 2), lax.rem(s, 2)
        top, total = top_s[s] * SCALE, mix_s[s, HEAD : HEAD + 1, :]
        before = jnp.where(first, NEG, lse_in[m, pl.ds(n, 1), :])
        most = jnp.maximum(top, before)
        wa, wb = jnp.exp(top - most), jnp.exp(before - most)
        whole = total * wa + wb
        scale = 1 / whole
        o_ref[n, m, :HEAD, :] = (mix_s[s, :HEAD, :] * (wa * scale) + in_s[n, m] * (wb * scale)).astype(o_ref.dtype)
        o_ref[n, m, HEAD:, :] = _apart(most + jnp.log(whole))

    lax.fori_loop(0, 4, finish, None)


def _apart(row):
    rows = []
    for _ in range(3):
        rows.append(row.astype(jnp.bfloat16).astype(jnp.float32))
        row = row - rows[-1]
    return jnp.concatenate(rows + [jnp.zeros((13, row.shape[1]), jnp.float32)], axis=0).astype(jnp.bfloat16)


def _together(rows):
    wide = rows.astype(jnp.float32)
    return wide[0:1] + wide[1:2] + wide[2:3]


def attend_cross(at, came, made, own_o, own_lse, i):
    tokens = made.shape[2]
    half = tokens // 2
    bq = half // CHUNKS
    anywhere = pl.BlockSpec(memory_space=pl.ANY)
    return pl.pallas_call(
        functools.partial(_cross, chunk=i),
        grid_spec=pltpu.PrefetchScalarGridSpec(
            num_scalar_prefetch=1, grid=(1,),
            in_specs=[anywhere, anywhere, anywhere, pl.BlockSpec((2, 2, bq), lambda g, at_ref: (0, 0, i))],
            out_specs=pl.BlockSpec((2, 2, HEAD + 16, bq), lambda g, at_ref: (0, 0, 0, 0)),
            scratch_shapes=[
                pltpu.VMEM((2, 2, bq, HEAD), jnp.bfloat16), pltpu.VMEM((tokens, HEAD), jnp.bfloat16), pltpu.VMEM((tokens, HEAD), jnp.bfloat16),
                pltpu.VMEM((2, 2, HEAD, bq), jnp.float32), pltpu.VMEM((2, KEYS, STRIP), jnp.float32), pltpu.VMEM((HEAD + 8, KEYS), jnp.bfloat16),
                pltpu.VMEM((4, 1, STRIP), jnp.float32), pltpu.VMEM((4, HEAD + 8, STRIP), jnp.float32),
                pltpu.SemaphoreType.DMA((8 + 2 * (tokens // KEYS),)),
            ],
        ),
        out_shape=jax.ShapeDtypeStruct((2, 2, HEAD + 16, bq), jnp.bfloat16),
        compiler_params=pltpu.CompilerParams(dimension_semantics=("arbitrary",), vmem_limit_bytes=VMEM),
        cost_estimate=pl.CostEstimate(flops=16 * bq * tokens * HEAD, transcendentals=4 * bq * tokens, bytes_accessed=8 * tokens * HEAD),
        name="attend_cross",
    )(at, came, made, own_o, own_lse)


def _merge(at_ref, low0_ref, low1_ref, lse_ref, high0_ref, high1_ref, far0_ref, o0_ref, far1_ref, o1_ref, keep_ref, give_ref):
    chip, core = at_ref[CHIP], at_ref[CORE]
    n = pl.program_id(0)
    bq = far0_ref.shape[3]

    def fill(to_ref, low_ref, high_ref, side):
        for c, (far_ref, o_ref) in enumerate(((far0_ref, o0_ref), (far1_ref, o1_ref))):
            here = slice(c * bq, (c + 1) * bq)
            lse = lse_ref[side, pl.ds(n, 1), here]
            far_lse = jnp.where(chip == 0, NEG, _together(far_ref[0, side, HEAD:, :]))
            top = jnp.maximum(lse, far_lse)
            wa, wb = jnp.exp(lse - top), jnp.exp(far_lse - top)
            scale = 1 / (wa + wb)
            low = low_ref[0, :, here] * (wa * scale) + far_ref[0, side, :HEAD, :].astype(jnp.float32) * (wb * scale)
            high = jnp.where(chip == 0, high_ref[0, :, here].astype(jnp.bfloat16), o_ref[0, side, :HEAD, :])
            to_ref[0, 0, here, :] = low.astype(jnp.bfloat16).T
            to_ref[1, 0, here, :] = high.T

    fill(keep_ref, low0_ref, high0_ref, core)
    fill(give_ref, low1_ref, high1_ref, 1 - core)


def merge(at, low, low_lse, high, first, second, i):
    bq = first[0].shape[3]
    mine = [
        pl.BlockSpec((1, HEAD, 2 * bq), lambda n, at_ref: (n, 0, at_ref[CORE] * (CHUNKS // 2) + i)),
        pl.BlockSpec((1, HEAD, 2 * bq), lambda n, at_ref: (n, 0, (1 - at_ref[CORE]) * (CHUNKS // 2) + i)),
    ]
    part = pl.BlockSpec((1, 2, HEAD + 16, bq), lambda n, at_ref: (n, 0, 0, 0))
    result = pl.BlockSpec((2, 1, 2 * bq, HEAD), lambda n, at_ref: (0, n, 0, 0))
    return pl.pallas_call(
        _merge,
        grid_spec=pltpu.PrefetchScalarGridSpec(
            num_scalar_prefetch=1, grid=(2,),
            in_specs=[*mine, pl.BlockSpec((2, 2, 2 * bq), lambda n, at_ref: (0, 0, i)), *mine, part, part, part, part],
            out_specs=[result, result],
        ),
        out_shape=[jax.ShapeDtypeStruct((2, 2, 2 * bq, HEAD), jnp.bfloat16)] * 2,
        compiler_params=pltpu.CompilerParams(dimension_semantics=("arbitrary",), vmem_limit_bytes=VMEM),
        cost_estimate=pl.CostEstimate(flops=128 * bq * HEAD, transcendentals=0, bytes_accessed=128 * bq * HEAD),
        name="merge",
    )(at, low, low, low_lse, high, high, *first, *second)


def _output(at_ref, own_ref, sib_ref, x_ref, w_own, w_sib, wx, wy, vx, vy, *rest):
    y_ref = rest[-1]
    chip, group = at_ref[CHIP], at_ref[GROUP]
    weights = jnp.concatenate([w_own[...], wx[...], wy[...], w_sib[...], vx[...], vy[...]], axis=0)
    for at in range(0, y_ref.shape[0], 512):
        here = slice(at, at + 512)
        parts = []
        for o_ref in (own_ref, sib_ref):
            parts += [o_ref[chip, 0, here], o_ref[chip, 1, here], o_ref[1 - chip, group, here], o_ref[1 - chip, 1 - group, here]]
        y = _dot(jnp.concatenate(parts, axis=1), weights, 1, 0)
        y_ref[here, :] = (x_ref[here, :].astype(jnp.float32) + y).astype(y_ref.dtype)


def output(at, x, weights, own, sib, i, done):
    rows, width = own.shape[2], x.shape[1]
    bn = 768
    part = pl.BlockSpec(own.shape, lambda j, at_ref: (0, 0, 0, 0))
    here = pl.BlockSpec((rows, bn), lambda j, at_ref: (i, j))
    given = [own, sib, x, *weights]
    specs = [part, part, here] + [pl.BlockSpec((w.shape[0], bn), lambda j, at_ref: (0, j)) for w in weights]
    alias = {}
    if done is not None:
        given.append(done)
        specs.append(pl.BlockSpec(memory_space=pl.ANY))
        alias = {len(given): 0}
    return pl.pallas_call(
        _output,
        grid_spec=pltpu.PrefetchScalarGridSpec(num_scalar_prefetch=1, grid=(width // bn,), in_specs=specs, out_specs=here),
        out_shape=jax.ShapeDtypeStruct(x.shape, jnp.bfloat16),
        input_output_aliases=alias,
        compiler_params=pltpu.CompilerParams(dimension_semantics=("arbitrary",), vmem_limit_bytes=VMEM),
        cost_estimate=pl.CostEstimate(flops=2 * rows * 8 * HEAD * width, transcendentals=0, bytes_accessed=16 * HEAD * width),
        name="output",
    )(at, *given)


def tables(place):
    half = HEAD // 2
    angle = place.astype(jnp.float32)[:, None] * THETA ** (-jnp.arange(half, dtype=jnp.float32) / half)
    return jnp.cos(angle), jnp.sin(angle)


def solution(mesh):
    def step(x, gain, wq, wk, wv, wo):
        own = x.shape[0]
        rank, group = lax.axis_index("sp"), lax.axis_index("dp")
        chip, core = rank // 2, rank % 2

        pick = lambda n, which: jnp.where(which == 0, ORDER[0][n], ORDER[1][n])
        at = jnp.stack([pick(n, chip) for n in range(4)] + [pick(n, 1 - chip) for n in range(4)] + [chip, core, group]).astype(jnp.int32)

        w_own, w_give = share(at, wq, wk, wv)
        w_sib = lax.ppermute(w_give, "sp", SIBLING)
        leaving = leave(at, w_own, w_sib)
        wx, wy = [], []
        for n in range(4):
            wx.append(lax.ppermute(leaving[n], "sp", ACROSS))
            wy.append(lax.ppermute(wx[n], "dp", GROUPS))

        a_own = normed(x, gain)
        a_sib = lax.ppermute(a_own, "sp", SIBLING)
        cos, sin = tables(chip * 2 * own + jnp.arange(2 * own))

        made, sent = None, None
        for n in range(4):
            got = project(at, a_own, a_sib, w_own, w_sib, wx[n], wy[n], cos, sin, n, made)
            made = got[0]
            if n == 0:
                sent = got[1]
        came = lax.ppermute(sent, "sp", ACROSS)

        wo_here, _ = lax.optimization_barrier((wo, sent))
        wo_half = lax.dynamic_slice_in_dim(wo_here, group * HEAD, HEAD, axis=0)
        ox = lax.ppermute(wo_half, "sp", ACROSS)
        oy = lax.ppermute(ox, "dp", GROUPS)
        wo_sib, ox_sib, oy_sib = (lax.ppermute(w, "sp", SIBLING) for w in (wo_here, ox, oy))
        weights = (wo, wo_sib, ox, oy, ox_sib, oy_sib)

        high, high_lse = attend_own(made, 1)
        parts = []
        for i in range(CHUNKS):
            o = attend_cross(at, came, made, high, high_lse, i)
            parts.append((lax.ppermute(o, "sp", BACK), o))
        low, low_lse = attend_own(made, 0)
        y, results = None, []
        for i in range(CHUNKS // 2):
            keep, give = merge(at, low, low_lse, high, *parts[2 * i : 2 * i + 2], i)
            results.append((keep, lax.ppermute(give, "sp", SIBLING)))
        for i, (keep, take) in enumerate(results):
            y = output(at, x, weights, keep, take, i, y)
        return y

    tokens, whole = P(("dp", "sp"), None), P("sp", None)
    return jax.shard_map(
        step,
        mesh=mesh,
        in_specs=(tokens, P(None), whole, whole, whole, whole),
        out_specs=tokens,
        check_vma=False,
    )
```
